32 devices in a mesh: lat: 4 (over y, x), lon: 8 (over z, core).
Axes of the slice: x: 2, y: 2, z: 4, core: 2. Of those that a mesh axis runs over, the one named last changes fastest.
Arguments:
- pressure: float32 [4, 30, 5120], P('lat', None, 'lon'), may hold values from -6 to 6
- velocity: float32 [4, 30, 7680], P('lat', None, 'lon'), may hold values from -6 to 6
- edge_cells: int32 [4, 2, 7680], P('lat', None, 'lon'), may hold values from 0 to 1663
- cell_edges: int32 [4, 3, 5120], P('lat', None, 'lon'), may hold values from 0 to 1983
- send_cells: int32 [4, 8, 1024], P('lat', None, 'lon'), may hold values from 0 to 639
- send_edges: int32 [4, 8, 1024], P('lat', None, 'lon'), may hold values from 0 to 959
- inv_dual: float32 [4, 7680], P('lat', 'lon'), may hold values from 0.5 to 2
- edge_weight: float32 [4, 3, 5120], P('lat', None, 'lon'), may hold values from -3 to 3
- sound_speed: float32 [4, 5120], P('lat', 'lon'), may hold values from 0.1 to 0.6
- coupling: float32 [4, 30, 5120], P('lat', None, 'lon'), may hold values from 0.1 to 2
Outputs:
- pressure_out: float32 [4, 30, 5120], P('lat', None, 'lon')
- velocity_out: float32 [4, 30, 7680], P('lat', None, 'lon')
The draws below stay inside these ranges and needn't reach their ends.
Inputs may be any that keep to these rules, and one draw needn't show every extreme that they name: `edge_cells`: positions below 640 are own cells; position 640 + r * 128 + j is slot j of the halo piece from the neighbour at offset number r. `cell_edges`: positions below 960 are own edges; position 960 + r * 128 + j is slot j of the edge halo piece from the neighbour at offset number r. `send_cells`: indices of own cells. `send_edges`: indices of own edges.
All inputs are finite; a program needn't handle non-finite values.
Results may differ from the reference program's by a relative error of at most 0.0001.
Values sent between devices are 32-bit elements; how exact they have to be, the bound alone decides.
No kernel may reach another device: no remote copies, remote signals or barrier semaphores. Data moves between devices by JAX's collectives and lax.ppermute only.
A program may use at most 64 MiB of HBM per device.

```python
import math
import jax
import jax.numpy as jnp
from jax import lax

C_DEV = 640
E_DEV = 960
HALO = 128
NLEV = 30
NSUB = 3
CELLS_ROW = 5120
EDGES_ROW = 7680
SLOTS_ROW = 1024
N_LAT = 4
N_LON = 8


def with_ends(values, own_key, smallest, largest):
    spot = [jax.random.randint(jax.random.fold_in(own_key, axis), (), 0, length) for axis, length in enumerate(values.shape)]
    longest = values.shape.index(max(values.shape))
    neighbour = spot[:longest] + [(spot[longest] + 1) % values.shape[longest]] + spot[longest + 1:]
    return values.at[tuple(spot)].set(smallest).at[tuple(neighbour)].set(largest)


def block_levels(own_key, dims, cuts, low, top_value):
    factor_of, own = 1.0, jax.random.fold_in(own_key, 6)
    for dim, shards_of in cuts:
        heights = jnp.exp(jax.random.uniform(jax.random.fold_in(own, dim), (shards_of,), jnp.float32, low / len(cuts), top_value / len(cuts)))
        factor_of = factor_of * jnp.repeat(heights, dims[dim] // shards_of).reshape([-1 if axis == dim else 1 for axis in range(len(dims))])
    return factor_of


def normal_values(rng, extent, scale, bound, cuts=(), kind=jnp.bfloat16):
    values = scale * jax.random.normal(rng, extent, jnp.float32)
    if cuts:
        values = values * block_levels(rng, extent, cuts, -0.22, 0.18)
    return jnp.clip(values, -bound, bound).astype(kind)


def setup_inputs(seed: int = 0) -> dict:
    streams_of = jax.random.split(jax.random.key(seed), 11)
    return {
        "pressure": normal_values(streams_of[0], (N_LAT, NLEV, CELLS_ROW), 1.0, 6.0, ((0, 4), (2, 8)), jnp.float32),
        "velocity": normal_values(streams_of[1], (N_LAT, NLEV, EDGES_ROW), 1.0, 6.0, ((0, 4), (2, 8)), jnp.float32),
        "edge_cells": with_ends(jax.random.randint(streams_of[2], (N_LAT, 2, EDGES_ROW), 0, C_DEV + 8 * HALO), jax.random.fold_in(streams_of[2], 1), 0, (C_DEV + 8 * HALO) - 1).astype(jnp.int32),
        "cell_edges": with_ends(jax.random.randint(streams_of[3], (N_LAT, 3, CELLS_ROW), 0, E_DEV + 8 * HALO), jax.random.fold_in(streams_of[3], 1), 0, (E_DEV + 8 * HALO) - 1).astype(jnp.int32),
        "send_cells": with_ends(jax.random.randint(streams_of[4], (N_LAT, 8, SLOTS_ROW), 0, C_DEV), jax.random.fold_in(streams_of[4], 1), 0, C_DEV - 1).astype(jnp.int32),
        "send_edges": with_ends(jax.random.randint(streams_of[5], (N_LAT, 8, SLOTS_ROW), 0, E_DEV), jax.random.fold_in(streams_of[5], 1), 0, E_DEV - 1).astype(jnp.int32),
        "inv_dual": jnp.clip(jnp.exp(math.log(2.0) - 1.3862944 * jax.random.uniform(streams_of[6], (N_LAT, EDGES_ROW), jnp.float32) ** block_levels(streams_of[6], (N_LAT, EDGES_ROW), ((0, 4), (1, 8)), -0.2, 0.2)), 0.5, 2.0),
        "edge_weight": normal_values(streams_of[7], (N_LAT, 3, CELLS_ROW), 0.5, 3.0, ((0, 4), (2, 8)), jnp.float32),
        "sound_speed": jnp.clip(jnp.exp(math.log(0.6) - 1.7917595 * jax.random.uniform(streams_of[8], (N_LAT, CELLS_ROW), jnp.float32) ** block_levels(streams_of[8], (N_LAT, CELLS_ROW), ((0, 4), (1, 8)), -0.2, 0.2)), 0.1, 0.6),
        "coupling": jnp.clip(jnp.exp(math.log(2.0) - 2.9957323 * jax.random.uniform(streams_of[9], (N_LAT, NLEV, CELLS_ROW), jnp.float32) ** block_levels(streams_of[9], (N_LAT, NLEV, CELLS_ROW), ((0, 4), (2, 8)), -0.2, 0.2)), 0.1, 2.0),
    }


DIRECTIONS = ((-1, -1), (-1, 0), (-1, 1), (0, -1), (0, 1), (1, -1), (1, 0), (1, 1))
step_scale = 0.5


def position(offset):
    return DIRECTIONS.index(offset)


def edge_update(normal, extended, edge_cells, inv_dual):
    gradient = (jnp.take(extended, edge_cells[1], axis=1) - jnp.take(extended, edge_cells[0], axis=1)) * inv_dual[None, :]
    return normal - step_scale * gradient


def column_solve(right_side, coupling):
    levels = right_side.shape[0]
    ratios = []
    scaled = []
    for level_index in range(levels):
        if level_index < levels - 1:
            upper_term = -coupling[level_index]
        else:
            upper_term = 0.0 * coupling[0]
        if level_index == 0:
            divisor = 1.0 + coupling[0]
            current = right_side[0] / divisor
        else:
            lower_term = -coupling[level_index - 1]
            diagonal = 1.0 + coupling[level_index - 1] + coupling[level_index]
            divisor = diagonal - lower_term * ratios[-1]
            current = (right_side[level_index] - lower_term * scaled[-1]) / divisor
        ratios.append(upper_term / divisor)
        scaled.append(current)
    result = [scaled[-1]]
    for level_index in range(levels - 2, -1, -1):
        result.insert(0, scaled[level_index] - ratios[level_index] * result[0])
    return jnp.stack(result)


def cell_update(values, edges_ext, cell_edges, edge_weight, sound_speed, coupling):
    divergence = jnp.take(edges_ext, cell_edges[0], axis=1) * edge_weight[0][None, :]
    divergence = divergence + jnp.take(edges_ext, cell_edges[1], axis=1) * edge_weight[1][None, :]
    divergence = divergence + jnp.take(edges_ext, cell_edges[2], axis=1) * edge_weight[2][None, :]
    right_side = values - sound_speed[None, :] * divergence
    return column_solve(right_side, coupling)


def device_layout(array, width):
    if array.ndim == 2:
        return array.reshape(N_LAT, N_LON, width)
    return array.reshape(N_LAT, array.shape[1], N_LON, width).transpose(0, 2, 1, 3)


def global_layout(array):
    return array.transpose(0, 2, 1, 3).reshape(N_LAT, array.shape[2], N_LON * array.shape[3])


def take_pieces(source, indices):
    return jnp.take(source, indices, axis=1)


def reference_extend(source, send_list):
    taker = jax.vmap(jax.vmap(take_pieces))
    pieces = []
    for offset in DIRECTIONS:
        piece = taker(source, send_list[:, :, position((-offset[0], -offset[1]))])
        piece = jnp.roll(piece, -offset[1], axis=1)
        if offset[0] == 1:
            piece = jnp.concatenate([piece[1:], jnp.zeros_like(piece[:1])], axis=0)
        elif offset[0] == -1:
            piece = jnp.concatenate([jnp.zeros_like(piece[:1]), piece[:-1]], axis=0)
        pieces.append(piece)
    return jnp.concatenate([source] + pieces, axis=3)


def band_edges(operands):
    return jax.vmap(edge_update)(*operands)


def band_cells(operands):
    return jax.vmap(cell_update)(*operands)


def reference(pressure, velocity, edge_cells, cell_edges, send_cells, send_edges, inv_dual, edge_weight, sound_speed, coupling):
    values = device_layout(pressure, C_DEV)
    normal = device_layout(velocity, E_DEV)
    edge_pairs = device_layout(edge_cells, E_DEV)
    cell_sides = device_layout(cell_edges, C_DEV)
    cell_lists = device_layout(send_cells, HALO)
    edge_lists = device_layout(send_edges, HALO)
    inverse = device_layout(inv_dual, E_DEV)
    weights = device_layout(edge_weight, C_DEV)
    speeds = device_layout(sound_speed, C_DEV)
    couples = device_layout(coupling, C_DEV)
    for substep in range(NSUB):
        extended = reference_extend(values, cell_lists)
        normal = lax.map(band_edges, (normal, extended, edge_pairs, inverse))
        edges_ext = reference_extend(normal, edge_lists)
        values = lax.map(band_cells, (values, edges_ext, cell_sides, weights, speeds, couples))
    return global_layout(values), global_layout(normal)
```

```python
import functools

import jax
import jax.numpy as jnp
from jax import lax
from jax.experimental import pallas as pl
from jax.experimental.pallas import tpu as pltpu
from jax.sharding import PartitionSpec as P

NSUB = 3
STEP_SCALE = 0.5
LANES = 128
PARTS = 3

f32 = jnp.float32
bf16 = jnp.bfloat16


def round_up(value, step):
    return -(-value // step) * step


def swap_routes(count):
    inner = [(i, i ^ 1) for i in range(count)]
    outer = [(i, (((i + 1) ^ 1) - 1) % count) for i in range(count)]
    return inner, outer


LOCAL = ((0, 1), (0, 2), (1, 1), (1, 2), (1, 0), (2, 1), (2, 2), (2, 0))
SENT = ((0, 1), (1, 1), (2, 1), (0, 2), (1, 2), (2, 2), (1, 0), (2, 0))


def link_signs(a, b):
    lat_inner = 1 - 2 * lax.rem(a, 2)
    lon_inner = 1 - 2 * lax.rem(b, 2)
    return lat_inner, lon_inner


def sent_row(member, lat_inner, lon_inner):
    lat_link, lon_link = member
    p = (0, lat_inner, -lat_inner)[lat_link]
    q = (0, lon_inner, -lon_inner)[lon_link]
    flat = (p + 1) * 3 + (q + 1)
    return flat - jnp.where(flat > 4, 1, 0)


def local_positions(index, own, own_padded, halo, a, b, lat_count):
    lat_inner, lon_inner = link_signs(a, b)
    beyond = index - own
    piece = lax.div(jnp.maximum(beyond, 0), halo)
    slot = beyond - piece * halo
    flat = piece + jnp.where(piece >= 4, 1, 0)
    p = jnp.where(flat >= 6, 1, jnp.where(flat >= 3, 0, -1))
    q = flat - 3 * (p + 1) - 1
    lat_is_inner = p == lat_inner
    lon_member = jnp.where(q == 0, 2, jnp.where(q == lon_inner, 0, 1))
    member = jnp.where(p == 0, lon_member, jnp.where(lat_is_inner, 2, 5) + lon_member)
    outside = (a + p < 0) | (a + p >= lat_count)
    row = own_padded + member * halo + slot
    return jnp.where(beyond < 0, index, jnp.where(outside, -1, row))


def split_parts(value):
    parts = []
    rest = value
    for part in range(PARTS):
        piece = rest.astype(bf16)
        parts.append(piece)
        if part < PARTS - 1:
            rest = rest - piece.astype(f32)
    return parts


def put_parts(stack_ref, value, start):
    rows, width = value.shape
    for part, piece in enumerate(split_parts(value)):
        stack_ref[part * rows : (part + 1) * rows, start : start + width] = piece


def sum_parts(product, rows):
    total = product[(PARTS - 1) * rows : PARTS * rows]
    for part in range(PARTS - 2, -1, -1):
        total = total + product[part * rows : (part + 1) * rows]
    return total


def matmul(left, right):
    return jnp.dot(left, right, preferred_element_type=f32)


def fill_sent(matrix_ref, list_ref, lat_inner, lon_inner):
    rows = matrix_ref.shape[0]
    halo = list_ref.shape[1]
    lanes = [list_ref[pl.ds(sent_row(member, lat_inner, lon_inner), 1), :] for member in SENT]
    block = 16

    def body(step, carry):
        first = pl.multiple_of(step * block, block)
        row = lax.broadcasted_iota(jnp.int32, (block, halo), 0) + first
        for member, index in enumerate(lanes):
            hit = jnp.where(row == index, 1.0, 0.0).astype(bf16)
            matrix_ref[pl.ds(first, block), member * halo : (member + 1) * halo] = hit
        return carry

    lax.fori_loop(0, rows // block, body, 0)


def store_sent(product, rows, halo, inner_ref, outer_ref, lat_inner_ref, lat_outer_ref):
    pieces = sum_parts(product, rows)
    for member in range(3):
        inner_ref[member] = pieces[:, member * halo : (member + 1) * halo]
        outer_ref[member] = pieces[:, (3 + member) * halo : (4 + member) * halo]
    lat_inner_ref[...] = pieces[:, 6 * halo : 7 * halo]
    lat_outer_ref[...] = pieces[:, 7 * halo : 8 * halo]


def put_extended(stack_ref, own, inner_ref, outer_ref, lat_inner_ref, lat_outer_ref):
    halo = inner_ref.shape[2]
    start = own.shape[1]
    put_parts(stack_ref, own, 0)
    pieces = [inner_ref[0], outer_ref[0]]
    pieces += [lat_inner_ref[i] for i in range(3)] + [lat_outer_ref[i] for i in range(3)]
    for member, piece in enumerate(pieces):
        put_parts(stack_ref, piece, start + member * halo)


def start_kernel(pressure_ref, list_ref, cells_ref, inner_ref, outer_ref, lat_inner_ref, lat_outer_ref, matrix_ref, stack_ref):
    a, b = lax.axis_index("lat"), lax.axis_index("lon")
    lat_inner, lon_inner = link_signs(a, b)
    levels = pressure_ref.shape[0]
    rows = cells_ref.shape[0]
    cells_ref[0:levels, :] = pressure_ref[:, 0, :]
    cells_ref[levels:rows, :] = jnp.zeros((rows - levels, cells_ref.shape[1]), f32)
    fill_sent(matrix_ref, list_ref, lat_inner, lon_inner)
    put_parts(stack_ref, cells_ref[...], 0)
    product = matmul(stack_ref[...], matrix_ref[...])
    store_sent(product, rows, list_ref.shape[1], inner_ref, outer_ref, lat_inner_ref, lat_outer_ref)


def build_kernel(
    velocity_ref,
    edge_cells_ref,
    cell_edges_ref,
    send_edges_ref,
    weight_ref,
    coupling_ref,
    edges_ref,
    gradient_ref,
    high_ref,
    low_ref,
    matrix_ref,
    inverse_ref,
    forward_ref,
    back_ref,
    coupling_scr,
    *,
    lat_count,
):
    a, b = lax.axis_index("lat"), lax.axis_index("lon")
    lat_inner, lon_inner = link_signs(a, b)
    levels = velocity_ref.shape[0]
    rows, edge_pad = edges_ref.shape
    edges = velocity_ref.shape[2]
    cells = cell_edges_ref.shape[1]
    halo = send_edges_ref.shape[1]

    edges_ref[...] = jnp.zeros((rows, edge_pad), f32)
    edges_ref[0:levels, 0:edges] = velocity_ref[:, 0, :]
    fill_sent(matrix_ref, send_edges_ref, lat_inner, lon_inner)

    ends = local_positions(edge_cells_ref[...], cells, cells, halo, a, b, lat_count)
    if edge_pad > edges:
        ends = jnp.concatenate([ends, jnp.full((2, edge_pad - edges), -1, jnp.int32)], axis=1)
    near = ends[0:1, :]
    far = ends[1:2, :]
    block = 16

    def gradient_body(step, carry):
        first = pl.multiple_of(step * block, block)
        row = lax.broadcasted_iota(jnp.int32, (block, edge_pad), 0) + first
        entry = jnp.where(row == far, 1.0, 0.0) - jnp.where(row == near, 1.0, 0.0)
        gradient_ref[pl.ds(first, block), :] = entry.astype(bf16)
        return carry

    lax.fori_loop(0, gradient_ref.shape[0] // block, gradient_body, 0)

    sides = local_positions(cell_edges_ref[...], edges, edge_pad, halo, a, b, lat_count)
    weight = weight_ref[...]

    def weight_body(step, carry):
        first = pl.multiple_of(step * block, block)
        row = lax.broadcasted_iota(jnp.int32, (block, cells), 0) + first
        entry = jnp.where(row == sides[0:1, :], weight[0:1, :], 0.0)
        entry = entry + jnp.where(row == sides[1:2, :], weight[1:2, :], 0.0)
        entry = entry + jnp.where(row == sides[2:3, :], weight[2:3, :], 0.0)
        high = entry.astype(bf16)
        high_ref[pl.ds(first, block), :] = high
        low_ref[pl.ds(first, block), :] = (entry - high.astype(f32)).astype(bf16)
        return carry

    lax.fori_loop(0, high_ref.shape[0] // block, weight_body, 0)

    for group in range(cells // LANES):
        coupling_scr[0:levels, group, :] = coupling_ref[:, 0, group * LANES : (group + 1) * LANES]
    above = coupling_scr[0]
    divisor = 1.0 + above
    inverse = 1.0 / divisor
    inverse_ref[0] = inverse
    ratio = above * inverse
    back_ref[0] = ratio
    for level in range(1, levels):
        below = above
        above = coupling_scr[level]
        divisor = 1.0 + below + above - below * ratio
        inverse = 1.0 / divisor
        inverse_ref[level] = inverse
        forward_ref[level] = below * inverse
        ratio = above * inverse
        back_ref[level] = ratio


def edge_kernel(
    cells_ref,
    inner_in,
    outer_in,
    lat_inner_in,
    lat_outer_in,
    edges_ref,
    dual_ref,
    gradient_ref,
    matrix_ref,
    new_edges_ref,
    inner_ref,
    outer_ref,
    lat_inner_ref,
    lat_outer_ref,
    stack_ref,
    own_stack_ref,
):
    rows = cells_ref.shape[0]
    edges = dual_ref.shape[1]
    edge_pad = edges_ref.shape[1]
    put_extended(stack_ref, cells_ref[...], inner_in, outer_in, lat_inner_in, lat_outer_in)
    difference = sum_parts(matmul(stack_ref[...], gradient_ref[...]), rows)
    scale = STEP_SCALE * dual_ref[...]
    if edge_pad > edges:
        scale = jnp.concatenate([scale, jnp.zeros((1, edge_pad - edges), f32)], axis=1)
    new_edges = edges_ref[...] - scale * difference
    new_edges_ref[...] = new_edges
    put_parts(own_stack_ref, new_edges, 0)
    product = matmul(own_stack_ref[...], matrix_ref[...])
    store_sent(product, rows, inner_in.shape[2], inner_ref, outer_ref, lat_inner_ref, lat_outer_ref)


def solve_columns(edges_ref, pieces, cells_ref, speed_ref, high_ref, low_ref, inverse_ref, forward_ref, back_ref, levels, stack_ref, column_scr):
    rows, cells = cells_ref.shape
    put_extended(stack_ref, edges_ref[...], *pieces)
    stack = stack_ref[...]
    divergence = sum_parts(matmul(stack, high_ref[...]) + matmul(stack, low_ref[...]), rows)
    right_side = cells_ref[...] - speed_ref[...] * divergence
    for group in range(cells // LANES):
        column_scr[:, group, :] = right_side[:, group * LANES : (group + 1) * LANES]
    current = column_scr[0] * inverse_ref[0]
    scaled = [current]
    for level in range(1, levels):
        current = column_scr[level] * inverse_ref[level] + forward_ref[level] * current
        scaled.append(current)
    column_scr[levels - 1] = current
    for level in range(levels - 2, -1, -1):
        current = scaled[level] + back_ref[level] * current
        column_scr[level] = current
    for level in range(levels, rows):
        column_scr[level] = jnp.zeros_like(current)


def cell_kernel(
    edges_ref,
    inner_in,
    outer_in,
    lat_inner_in,
    lat_outer_in,
    cells_ref,
    speed_ref,
    high_ref,
    low_ref,
    inverse_ref,
    forward_ref,
    back_ref,
    matrix_ref,
    new_cells_ref,
    inner_ref,
    outer_ref,
    lat_inner_ref,
    lat_outer_ref,
    stack_ref,
    own_stack_ref,
    column_scr,
    *,
    levels,
):
    rows, cells = cells_ref.shape
    pieces = (inner_in, outer_in, lat_inner_in, lat_outer_in)
    solve_columns(edges_ref, pieces, cells_ref, speed_ref, high_ref, low_ref, inverse_ref, forward_ref, back_ref, levels, stack_ref, column_scr)
    for group in range(cells // LANES):
        part = column_scr[:, group, :]
        new_cells_ref[:, group * LANES : (group + 1) * LANES] = part
        put_parts(own_stack_ref, part, group * LANES)
    product = matmul(own_stack_ref[...], matrix_ref[...])
    store_sent(product, rows, inner_in.shape[2], inner_ref, outer_ref, lat_inner_ref, lat_outer_ref)


def last_kernel(
    edges_ref,
    inner_in,
    outer_in,
    lat_inner_in,
    lat_outer_in,
    cells_ref,
    speed_ref,
    high_ref,
    low_ref,
    inverse_ref,
    forward_ref,
    back_ref,
    out_ref,
    stack_ref,
    column_scr,
    *,
    levels,
):
    cells = cells_ref.shape[1]
    pieces = (inner_in, outer_in, lat_inner_in, lat_outer_in)
    solve_columns(edges_ref, pieces, cells_ref, speed_ref, high_ref, low_ref, inverse_ref, forward_ref, back_ref, levels, stack_ref, column_scr)
    for group in range(cells // LANES):
        out_ref[:, 0, group * LANES : (group + 1) * LANES] = column_scr[0:levels, group, :]


def call(body, name, outs, scratch, limit_mib, *operands):
    return pl.pallas_call(
        body,
        out_shape=tuple(jax.ShapeDtypeStruct(shape, kind) for shape, kind in outs),
        scratch_shapes=[pltpu.VMEM(shape, kind) for shape, kind in scratch],
        compiler_params=pltpu.CompilerParams(vmem_limit_bytes=limit_mib * 1024 * 1024),
        name=name,
    )(*operands)


def on_device(lat_count, lon_count, pressure, velocity, edge_cells, cell_edges, send_cells, send_edges, inv_dual, edge_weight, sound_speed, coupling):
    _, levels, cells = pressure.shape
    edges = velocity.shape[2]
    halo = send_cells.shape[2]
    rows = round_up(levels, 16)
    edge_pad = round_up(edges, 2 * LANES)
    sent = [((3, rows, halo), f32)] * 2 + [((rows, halo), f32)] * 2
    lon_routes = swap_routes(lon_count)
    lat_routes = swap_routes(lat_count)

    def exchange(pieces):
        inner, outer, lat_inner, lat_outer = pieces
        outer_in = lax.ppermute(outer, "lon", lon_routes[1])
        inner_in = lax.ppermute(inner, "lon", lon_routes[0])
        first = jnp.stack([inner_in[1], outer_in[1], lat_inner])
        second = jnp.stack([inner_in[2], outer_in[2], lat_outer])
        second_in = lax.ppermute(second, "lat", lat_routes[1])
        first_in = lax.ppermute(first, "lat", lat_routes[0])
        return inner_in, outer_in, first_in, second_in

    by_level = lambda value: value.transpose(1, 0, 2)
    stack_cells = ((PARTS * rows, cells), bf16)
    stack_edges = ((PARTS * rows, edge_pad), bf16)
    column = ((rows, cells // LANES, LANES), f32)

    values, *pieces, cell_matrix = call(
        start_kernel,
        "start",
        [((rows, cells), f32)] + sent + [((cells, 8 * halo), bf16)],
        [stack_cells],
        16,
        by_level(pressure),
        send_cells[0],
    )
    normal, gradient, high, low, edge_matrix, inverse, forward, back = call(
        functools.partial(build_kernel, lat_count=lat_count),
        "build",
        [
            ((rows, edge_pad), f32),
            ((cells + 8 * halo, edge_pad), bf16),
            ((edge_pad + 8 * halo, cells), bf16),
            ((edge_pad + 8 * halo, cells), bf16),
            ((edge_pad, 8 * halo), bf16),
            column,
            column,
            column,
        ],
        [column],
        24,
        by_level(velocity),
        edge_cells[0],
        cell_edges[0],
        send_edges[0],
        edge_weight[0],
        by_level(coupling),
    )
    for substep in range(NSUB):
        arrived = exchange(pieces)
        normal, *pieces = call(
            edge_kernel,
            "edges",
            [((rows, edge_pad), f32)] + sent,
            [((PARTS * rows, cells + 8 * halo), bf16), stack_edges],
            24,
            values,
            *arrived,
            normal,
            inv_dual,
            gradient,
            edge_matrix,
        )
        arrived = exchange(pieces)
        operands = (normal, *arrived, values, sound_speed, high, low, inverse, forward, back)
        stack = ((PARTS * rows, edge_pad + 8 * halo), bf16)
        if substep < NSUB - 1:
            values, *pieces = call(
                functools.partial(cell_kernel, levels=levels),
                "cells",
                [((rows, cells), f32)] + sent,
                [stack, stack_cells, column],
                24,
                *operands,
                cell_matrix,
            )
        else:
            (values,) = call(
                functools.partial(last_kernel, levels=levels),
                "last",
                [((levels, 1, cells), f32)],
                [stack, column],
                24,
                *operands,
            )
    return by_level(values), normal[:levels, :edges][None]


def solution(mesh):
    return jax.shard_map(
        functools.partial(on_device, mesh.shape["lat"], mesh.shape["lon"]),
        mesh=mesh,
        in_specs=(
            P("lat", None, "lon"),
            P("lat", None, "lon"),
            P("lat", None, "lon"),
            P("lat", None, "lon"),
            P("lat", None, "lon"),
            P("lat", None, "lon"),
            P("lat", "lon"),
            P("lat", None, "lon"),
            P("lat", "lon"),
            P("lat", None, "lon"),
        ),
        out_specs=(P("lat", None, "lon"), P("lat", None, "lon")),
        check_vma=False,
    )
```

```python
import functools

import jax
import jax.numpy as jnp
from jax import lax
from jax.experimental import pallas as pl
from jax.experimental.pallas import tpu as pltpu
from jax.sharding import PartitionSpec as P


NSUB = 3
STEP_SCALE = 0.5
LANES = 128
PARTS = 3

f32 = jnp.float32
bf16 = jnp.bfloat16
i16 = jnp.int16


def round_up(value, step):
    return -(-value // step) * step


def swap_routes(count):
    inner = [(i, i ^ 1) for i in range(count)]
    outer = [(i, (((i + 1) ^ 1) - 1) % count) for i in range(count)]
    return inner, outer


OUTER_SENT = ((0, 2), (1, 2), (2, 2))
REST_SENT = ((0, 1), (1, 1), (2, 1), (1, 0), (2, 0))


def link_signs():
    lat_inner = 1 - 2 * lax.rem(lax.axis_index("lat"), 2)
    lon_inner = 1 - 2 * lax.rem(lax.axis_index("lon"), 2)
    return lat_inner, lon_inner


def sent_row(member):
    lat_inner, lon_inner = link_signs()
    lat_link, lon_link = member
    p = (0, lat_inner, -lat_inner)[lat_link]
    q = (0, lon_inner, -lon_inner)[lon_link]
    flat = (p + 1) * 3 + (q + 1)
    return flat - jnp.where(flat > 4, 1, 0)


def local_positions(index, own, own_padded, halo, lat_count):
    lat_inner, lon_inner = link_signs()
    a = lax.axis_index("lat")
    beyond = index - own
    piece = lax.div(jnp.maximum(beyond, 0), halo)
    slot = beyond - piece * halo
    flat = piece + jnp.where(piece >= 4, 1, 0)
    p = jnp.where(flat >= 6, 1, jnp.where(flat >= 3, 0, -1))
    q = flat - 3 * (p + 1) - 1
    lon_member = jnp.where(q == 0, 2, jnp.where(q == lon_inner, 0, 1))
    member = jnp.where(p == 0, lon_member, jnp.where(p == lat_inner, 2, 5) + lon_member)
    outside = (a + p < 0) | (a + p >= lat_count)
    row = own_padded + member * halo + slot
    return jnp.where(beyond < 0, index, jnp.where(outside, -1, row))


def put_parts(stack_ref, value, start):
    rows, width = value.shape
    rest = value
    for part in range(PARTS):
        piece = rest.astype(bf16)
        stack_ref[part * rows : (part + 1) * rows, start : start + width] = piece
        if part < PARTS - 1:
            rest = rest - piece.astype(f32)


def sum_parts(product, rows):
    total = product[(PARTS - 1) * rows : PARTS * rows]
    for part in range(PARTS - 2, -1, -1):
        total = total + product[part * rows : (part + 1) * rows]
    return total


def gather_matmul(stack_ref, matrices, rows):
    product = None
    for matrix in matrices:
        term = jnp.dot(stack_ref[...], matrix, preferred_element_type=f32)
        product = term if product is None else product + term
    return sum_parts(product, rows)


def fetch(pairs, sems):
    copies = [pltpu.make_async_copy(source, target, sems.at[i]) for i, (source, target) in enumerate(pairs)]
    for copy in copies:
        copy.start()
    for copy in copies:
        copy.wait()


def by_blocks(rows, body):
    block = 64 if rows % 64 == 0 else 16

    def step(i, carry):
        first = pl.multiple_of(i * block, block)
        body(first, block)
        return carry

    lax.fori_loop(0, rows // block, step, 0)


def row_numbers(first, block, width):
    return (lax.broadcasted_iota(jnp.int32, (block, width), 0) + first).astype(i16)


def fill_sent(matrix_ref, list_ref, members):
    rows = matrix_ref.shape[0]
    halo = list_ref.shape[1]
    lanes = [list_ref[pl.ds(sent_row(member), 1), :].astype(i16) for member in members]

    def body(first, block):
        row = row_numbers(first, block, halo)
        for member, index in enumerate(lanes):
            hit = jnp.where(row == index, jnp.ones((), bf16), jnp.zeros((), bf16))
            matrix_ref[pl.ds(first, block), member * halo : (member + 1) * halo] = hit

    by_blocks(rows, body)


def store_outer(pieces, outer_ref):
    halo = outer_ref.shape[2]
    for member in range(3):
        outer_ref[member] = pieces[:, member * halo : (member + 1) * halo]


def store_rest(pieces, inner_ref, lat_inner_ref, lat_outer_ref):
    halo = inner_ref.shape[2]
    for member in range(3):
        inner_ref[member] = pieces[:, member * halo : (member + 1) * halo]
    lat_inner_ref[...] = pieces[:, 3 * halo : 4 * halo]
    lat_outer_ref[...] = pieces[:, 4 * halo : 5 * halo]


def start_kernel(pressure_hbm, list_hbm, cells_ref, stack_ref, outer_ref, matrix_ref, lists_ref, pressure_ref, sems):
    fetch([(list_hbm, lists_ref), (pressure_hbm, pressure_ref)], sems)
    levels = pressure_ref.shape[0]
    rows = cells_ref.shape[0]
    fill_sent(matrix_ref, lists_ref, OUTER_SENT)
    cells_ref[0:levels, :] = pressure_ref[:, 0, :]
    cells_ref[levels:rows, :] = jnp.zeros((rows - levels, cells_ref.shape[1]), f32)
    put_parts(stack_ref, cells_ref[...], 0)
    store_outer(gather_matmul(stack_ref, [matrix_ref[...]], rows), outer_ref)


def first_rest_kernel(stack_ref, list_ref, inner_ref, lat_inner_ref, lat_outer_ref, matrix_ref):
    fill_sent(matrix_ref, list_ref, REST_SENT)
    store_rest(gather_matmul(stack_ref, [matrix_ref[...]], inner_ref.shape[1]), inner_ref, lat_inner_ref, lat_outer_ref)


def rest_kernel(stack_ref, matrix_ref, inner_ref, lat_inner_ref, lat_outer_ref):
    store_rest(gather_matmul(stack_ref, [matrix_ref[...]], inner_ref.shape[1]), inner_ref, lat_inner_ref, lat_outer_ref)


def gradient_kernel(edge_cells_hbm, near_ref, far_ref, ends_ref, sems, *, cells, halo, lat_count):
    fetch([(edge_cells_hbm, ends_ref)], sems)
    edges = ends_ref.shape[1]
    edge_pad = near_ref.shape[1]
    ends = local_positions(ends_ref[...], cells, cells, halo, lat_count)
    near, far = ends[0:1, :], ends[1:2, :]
    same = near == far
    near, far = jnp.where(same, -1, near), jnp.where(same, -1, far)
    if edge_pad > edges:
        fill = jnp.full((1, edge_pad - edges), -1, jnp.int32)
        near, far = jnp.concatenate([near, fill], axis=1), jnp.concatenate([far, fill], axis=1)
    near, far = near.astype(i16), far.astype(i16)

    def fill_rows(matrix_ref, base):
        def body(first, block):
            row = row_numbers(first + base, block, edge_pad)
            one = jnp.ones((), bf16)
            matrix_ref[pl.ds(first, block), :] = jnp.where(row == far, one, jnp.where(row == near, -one, jnp.zeros((), bf16)))

        by_blocks(matrix_ref.shape[0], body)

    fill_rows(near_ref, 0)
    fill_rows(far_ref, near_ref.shape[0])


def edge_setup_kernel(velocity_hbm, list_hbm, dual_hbm, edges_ref, scale_ref, outer_matrix_ref, rest_matrix_ref, velocity_ref, list_ref, dual_ref, sems):
    fetch([(list_hbm, list_ref), (velocity_hbm, velocity_ref), (dual_hbm, dual_ref)], sems)
    levels, _, edges = velocity_ref.shape
    edges_ref[...] = jnp.zeros(edges_ref.shape, f32)
    edges_ref[0:levels, 0:edges] = velocity_ref[:, 0, :]
    scale_ref[...] = jnp.zeros(scale_ref.shape, f32)
    scale_ref[:, 0:edges] = STEP_SCALE * dual_ref[...]
    fill_sent(outer_matrix_ref, list_ref, OUTER_SENT)
    fill_sent(rest_matrix_ref, list_ref, REST_SENT)


def weight_kernel(
    sides_hbm, weight_hbm, near_high_ref, near_low_ref, far_high_ref, far_low_ref, sides_ref, weight_ref, sems, *, edges, edge_pad, halo, lat_count
):
    fetch([(sides_hbm, sides_ref), (weight_hbm, weight_ref)], sems)
    cells = sides_ref.shape[2]
    place = [local_positions(sides_ref[i], edges, edge_pad, halo, lat_count) for i in range(3)]
    weight = [weight_ref[i] for i in range(3)]
    for later in (1, 2):
        for earlier in range(later):
            same = place[later] == place[earlier]
            weight[earlier] = weight[earlier] + jnp.where(same, weight[later], 0.0)
            weight[later] = jnp.where(same, 0.0, weight[later])
            place[later] = jnp.where(same, -1, place[later])
    high = [value.astype(bf16) for value in weight]
    low = [(value - top.astype(f32)).astype(bf16) for value, top in zip(weight, high)]
    place = [value.astype(i16) for value in place]
    zero = jnp.zeros((), bf16)

    def fill_rows(high_ref, low_ref, base):
        def body(first, block):
            row = row_numbers(first + base, block, cells)
            hits = [row == value for value in place]
            for target, values in ((high_ref, high), (low_ref, low)):
                entry = jnp.where(hits[0], values[0], jnp.where(hits[1], values[1], jnp.where(hits[2], values[2], zero)))
                target[pl.ds(first, block), :] = entry

        by_blocks(high_ref.shape[0], body)

    fill_rows(near_high_ref, near_low_ref, 0)
    fill_rows(far_high_ref, far_low_ref, near_high_ref.shape[0])


def cell_setup_kernel(
    coupling_hbm, list_ref, speed_hbm, speed_ref, inverse_ref, forward_ref, back_ref, outer_matrix_ref, rest_matrix_ref, coupling_ref, column_ref, sems
):
    fetch([(coupling_hbm, coupling_ref), (speed_hbm, speed_ref)], sems)
    levels, _, cells = coupling_ref.shape
    for group in range(cells // LANES):
        column_ref[0:levels, group, :] = coupling_ref[:, 0, group * LANES : (group + 1) * LANES]
    above = column_ref[0]
    inverse = 1.0 / (1.0 + above)
    inverse_ref[0] = inverse
    ratio = above * inverse
    back_ref[0] = ratio
    for level in range(1, levels):
        below = above
        above = column_ref[level]
        inverse = 1.0 / (1.0 + below + above - below * ratio)
        inverse_ref[level] = inverse
        forward_ref[level] = below * inverse
        ratio = above * inverse
        back_ref[level] = ratio
    fill_sent(outer_matrix_ref, list_ref, OUTER_SENT)
    fill_sent(rest_matrix_ref, list_ref, REST_SENT)


def part_kernel(own_ref, inner_ref, outer_ref, *rest):
    *matrix_refs, total_ref, stack_ref = rest
    rows, width = own_ref.shape
    halo = inner_ref.shape[2]
    put_parts(stack_ref, own_ref[...], 0)
    put_parts(stack_ref, inner_ref[0], width)
    put_parts(stack_ref, outer_ref[0], width + halo)
    total_ref[...] = gather_matmul(stack_ref, [ref[...] for ref in matrix_refs], rows)


def lat_share(total_ref, lat_inner_ref, lat_outer_ref, matrix_refs, stack_ref):
    rows = total_ref.shape[0]
    halo = lat_inner_ref.shape[2]
    for member in range(3):
        put_parts(stack_ref, lat_inner_ref[member], member * halo)
        put_parts(stack_ref, lat_outer_ref[member], (3 + member) * halo)
    return total_ref[...] + gather_matmul(stack_ref, [ref[...] for ref in matrix_refs], rows)


def edge_kernel(total_ref, lat_inner_ref, lat_outer_ref, far_ref, edges_ref, scale_ref, matrix_ref, new_edges_ref, outer_ref, own_stack_ref, stack_ref):
    rows = edges_ref.shape[0]
    difference = lat_share(total_ref, lat_inner_ref, lat_outer_ref, [far_ref], stack_ref)
    new_edges = edges_ref[...] - scale_ref[...] * difference
    new_edges_ref[...] = new_edges
    put_parts(own_stack_ref, new_edges, 0)
    store_outer(gather_matmul(own_stack_ref, [matrix_ref[...]], rows), outer_ref)


def solve_columns(total_ref, lat_inner_ref, lat_outer_ref, high_ref, low_ref, cells_ref, speed_ref, inverse_ref, forward_ref, back_ref, levels, stack_ref, column_ref):
    rows, cells = cells_ref.shape
    divergence = lat_share(total_ref, lat_inner_ref, lat_outer_ref, [high_ref, low_ref], stack_ref)
    right_side = cells_ref[...] - speed_ref[...] * divergence
    for group in range(cells // LANES):
        column_ref[:, group, :] = right_side[:, group * LANES : (group + 1) * LANES]
    current = column_ref[0] * inverse_ref[0]
    scaled = [current]
    for level in range(1, levels):
        current = column_ref[level] * inverse_ref[level] + forward_ref[level] * current
        scaled.append(current)
    column_ref[levels - 1] = current
    for level in range(levels - 2, -1, -1):
        current = scaled[level] + back_ref[level] * current
        column_ref[level] = current
    for level in range(levels, rows):
        column_ref[level] = jnp.zeros_like(current)


def cell_kernel(
    total_ref,
    lat_inner_ref,
    lat_outer_ref,
    high_ref,
    low_ref,
    cells_ref,
    speed_ref,
    inverse_ref,
    forward_ref,
    back_ref,
    matrix_ref,
    new_cells_ref,
    outer_ref,
    own_stack_ref,
    stack_ref,
    column_ref,
    *,
    levels,
):
    rows, cells = cells_ref.shape
    solve_columns(total_ref, lat_inner_ref, lat_outer_ref, high_ref, low_ref, cells_ref, speed_ref, inverse_ref, forward_ref, back_ref, levels, stack_ref, column_ref)
    for group in range(cells // LANES):
        part = column_ref[:, group, :]
        new_cells_ref[:, group * LANES : (group + 1) * LANES] = part
        put_parts(own_stack_ref, part, group * LANES)
    store_outer(gather_matmul(own_stack_ref, [matrix_ref[...]], rows), outer_ref)


def last_kernel(
    total_ref, lat_inner_ref, lat_outer_ref, high_ref, low_ref, cells_ref, speed_ref, inverse_ref, forward_ref, back_ref, out_ref, stack_ref, column_ref, *, levels
):
    cells = cells_ref.shape[1]
    solve_columns(total_ref, lat_inner_ref, lat_outer_ref, high_ref, low_ref, cells_ref, speed_ref, inverse_ref, forward_ref, back_ref, levels, stack_ref, column_ref)
    for group in range(cells // LANES):
        out_ref[:, 0, group * LANES : (group + 1) * LANES] = column_ref[0:levels, group, :]


def call(body, outs, scratch, *operands, raw=(), copies=0):
    in_vmem = pl.BlockSpec(memory_space=pltpu.VMEM)
    in_hbm = pl.BlockSpec(memory_space=pltpu.HBM)
    scratch_shapes = [pltpu.VMEM(shape, kind) for shape, kind in scratch]
    if copies:
        scratch_shapes.append(pltpu.SemaphoreType.DMA((copies,)))
    return pl.pallas_call(
        body,
        out_shape=tuple(jax.ShapeDtypeStruct(shape, kind) for shape, kind in outs),
        in_specs=[in_hbm if i in raw else in_vmem for i in range(len(operands))],
        out_specs=tuple(in_vmem for _ in outs),
        scratch_shapes=scratch_shapes,
        compiler_params=pltpu.CompilerParams(vmem_limit_bytes=24 * 1024 * 1024),
    )(*operands)


def on_device(lat_count, lon_count, pressure, velocity, edge_cells, cell_edges, send_cells, send_edges, inv_dual, edge_weight, sound_speed, coupling):
    _, levels, cells = pressure.shape
    edges = velocity.shape[2]
    halo = send_cells.shape[2]
    rows = round_up(levels, 16)
    edge_pad = round_up(edges, 2 * LANES)
    bundle = ((3, rows, halo), f32)
    straight = ((rows, halo), f32)
    lon_routes = swap_routes(lon_count)
    lat_routes = swap_routes(lat_count)
    i32 = jnp.int32

    by_level = lambda value: value.transpose(1, 0, 2)
    stack_cells = ((PARTS * rows, cells), bf16)
    stack_edges = ((PARTS * rows, edge_pad), bf16)
    stack_lat = ((PARTS * rows, 6 * halo), bf16)
    column = ((rows, cells // LANES, LANES), f32)
    sent_outer = lambda width: ((width, 3 * halo), bf16)
    sent_rest = lambda width: ((width, 5 * halo), bf16)

    for phase in range(2 * NSUB):
        at_cells = phase % 2 == 0
        if phase == 0:
            values, stack, outer, cell_outer, cell_list = call(
                start_kernel,
                [((rows, cells), f32), stack_cells, bundle, sent_outer(cells), (send_cells.shape[1:], i32)],
                [((levels, 1, cells), f32)],
                by_level(pressure),
                send_cells[0],
                raw=(0, 1),
                copies=2,
            )
        outer_in = lax.ppermute(outer, "lon", lon_routes[1])
        if phase == 0:
            inner, lat_inner, lat_outer = call(first_rest_kernel, [bundle, straight, straight], [sent_rest(cells)], stack, cell_list)
        else:
            inner, lat_inner, lat_outer = call(rest_kernel, [bundle, straight, straight], [], stack, cell_rest if at_cells else edge_rest)
        inner_in = lax.ppermute(inner, "lon", lon_routes[0])
        if phase == 0:
            gradient_near, gradient_far = call(
                functools.partial(gradient_kernel, cells=cells, halo=halo, lat_count=lat_count),
                [((cells + 2 * halo, edge_pad), bf16), ((6 * halo, edge_pad), bf16)],
                [(edge_cells.shape[1:], i32)],
                edge_cells[0],
                raw=(0,),
                copies=1,
            )
        if phase == 1:
            near_high, near_low, far_high, far_low = call(
                functools.partial(weight_kernel, edges=edges, edge_pad=edge_pad, halo=halo, lat_count=lat_count),
                [((edge_pad + 2 * halo, cells), bf16)] * 2 + [((6 * halo, cells), bf16)] * 2,
                [((3, 1, cells), i32), ((3, 1, cells), f32)],
                by_level(cell_edges),
                by_level(edge_weight),
                raw=(0, 1),
                copies=2,
            )
        first = jnp.stack([inner_in[1], outer_in[1], lat_inner])
        second = jnp.stack([inner_in[2], outer_in[2], lat_outer])
        second_in = lax.ppermute(second, "lat", lat_routes[1])
        first_in = lax.ppermute(first, "lat", lat_routes[0])
        if phase == 0:
            normal, scale, edge_outer, edge_rest = call(
                edge_setup_kernel,
                [((rows, edge_pad), f32), ((1, edge_pad), f32), sent_outer(edge_pad), sent_rest(edge_pad)],
                [((levels, 1, edges), f32), (send_edges.shape[1:], i32), ((1, edges), f32)],
                by_level(velocity),
                send_edges[0],
                inv_dual,
                raw=(0, 1, 2),
                copies=3,
            )
        if phase == 1:
            speed, inverse, forward, back, cell_outer, cell_rest = call(
                cell_setup_kernel,
                [((1, cells), f32), column, column, column, sent_outer(cells), sent_rest(cells)],
                [((levels, 1, cells), f32), column],
                by_level(coupling),
                cell_list,
                sound_speed,
                raw=(0, 2),
                copies=2,
            )
        if at_cells:
            (total,) = call(
                part_kernel,
                [((rows, edge_pad), f32)],
                [((PARTS * rows, cells + 2 * halo), bf16)],
                values,
                inner_in,
                outer_in,
                gradient_near,
            )
            normal, outer, stack = call(
                edge_kernel,
                [((rows, edge_pad), f32), bundle, stack_edges],
                [stack_lat],
                total,
                first_in,
                second_in,
                gradient_far,
                normal,
                scale,
                edge_outer,
            )
        else:
            (total,) = call(
                part_kernel,
                [((rows, cells), f32)],
                [((PARTS * rows, edge_pad + 2 * halo), bf16)],
                normal,
                inner_in,
                outer_in,
                near_high,
                near_low,
            )
            operands = (total, first_in, second_in, far_high, far_low, values, speed, inverse, forward, back)
            if phase < 2 * NSUB - 1:
                values, outer, stack = call(
                    functools.partial(cell_kernel, levels=levels),
                    [((rows, cells), f32), bundle, stack_cells],
                    [stack_lat, column],
                    *operands,
                    cell_outer,
                )
            else:
                (values,) = call(functools.partial(last_kernel, levels=levels), [((levels, 1, cells), f32)], [stack_lat, column], *operands)
    return by_level(values), normal[:levels, :edges][None]


def solution(mesh):
    return jax.shard_map(
        functools.partial(on_device, mesh.shape["lat"], mesh.shape["lon"]),
        mesh=mesh,
        in_specs=(
            P("lat", None, "lon"),
            P("lat", None, "lon"),
            P("lat", None, "lon"),
            P("lat", None, "lon"),
            P("lat", None, "lon"),
            P("lat", None, "lon"),
            P("lat", "lon"),
            P("lat", None, "lon"),
            P("lat", "lon"),
            P("lat", None, "lon"),
        ),
        out_specs=(P("lat", None, "lon"), P("lat", None, "lon")),
        check_vma=False,
    )
```

```python
import functools

import jax
import jax.numpy as jnp
from jax import lax
from jax.experimental import pallas as pl
from jax.experimental.pallas import tpu as pltpu
from jax.sharding import PartitionSpec as P


NSUB = 3
STEP_SCALE = 0.5
LANES = 128
PARTS = 3

f32 = jnp.float32
bf16 = jnp.bfloat16
i16 = jnp.int16


def round_up(value, step):
    return -(-value // step) * step


def swap_routes(count):
    inner = [(i, i ^ 1) for i in range(count)]
    outer = [(i, (((i + 1) ^ 1) - 1) % count) for i in range(count)]
    return inner, outer


OUTER_SENT = ((0, 2), (1, 2), (2, 2))
REST_SENT = ((0, 1), (1, 1), (2, 1), (1, 0), (2, 0))


def link_signs():
    lat_inner = 1 - 2 * lax.rem(lax.axis_index("lat"), 2)
    lon_inner = 1 - 2 * lax.rem(lax.axis_index("lon"), 2)
    return lat_inner, lon_inner


def sent_row(member):
    lat_inner, lon_inner = link_signs()
    lat_link, lon_link = member
    p = (0, lat_inner, -lat_inner)[lat_link]
    q = (0, lon_inner, -lon_inner)[lon_link]
    flat = (p + 1) * 3 + (q + 1)
    return flat - jnp.where(flat > 4, 1, 0)


def local_positions(index, own, own_padded, halo, lat_count):
    lat_inner, lon_inner = link_signs()
    a = lax.axis_index("lat")
    beyond = index - own
    piece = lax.div(jnp.maximum(beyond, 0), halo)
    slot = beyond - piece * halo
    flat = piece + jnp.where(piece >= 4, 1, 0)
    p = jnp.where(flat >= 6, 1, jnp.where(flat >= 3, 0, -1))
    q = flat - 3 * (p + 1) - 1
    lon_member = jnp.where(q == 0, 2, jnp.where(q == lon_inner, 0, 1))
    member = jnp.where(p == 0, lon_member, jnp.where(p == lat_inner, 2, 5) + lon_member)
    outside = (a + p < 0) | (a + p >= lat_count)
    row = own_padded + member * halo + slot
    return jnp.where(beyond < 0, index, jnp.where(outside, -1, row))


def put_parts(stack_ref, value, start):
    rows, width = value.shape
    rest = value
    for part in range(PARTS):
        piece = rest.astype(bf16)
        stack_ref[part * rows : (part + 1) * rows, start : start + width] = piece
        if part < PARTS - 1:
            rest = rest - piece.astype(f32)


def sum_parts(product, rows):
    total = product[(PARTS - 1) * rows : PARTS * rows]
    for part in range(PARTS - 2, -1, -1):
        total = total + product[part * rows : (part + 1) * rows]
    return total


def gather_matmul(stack_ref, matrices, rows):
    product = None
    for matrix in matrices:
        term = jnp.dot(stack_ref[...], matrix, preferred_element_type=f32)
        product = term if product is None else product + term
    return sum_parts(product, rows)


def start_fetch(pairs, sems):
    copies = [pltpu.make_async_copy(source, target, sems.at[i]) for i, (source, target) in enumerate(pairs)]
    for copy in copies:
        copy.start()
    return copies


def fetch(pairs, sems):
    for copy in start_fetch(pairs, sems):
        copy.wait()


def by_blocks(rows, body):
    block = 64 if rows % 64 == 0 else 16

    def step(i, carry):
        first = pl.multiple_of(i * block, block)
        body(first, block)
        return carry

    lax.fori_loop(0, rows // block, step, 0)


def row_numbers(first, block, width):
    return (lax.broadcasted_iota(jnp.int32, (block, width), 0) + first).astype(i16)


def fill_sent(matrix_ref, list_ref, members):
    rows = matrix_ref.shape[0]
    halo = list_ref.shape[1]
    lanes = [list_ref[pl.ds(sent_row(member), 1), :].astype(i16) for member in members]

    def body(first, block):
        row = row_numbers(first, block, halo)
        for member, index in enumerate(lanes):
            hit = jnp.where(row == index, jnp.ones((), bf16), jnp.zeros((), bf16))
            matrix_ref[pl.ds(first, block), member * halo : (member + 1) * halo] = hit

    by_blocks(rows, body)


def store_outer(pieces, outer_ref):
    halo = outer_ref.shape[2]
    for member in range(3):
        outer_ref[member] = pieces[:, member * halo : (member + 1) * halo]


def store_rest(pieces, inner_ref, lat_inner_ref, lat_outer_ref):
    halo = inner_ref.shape[2]
    for member in range(3):
        inner_ref[member] = pieces[:, member * halo : (member + 1) * halo]
    lat_inner_ref[...] = pieces[:, 3 * halo : 4 * halo]
    lat_outer_ref[...] = pieces[:, 4 * halo : 5 * halo]


def start_kernel(pressure_hbm, list_hbm, cells_ref, stack_ref, outer_ref, lists_ref, pressure_ref, matrix_ref, sems):
    lists, pressure = start_fetch([(list_hbm, lists_ref), (pressure_hbm, pressure_ref)], sems)
    levels = pressure_ref.shape[0]
    rows = cells_ref.shape[0]
    lists.wait()
    fill_sent(matrix_ref, lists_ref, OUTER_SENT)
    pressure.wait()
    cells_ref[0:levels, :] = pressure_ref[:, 0, :]
    cells_ref[levels:rows, :] = jnp.zeros((rows - levels, cells_ref.shape[1]), f32)
    put_parts(stack_ref, cells_ref[...], 0)
    store_outer(gather_matmul(stack_ref, [matrix_ref[...]], rows), outer_ref)


def first_rest_kernel(stack_ref, list_ref, inner_ref, lat_inner_ref, lat_outer_ref, matrix_ref):
    fill_sent(matrix_ref, list_ref, REST_SENT)
    store_rest(gather_matmul(stack_ref, [matrix_ref[...]], inner_ref.shape[1]), inner_ref, lat_inner_ref, lat_outer_ref)


def rest_kernel(stack_ref, matrix_ref, inner_ref, lat_inner_ref, lat_outer_ref):
    store_rest(gather_matmul(stack_ref, [matrix_ref[...]], inner_ref.shape[1]), inner_ref, lat_inner_ref, lat_outer_ref)


def gradient_kernel(edge_cells_hbm, near_ref, far_ref, ends_ref, sems, *, cells, halo, lat_count):
    fetch([(edge_cells_hbm, ends_ref)], sems)
    edges = ends_ref.shape[1]
    edge_pad = near_ref.shape[1]
    ends = local_positions(ends_ref[...], cells, cells, halo, lat_count)
    near, far = ends[0:1, :], ends[1:2, :]
    same = near == far
    near, far = jnp.where(same, -1, near), jnp.where(same, -1, far)
    if edge_pad > edges:
        fill = jnp.full((1, edge_pad - edges), -1, jnp.int32)
        near, far = jnp.concatenate([near, fill], axis=1), jnp.concatenate([far, fill], axis=1)
    near, far = near.astype(i16), far.astype(i16)

    def fill_rows(matrix_ref, base):
        def body(first, block):
            row = row_numbers(first + base, block, edge_pad)
            one = jnp.ones((), bf16)
            matrix_ref[pl.ds(first, block), :] = jnp.where(row == far, one, jnp.where(row == near, -one, jnp.zeros((), bf16)))

        by_blocks(matrix_ref.shape[0], body)

    fill_rows(near_ref, 0)
    fill_rows(far_ref, near_ref.shape[0])


def edge_setup_kernel(velocity_hbm, list_hbm, dual_hbm, edges_ref, scale_ref, outer_matrix_ref, rest_matrix_ref, velocity_ref, list_ref, dual_ref, sems):
    lists, velocity, dual = start_fetch([(list_hbm, list_ref), (velocity_hbm, velocity_ref), (dual_hbm, dual_ref)], sems)
    levels, _, edges = velocity_ref.shape
    edges_ref[...] = jnp.zeros(edges_ref.shape, f32)
    scale_ref[...] = jnp.zeros(scale_ref.shape, f32)
    lists.wait()
    fill_sent(outer_matrix_ref, list_ref, OUTER_SENT)
    fill_sent(rest_matrix_ref, list_ref, REST_SENT)
    velocity.wait()
    dual.wait()
    edges_ref[0:levels, 0:edges] = velocity_ref[:, 0, :]
    scale_ref[:, 0:edges] = STEP_SCALE * dual_ref[...]


def weight_kernel(
    sides_hbm, weight_hbm, near_high_ref, near_low_ref, far_high_ref, far_low_ref, sides_ref, weight_ref, sems, *, edges, edge_pad, halo, lat_count
):
    fetch([(sides_hbm, sides_ref), (weight_hbm, weight_ref)], sems)
    cells = sides_ref.shape[2]
    place = [local_positions(sides_ref[i], edges, edge_pad, halo, lat_count) for i in range(3)]
    weight = [weight_ref[i] for i in range(3)]
    for later in (1, 2):
        for earlier in range(later):
            same = place[later] == place[earlier]
            weight[earlier] = weight[earlier] + jnp.where(same, weight[later], 0.0)
            weight[later] = jnp.where(same, 0.0, weight[later])
            place[later] = jnp.where(same, -1, place[later])
    high = [value.astype(bf16) for value in weight]
    low = [(value - top.astype(f32)).astype(bf16) for value, top in zip(weight, high)]
    place = [value.astype(i16) for value in place]
    zero = jnp.zeros((), bf16)

    def fill_rows(high_ref, low_ref, base):
        def body(first, block):
            row = row_numbers(first + base, block, cells)
            hits = [row == value for value in place]
            for target, values in ((high_ref, high), (low_ref, low)):
                entry = jnp.where(hits[0], values[0], jnp.where(hits[1], values[1], jnp.where(hits[2], values[2], zero)))
                target[pl.ds(first, block), :] = entry

        by_blocks(high_ref.shape[0], body)

    fill_rows(near_high_ref, near_low_ref, 0)
    fill_rows(far_high_ref, far_low_ref, near_high_ref.shape[0])


def cell_setup_kernel(
    coupling_hbm, list_ref, speed_hbm, speed_ref, inverse_ref, forward_ref, back_ref, outer_matrix_ref, rest_matrix_ref, coupling_ref, column_ref, sems
):
    coupling, speed = start_fetch([(coupling_hbm, coupling_ref), (speed_hbm, speed_ref)], sems)
    levels, _, cells = coupling_ref.shape
    fill_sent(outer_matrix_ref, list_ref, OUTER_SENT)
    fill_sent(rest_matrix_ref, list_ref, REST_SENT)
    coupling.wait()
    speed.wait()
    for group in range(cells // LANES):
        column_ref[0:levels, group, :] = coupling_ref[:, 0, group * LANES : (group + 1) * LANES]
    above = column_ref[0]
    inverse = 1.0 / (1.0 + above)
    inverse_ref[0] = inverse
    ratio = above * inverse
    back_ref[0] = ratio
    for level in range(1, levels):
        below = above
        above = column_ref[level]
        inverse = 1.0 / (1.0 + below + above - below * ratio)
        inverse_ref[level] = inverse
        forward_ref[level] = below * inverse
        ratio = above * inverse
        back_ref[level] = ratio


def part_kernel(own_ref, inner_ref, outer_ref, *rest):
    *matrix_refs, total_ref, stack_ref = rest
    rows, width = own_ref.shape
    halo = inner_ref.shape[2]
    put_parts(stack_ref, own_ref[...], 0)
    put_parts(stack_ref, inner_ref[0], width)
    put_parts(stack_ref, outer_ref[0], width + halo)
    total_ref[...] = gather_matmul(stack_ref, [ref[...] for ref in matrix_refs], rows)


def lat_share(total_ref, lat_inner_ref, lat_outer_ref, matrix_refs, stack_ref):
    rows = total_ref.shape[0]
    halo = lat_inner_ref.shape[2]
    for member in range(3):
        put_parts(stack_ref, lat_inner_ref[member], member * halo)
        put_parts(stack_ref, lat_outer_ref[member], (3 + member) * halo)
    return total_ref[...] + gather_matmul(stack_ref, [ref[...] for ref in matrix_refs], rows)


def edge_kernel(total_ref, lat_inner_ref, lat_outer_ref, far_ref, edges_ref, scale_ref, matrix_ref, new_edges_ref, outer_ref, own_stack_ref, stack_ref):
    rows = edges_ref.shape[0]
    difference = lat_share(total_ref, lat_inner_ref, lat_outer_ref, [far_ref], stack_ref)
    new_edges = edges_ref[...] - scale_ref[...] * difference
    new_edges_ref[...] = new_edges
    put_parts(own_stack_ref, new_edges, 0)
    store_outer(gather_matmul(own_stack_ref, [matrix_ref[...]], rows), outer_ref)


def solve_columns(total_ref, lat_inner_ref, lat_outer_ref, high_ref, low_ref, cells_ref, speed_ref, inverse_ref, forward_ref, back_ref, levels, stack_ref, column_ref):
    rows, cells = cells_ref.shape
    divergence = lat_share(total_ref, lat_inner_ref, lat_outer_ref, [high_ref, low_ref], stack_ref)
    right_side = cells_ref[...] - speed_ref[...] * divergence
    for group in range(cells // LANES):
        column_ref[:, group, :] = right_side[:, group * LANES : (group + 1) * LANES]
    current = column_ref[0] * inverse_ref[0]
    scaled = [current]
    for level in range(1, levels):
        current = column_ref[level] * inverse_ref[level] + forward_ref[level] * current
        scaled.append(current)
    column_ref[levels - 1] = current
    for level in range(levels - 2, -1, -1):
        current = scaled[level] + back_ref[level] * current
        column_ref[level] = current
    for level in range(levels, rows):
        column_ref[level] = jnp.zeros_like(current)


def cell_kernel(
    total_ref,
    lat_inner_ref,
    lat_outer_ref,
    high_ref,
    low_ref,
    cells_ref,
    speed_ref,
    inverse_ref,
    forward_ref,
    back_ref,
    matrix_ref,
    new_cells_ref,
    outer_ref,
    own_stack_ref,
    stack_ref,
    column_ref,
    *,
    levels,
):
    rows, cells = cells_ref.shape
    solve_columns(total_ref, lat_inner_ref, lat_outer_ref, high_ref, low_ref, cells_ref, speed_ref, inverse_ref, forward_ref, back_ref, levels, stack_ref, column_ref)
    for group in range(cells // LANES):
        part = column_ref[:, group, :]
        new_cells_ref[:, group * LANES : (group + 1) * LANES] = part
        put_parts(own_stack_ref, part, group * LANES)
    store_outer(gather_matmul(own_stack_ref, [matrix_ref[...]], rows), outer_ref)


def last_kernel(
    total_ref, lat_inner_ref, lat_outer_ref, high_ref, low_ref, cells_ref, speed_ref, inverse_ref, forward_ref, back_ref, out_ref, stack_ref, column_ref, *, levels
):
    cells = cells_ref.shape[1]
    solve_columns(total_ref, lat_inner_ref, lat_outer_ref, high_ref, low_ref, cells_ref, speed_ref, inverse_ref, forward_ref, back_ref, levels, stack_ref, column_ref)
    for group in range(cells // LANES):
        out_ref[:, 0, group * LANES : (group + 1) * LANES] = column_ref[0:levels, group, :]


def call(body, outs, scratch, *operands, raw=(), copies=0):
    in_vmem = pl.BlockSpec(memory_space=pltpu.VMEM)
    in_hbm = pl.BlockSpec(memory_space=pltpu.HBM)
    scratch_shapes = [pltpu.VMEM(shape, kind) for shape, kind in scratch]
    if copies:
        scratch_shapes.append(pltpu.SemaphoreType.DMA((copies,)))
    operands = [pltpu.with_memory_space_constraint(x, pltpu.HBM) if i in raw else x for i, x in enumerate(operands)]
    return pl.pallas_call(
        body,
        out_shape=tuple(jax.ShapeDtypeStruct(shape, kind) for shape, kind in outs),
        in_specs=[in_hbm if i in raw else in_vmem for i in range(len(operands))],
        out_specs=tuple(in_vmem for _ in outs),
        scratch_shapes=scratch_shapes,
        compiler_params=pltpu.CompilerParams(vmem_limit_bytes=24 * 1024 * 1024),
    )(*operands)


def on_device(lat_count, lon_count, pressure, velocity, edge_cells, cell_edges, send_cells, send_edges, inv_dual, edge_weight, sound_speed, coupling):
    _, levels, cells = pressure.shape
    edges = velocity.shape[2]
    halo = send_cells.shape[2]
    rows = round_up(levels, 16)
    edge_pad = round_up(edges, 2 * LANES)
    bundle = ((3, rows, halo), f32)
    straight = ((rows, halo), f32)
    lon_routes = swap_routes(lon_count)
    lat_routes = swap_routes(lat_count)
    i32 = jnp.int32

    by_level = lambda value: value.transpose(1, 0, 2)
    stack_cells = ((PARTS * rows, cells), bf16)
    stack_edges = ((PARTS * rows, edge_pad), bf16)
    stack_lat = ((PARTS * rows, 6 * halo), bf16)
    column = ((rows, cells // LANES, LANES), f32)
    sent_outer = lambda width: ((width, 3 * halo), bf16)
    sent_rest = lambda width: ((width, 5 * halo), bf16)

    for phase in range(2 * NSUB):
        at_cells = phase % 2 == 0
        if phase == 0:
            values, stack, outer, cell_list = call(
                start_kernel,
                [((rows, cells), f32), stack_cells, bundle, (send_cells.shape[1:], i32)],
                [((levels, 1, cells), f32), sent_outer(cells)],
                by_level(pressure),
                send_cells[0],
                raw=(0, 1),
                copies=2,
            )
        outer_in = lax.ppermute(outer, "lon", lon_routes[1])
        if phase == 0:
            inner, lat_inner, lat_outer = call(first_rest_kernel, [bundle, straight, straight], [sent_rest(cells)], stack, cell_list)
        else:
            inner, lat_inner, lat_outer = call(rest_kernel, [bundle, straight, straight], [], stack, cell_rest if at_cells else edge_rest)
        inner_in = lax.ppermute(inner, "lon", lon_routes[0])
        if phase == 0:
            gradient_near, gradient_far = call(
                functools.partial(gradient_kernel, cells=cells, halo=halo, lat_count=lat_count),
                [((cells + 2 * halo, edge_pad), bf16), ((6 * halo, edge_pad), bf16)],
                [(edge_cells.shape[1:], i32)],
                edge_cells[0],
                raw=(0,),
                copies=1,
            )
        if phase == 1:
            near_high, near_low, far_high, far_low = call(
                functools.partial(weight_kernel, edges=edges, edge_pad=edge_pad, halo=halo, lat_count=lat_count),
                [((edge_pad + 2 * halo, cells), bf16)] * 2 + [((6 * halo, cells), bf16)] * 2,
                [((3, 1, cells), i32), ((3, 1, cells), f32)],
                by_level(cell_edges),
                by_level(edge_weight),
                raw=(0, 1),
                copies=2,
            )
        first = jnp.stack([inner_in[1], outer_in[1], lat_inner])
        second = jnp.stack([inner_in[2], outer_in[2], lat_outer])
        second_in = lax.ppermute(second, "lat", lat_routes[1])
        first_in = lax.ppermute(first, "lat", lat_routes[0])
        if phase == 0:
            normal, scale, edge_outer, edge_rest = call(
                edge_setup_kernel,
                [((rows, edge_pad), f32), ((1, edge_pad), f32), sent_outer(edge_pad), sent_rest(edge_pad)],
                [((levels, 1, edges), f32), (send_edges.shape[1:], i32), ((1, edges), f32)],
                by_level(velocity),
                send_edges[0],
                inv_dual,
                raw=(0, 1, 2),
                copies=3,
            )
        if phase == 1:
            speed, inverse, forward, back, cell_outer, cell_rest = call(
                cell_setup_kernel,
                [((1, cells), f32), column, column, column, sent_outer(cells), sent_rest(cells)],
                [((levels, 1, cells), f32), column],
                by_level(coupling),
                cell_list,
                sound_speed,
                raw=(0, 2),
                copies=2,
            )
        if at_cells:
            (total,) = call(
                part_kernel,
                [((rows, edge_pad), f32)],
                [((PARTS * rows, cells + 2 * halo), bf16)],
                values,
                inner_in,
                outer_in,
                gradient_near,
            )
            normal, outer, stack = call(
                edge_kernel,
                [((rows, edge_pad), f32), bundle, stack_edges],
                [stack_lat],
                total,
                first_in,
                second_in,
                gradient_far,
                normal,
                scale,
                edge_outer,
            )
        else:
            (total,) = call(
                part_kernel,
                [((rows, cells), f32)],
                [((PARTS * rows, edge_pad + 2 * halo), bf16)],
                normal,
                inner_in,
                outer_in,
                near_high,
                near_low,
            )
            operands = (total, first_in, second_in, far_high, far_low, values, speed, inverse, forward, back)
            if phase < 2 * NSUB - 1:
                values, outer, stack = call(
                    functools.partial(cell_kernel, levels=levels),
                    [((rows, cells), f32), bundle, stack_cells],
                    [stack_lat, column],
                    *operands,
                    cell_outer,
                )
            else:
                (values,) = call(functools.partial(last_kernel, levels=levels), [((levels, 1, cells), f32)], [stack_lat, column], *operands)
    return by_level(values), normal[:levels, :edges][None]


def solution(mesh):
    return jax.shard_map(
        functools.partial(on_device, mesh.shape["lat"], mesh.shape["lon"]),
        mesh=mesh,
        in_specs=(
            P("lat", None, "lon"),
            P("lat", None, "lon"),
            P("lat", None, "lon"),
            P("lat", None, "lon"),
            P("lat", None, "lon"),
            P("lat", None, "lon"),
            P("lat", "lon"),
            P("lat", None, "lon"),
            P("lat", "lon"),
            P("lat", None, "lon"),
        ),
        out_specs=(P("lat", None, "lon"), P("lat", None, "lon")),
        check_vma=False,
    )
```

```python
import functools

import jax
import jax.numpy as jnp
from jax import lax
from jax.experimental import pallas as pl
from jax.experimental.pallas import tpu as pltpu
from jax.sharding import PartitionSpec as P


NSUB = 3
STEP_SCALE = 0.5
LANES = 128
PARTS = 3

f32 = jnp.float32
bf16 = jnp.bfloat16
i16 = jnp.int16


def round_up(value, step):
    return -(-value // step) * step


def swap_routes(count):
    inner = [(i, i ^ 1) for i in range(count)]
    outer = [(i, (((i + 1) ^ 1) - 1) % count) for i in range(count)]
    return inner, outer


def lat_outer_routes(lat_count, lon_count):
    routes = []
    for a, target in swap_routes(lat_count)[1]:
        for b in range(lon_count):
            alone = a in (0, lat_count - 1)
            routes.append((a * lon_count + b, a * lon_count + (b ^ 1) if alone else target * lon_count + b))
    return routes


OUTER_SENT = ((0, 2), (1, 2), (2, 2))
REST_SENT = ((0, 1), (1, 1), (2, 1), (1, 0), (2, 0))


def link_signs():
    lat_inner = 1 - 2 * lax.rem(lax.axis_index("lat"), 2)
    lon_inner = 1 - 2 * lax.rem(lax.axis_index("lon"), 2)
    return lat_inner, lon_inner


def sent_row(member):
    lat_inner, lon_inner = link_signs()
    lat_link, lon_link = member
    p = (0, lat_inner, -lat_inner)[lat_link]
    q = (0, lon_inner, -lon_inner)[lon_link]
    flat = (p + 1) * 3 + (q + 1)
    return flat - jnp.where(flat > 4, 1, 0)


def local_positions(index, own, own_padded, halo, lat_count):
    lat_inner, lon_inner = link_signs()
    a = lax.axis_index("lat")
    beyond = index - own
    piece = lax.div(jnp.maximum(beyond, 0), halo)
    slot = beyond - piece * halo
    flat = piece + jnp.where(piece >= 4, 1, 0)
    p = jnp.where(flat >= 6, 1, jnp.where(flat >= 3, 0, -1))
    q = flat - 3 * (p + 1) - 1
    lon_member = jnp.where(q == 0, 2, jnp.where(q == lon_inner, 0, 1))
    member = jnp.where(p == 0, lon_member, jnp.where(p == lat_inner, 2, 5) + lon_member)
    outside = (a + p < 0) | (a + p >= lat_count)
    row = own_padded + member * halo + slot
    return jnp.where(beyond < 0, index, jnp.where(outside, -1, row))


def put_parts(stack_ref, value, start):
    rows, width = value.shape
    rest = value
    for part in range(PARTS):
        piece = rest.astype(bf16)
        stack_ref[part * rows : (part + 1) * rows, start : start + width] = piece
        if part < PARTS - 1:
            rest = rest - piece.astype(f32)


def sum_parts(product, rows):
    total = product[(PARTS - 1) * rows : PARTS * rows]
    for part in range(PARTS - 2, -1, -1):
        total = total + product[part * rows : (part + 1) * rows]
    return total


def gather_matmul(stack_ref, matrices, rows):
    product = None
    for matrix in matrices:
        term = jnp.dot(stack_ref[...], matrix, preferred_element_type=f32)
        product = term if product is None else product + term
    return sum_parts(product, rows)


def start_fetch(pairs, sems):
    copies = [pltpu.make_async_copy(source, target, sems.at[i]) for i, (source, target) in enumerate(pairs)]
    for copy in copies:
        copy.start()
    return copies


def fetch(pairs, sems):
    for copy in start_fetch(pairs, sems):
        copy.wait()


def by_blocks(rows, body):
    block = 64 if rows % 64 == 0 else 16

    def step(i, carry):
        first = pl.multiple_of(i * block, block)
        body(first, block)
        return carry

    lax.fori_loop(0, rows // block, step, 0)


def row_numbers(first, block, width):
    return (lax.broadcasted_iota(jnp.int32, (block, width), 0) + first).astype(i16)


def fill_sent(matrix_ref, list_ref, members):
    rows = matrix_ref.shape[0]
    halo = list_ref.shape[1]
    lanes = [list_ref[pl.ds(sent_row(member), 1), :].astype(i16) for member in members]

    def body(first, block):
        row = row_numbers(first, block, halo)
        for member, index in enumerate(lanes):
            hit = jnp.where(row == index, jnp.ones((), bf16), jnp.zeros((), bf16))
            matrix_ref[pl.ds(first, block), member * halo : (member + 1) * halo] = hit

    by_blocks(rows, body)


def store_outer(pieces, outer_ref):
    halo = outer_ref.shape[2]
    for member in range(3):
        outer_ref[member] = pieces[:, member * halo : (member + 1) * halo]


def store_rest(pieces, inner_ref, lat_inner_ref, lat_outer_ref):
    halo = inner_ref.shape[2]
    for member in range(3):
        inner_ref[member] = pieces[:, member * halo : (member + 1) * halo]
    lat_inner_ref[...] = pieces[:, 3 * halo : 4 * halo]
    lat_outer_ref[...] = pieces[:, 4 * halo : 5 * halo]


def start_kernel(pressure_hbm, list_hbm, cells_ref, stack_ref, outer_ref, lists_ref, pressure_ref, matrix_ref, sems):
    lists, pressure = start_fetch([(list_hbm, lists_ref), (pressure_hbm, pressure_ref)], sems)
    levels = pressure_ref.shape[0]
    rows = cells_ref.shape[0]
    lists.wait()
    fill_sent(matrix_ref, lists_ref, OUTER_SENT)
    pressure.wait()
    cells_ref[0:levels, :] = pressure_ref[:, 0, :]
    cells_ref[levels:rows, :] = jnp.zeros((rows - levels, cells_ref.shape[1]), f32)
    put_parts(stack_ref, cells_ref[...], 0)
    store_outer(gather_matmul(stack_ref, [matrix_ref[...]], rows), outer_ref)


def first_rest_kernel(stack_ref, list_ref, inner_ref, lat_inner_ref, lat_outer_ref, matrix_ref):
    fill_sent(matrix_ref, list_ref, REST_SENT)
    store_rest(gather_matmul(stack_ref, [matrix_ref[...]], inner_ref.shape[1]), inner_ref, lat_inner_ref, lat_outer_ref)


def rest_kernel(stack_ref, matrix_ref, inner_ref, lat_inner_ref, lat_outer_ref):
    store_rest(gather_matmul(stack_ref, [matrix_ref[...]], inner_ref.shape[1]), inner_ref, lat_inner_ref, lat_outer_ref)


def gradient_kernel(edge_cells_hbm, near_ref, far_ref, ends_ref, sems, *, cells, halo, lat_count):
    fetch([(edge_cells_hbm, ends_ref)], sems)
    edges = ends_ref.shape[1]
    edge_pad = near_ref.shape[1]
    ends = local_positions(ends_ref[...], cells, cells, halo, lat_count)
    near, far = ends[0:1, :], ends[1:2, :]
    same = near == far
    near, far = jnp.where(same, -1, near), jnp.where(same, -1, far)
    if edge_pad > edges:
        fill = jnp.full((1, edge_pad - edges), -1, jnp.int32)
        near, far = jnp.concatenate([near, fill], axis=1), jnp.concatenate([far, fill], axis=1)
    near, far = near.astype(i16), far.astype(i16)

    def fill_rows(matrix_ref, base):
        def body(first, block):
            row = row_numbers(first + base, block, edge_pad)
            one = jnp.ones((), bf16)
            matrix_ref[pl.ds(first, block), :] = jnp.where(row == far, one, jnp.where(row == near, -one, jnp.zeros((), bf16)))

        by_blocks(matrix_ref.shape[0], body)

    fill_rows(near_ref, 0)
    fill_rows(far_ref, near_ref.shape[0])


def edge_setup_kernel(velocity_hbm, list_hbm, dual_hbm, edges_ref, scale_ref, outer_matrix_ref, rest_matrix_ref, velocity_ref, list_ref, dual_ref, sems):
    lists, velocity, dual = start_fetch([(list_hbm, list_ref), (velocity_hbm, velocity_ref), (dual_hbm, dual_ref)], sems)
    levels, _, edges = velocity_ref.shape
    edges_ref[...] = jnp.zeros(edges_ref.shape, f32)
    scale_ref[...] = jnp.zeros(scale_ref.shape, f32)
    lists.wait()
    fill_sent(outer_matrix_ref, list_ref, OUTER_SENT)
    fill_sent(rest_matrix_ref, list_ref, REST_SENT)
    velocity.wait()
    dual.wait()
    edges_ref[0:levels, 0:edges] = velocity_ref[:, 0, :]
    scale_ref[:, 0:edges] = STEP_SCALE * dual_ref[...]


def weight_kernel(
    sides_hbm, weight_hbm, near_high_ref, near_low_ref, far_high_ref, far_low_ref, sides_ref, weight_ref, sems, *, edges, edge_pad, halo, lat_count
):
    fetch([(sides_hbm, sides_ref), (weight_hbm, weight_ref)], sems)
    cells = sides_ref.shape[2]
    place = [local_positions(sides_ref[i], edges, edge_pad, halo, lat_count) for i in range(3)]
    weight = [weight_ref[i] for i in range(3)]
    for later in (1, 2):
        for earlier in range(later):
            same = place[later] == place[earlier]
            weight[earlier] = weight[earlier] + jnp.where(same, weight[later], 0.0)
            weight[later] = jnp.where(same, 0.0, weight[later])
            place[later] = jnp.where(same, -1, place[later])
    high = [value.astype(bf16) for value in weight]
    low = [(value - top.astype(f32)).astype(bf16) for value, top in zip(weight, high)]
    place = [value.astype(i16) for value in place]
    zero = jnp.zeros((), bf16)

    def fill_rows(high_ref, low_ref, base):
        def body(first, block):
            row = row_numbers(first + base, block, cells)
            hits = [row == value for value in place]
            for target, values in ((high_ref, high), (low_ref, low)):
                entry = jnp.where(hits[0], values[0], jnp.where(hits[1], values[1], jnp.where(hits[2], values[2], zero)))
                target[pl.ds(first, block), :] = entry

        by_blocks(high_ref.shape[0], body)

    fill_rows(near_high_ref, near_low_ref, 0)
    fill_rows(far_high_ref, far_low_ref, near_high_ref.shape[0])


def cell_setup_kernel(
    coupling_hbm, list_ref, speed_hbm, speed_ref, inverse_ref, forward_ref, back_ref, outer_matrix_ref, rest_matrix_ref, coupling_ref, column_ref, sems
):
    coupling, speed = start_fetch([(coupling_hbm, coupling_ref), (speed_hbm, speed_ref)], sems)
    levels, _, cells = coupling_ref.shape
    fill_sent(outer_matrix_ref, list_ref, OUTER_SENT)
    fill_sent(rest_matrix_ref, list_ref, REST_SENT)
    coupling.wait()
    speed.wait()
    for group in range(cells // LANES):
        column_ref[0:levels, group, :] = coupling_ref[:, 0, group * LANES : (group + 1) * LANES]
    above = column_ref[0]
    inverse = 1.0 / (1.0 + above)
    inverse_ref[0] = inverse
    ratio = above * inverse
    back_ref[0] = ratio
    for level in range(1, levels):
        below = above
        above = column_ref[level]
        inverse = 1.0 / (1.0 + below + above - below * ratio)
        inverse_ref[level] = inverse
        forward_ref[level] = below * inverse
        ratio = above * inverse
        back_ref[level] = ratio


def part_kernel(own_ref, inner_ref, outer_ref, *rest):
    *matrix_refs, total_ref, stack_ref = rest
    rows, width = own_ref.shape
    halo = inner_ref.shape[2]
    put_parts(stack_ref, own_ref[...], 0)
    put_parts(stack_ref, inner_ref[0], width)
    put_parts(stack_ref, outer_ref[0], width + halo)
    total_ref[...] = gather_matmul(stack_ref, [ref[...] for ref in matrix_refs], rows)


def lat_share(total_ref, lat_inner_ref, lat_outer_ref, matrix_refs, stack_ref):
    rows = total_ref.shape[0]
    halo = lat_inner_ref.shape[2]
    for member in range(3):
        put_parts(stack_ref, lat_inner_ref[member], member * halo)
        put_parts(stack_ref, lat_outer_ref[member], (3 + member) * halo)
    return total_ref[...] + gather_matmul(stack_ref, [ref[...] for ref in matrix_refs], rows)


def edge_kernel(total_ref, lat_inner_ref, lat_outer_ref, far_ref, edges_ref, scale_ref, matrix_ref, new_edges_ref, outer_ref, own_stack_ref, stack_ref):
    rows = edges_ref.shape[0]
    difference = lat_share(total_ref, lat_inner_ref, lat_outer_ref, [far_ref], stack_ref)
    new_edges = edges_ref[...] - scale_ref[...] * difference
    new_edges_ref[...] = new_edges
    put_parts(own_stack_ref, new_edges, 0)
    store_outer(gather_matmul(own_stack_ref, [matrix_ref[...]], rows), outer_ref)


def solve_columns(total_ref, lat_inner_ref, lat_outer_ref, high_ref, low_ref, cells_ref, speed_ref, inverse_ref, forward_ref, back_ref, levels, stack_ref, column_ref):
    rows, cells = cells_ref.shape
    divergence = lat_share(total_ref, lat_inner_ref, lat_outer_ref, [high_ref, low_ref], stack_ref)
    right_side = cells_ref[...] - speed_ref[...] * divergence
    for group in range(cells // LANES):
        column_ref[:, group, :] = right_side[:, group * LANES : (group + 1) * LANES]
    current = column_ref[0] * inverse_ref[0]
    scaled = [current]
    for level in range(1, levels):
        current = column_ref[level] * inverse_ref[level] + forward_ref[level] * current
        scaled.append(current)
    column_ref[levels - 1] = current
    for level in range(levels - 2, -1, -1):
        current = scaled[level] + back_ref[level] * current
        column_ref[level] = current
    for level in range(levels, rows):
        column_ref[level] = jnp.zeros_like(current)


def cell_kernel(
    total_ref,
    lat_inner_ref,
    lat_outer_ref,
    high_ref,
    low_ref,
    cells_ref,
    speed_ref,
    inverse_ref,
    forward_ref,
    back_ref,
    matrix_ref,
    new_cells_ref,
    outer_ref,
    own_stack_ref,
    stack_ref,
    column_ref,
    *,
    levels,
):
    rows, cells = cells_ref.shape
    solve_columns(total_ref, lat_inner_ref, lat_outer_ref, high_ref, low_ref, cells_ref, speed_ref, inverse_ref, forward_ref, back_ref, levels, stack_ref, column_ref)
    for group in range(cells // LANES):
        part = column_ref[:, group, :]
        new_cells_ref[:, group * LANES : (group + 1) * LANES] = part
        put_parts(own_stack_ref, part, group * LANES)
    store_outer(gather_matmul(own_stack_ref, [matrix_ref[...]], rows), outer_ref)


def last_kernel(
    total_ref, lat_inner_ref, lat_outer_ref, high_ref, low_ref, cells_ref, speed_ref, inverse_ref, forward_ref, back_ref, out_ref, stack_ref, column_ref, *, levels
):
    cells = cells_ref.shape[1]
    solve_columns(total_ref, lat_inner_ref, lat_outer_ref, high_ref, low_ref, cells_ref, speed_ref, inverse_ref, forward_ref, back_ref, levels, stack_ref, column_ref)
    for group in range(cells // LANES):
        out_ref[:, 0, group * LANES : (group + 1) * LANES] = column_ref[0:levels, group, :]


def call(body, outs, scratch, *operands, raw=(), copies=0):
    in_vmem = pl.BlockSpec(memory_space=pltpu.VMEM)
    in_hbm = pl.BlockSpec(memory_space=pltpu.HBM)
    scratch_shapes = [pltpu.VMEM(shape, kind) for shape, kind in scratch]
    if copies:
        scratch_shapes.append(pltpu.SemaphoreType.DMA((copies,)))
    operands = [pltpu.with_memory_space_constraint(x, pltpu.HBM) if i in raw else x for i, x in enumerate(operands)]
    return pl.pallas_call(
        body,
        out_shape=tuple(jax.ShapeDtypeStruct(shape, kind) for shape, kind in outs),
        in_specs=[in_hbm if i in raw else in_vmem for i in range(len(operands))],
        out_specs=tuple(in_vmem for _ in outs),
        scratch_shapes=scratch_shapes,
        compiler_params=pltpu.CompilerParams(vmem_limit_bytes=24 * 1024 * 1024),
    )(*operands)


def on_device(lat_count, lon_count, pressure, velocity, edge_cells, cell_edges, send_cells, send_edges, inv_dual, edge_weight, sound_speed, coupling):
    _, levels, cells = pressure.shape
    edges = velocity.shape[2]
    halo = send_cells.shape[2]
    rows = round_up(levels, 16)
    edge_pad = round_up(edges, 2 * LANES)
    bundle = ((3, rows, halo), f32)
    straight = ((rows, halo), f32)
    lon_routes = swap_routes(lon_count)
    lat_inner_route = swap_routes(lat_count)[0]
    lat_outer_route = lat_outer_routes(lat_count, lon_count)
    i32 = jnp.int32

    by_level = lambda value: value.transpose(1, 0, 2)
    stack_cells = ((PARTS * rows, cells), bf16)
    stack_edges = ((PARTS * rows, edge_pad), bf16)
    stack_lat = ((PARTS * rows, 6 * halo), bf16)
    column = ((rows, cells // LANES, LANES), f32)
    sent_outer = lambda width: ((width, 3 * halo), bf16)
    sent_rest = lambda width: ((width, 5 * halo), bf16)

    for phase in range(2 * NSUB):
        at_cells = phase % 2 == 0
        if phase == 0:
            values, stack, outer, cell_list = call(
                start_kernel,
                [((rows, cells), f32), stack_cells, bundle, (send_cells.shape[1:], i32)],
                [((levels, 1, cells), f32), sent_outer(cells)],
                by_level(pressure),
                send_cells[0],
                raw=(0, 1),
                copies=2,
            )
        outer_in = lax.ppermute(outer, "lon", lon_routes[1])
        if phase == 0:
            inner, lat_inner, lat_outer = call(first_rest_kernel, [bundle, straight, straight], [sent_rest(cells)], stack, cell_list)
        else:
            inner, lat_inner, lat_outer = call(rest_kernel, [bundle, straight, straight], [], stack, cell_rest if at_cells else edge_rest)
        inner_in = lax.ppermute(inner, "lon", lon_routes[0])
        if phase == 0:
            gradient_near, gradient_far = call(
                functools.partial(gradient_kernel, cells=cells, halo=halo, lat_count=lat_count),
                [((cells + 2 * halo, edge_pad), bf16), ((6 * halo, edge_pad), bf16)],
                [(edge_cells.shape[1:], i32)],
                edge_cells[0],
                raw=(0,),
                copies=1,
            )
        if phase == 1:
            near_high, near_low, far_high, far_low = call(
                functools.partial(weight_kernel, edges=edges, edge_pad=edge_pad, halo=halo, lat_count=lat_count),
                [((edge_pad + 2 * halo, cells), bf16)] * 2 + [((6 * halo, cells), bf16)] * 2,
                [((3, 1, cells), i32), ((3, 1, cells), f32)],
                by_level(cell_edges),
                by_level(edge_weight),
                raw=(0, 1),
                copies=2,
            )
        first = jnp.stack([inner_in[1], outer_in[1], lat_inner])
        second = jnp.stack([inner_in[2], outer_in[2], lat_outer])
        first_in = lax.ppermute(first, "lat", lat_inner_route)
        second_in = lax.ppermute(second, ("lat", "lon"), lat_outer_route)
        if phase == 0:
            normal, scale, edge_outer, edge_rest = call(
                edge_setup_kernel,
                [((rows, edge_pad), f32), ((1, edge_pad), f32), sent_outer(edge_pad), sent_rest(edge_pad)],
                [((levels, 1, edges), f32), (send_edges.shape[1:], i32), ((1, edges), f32)],
                by_level(velocity),
                send_edges[0],
                inv_dual,
                raw=(0, 1, 2),
                copies=3,
            )
        if phase == 1:
            speed, inverse, forward, back, cell_outer, cell_rest = call(
                cell_setup_kernel,
                [((1, cells), f32), column, column, column, sent_outer(cells), sent_rest(cells)],
                [((levels, 1, cells), f32), column],
                by_level(coupling),
                cell_list,
                sound_speed,
                raw=(0, 2),
                copies=2,
            )
        if at_cells:
            (total,) = call(
                part_kernel,
                [((rows, edge_pad), f32)],
                [((PARTS * rows, cells + 2 * halo), bf16)],
                values,
                inner_in,
                outer_in,
                gradient_near,
            )
            normal, outer, stack = call(
                edge_kernel,
                [((rows, edge_pad), f32), bundle, stack_edges],
                [stack_lat],
                total,
                first_in,
                second_in,
                gradient_far,
                normal,
                scale,
                edge_outer,
            )
        else:
            (total,) = call(
                part_kernel,
                [((rows, cells), f32)],
                [((PARTS * rows, edge_pad + 2 * halo), bf16)],
                normal,
                inner_in,
                outer_in,
                near_high,
                near_low,
            )
            operands = (total, first_in, second_in, far_high, far_low, values, speed, inverse, forward, back)
            if phase < 2 * NSUB - 1:
                values, outer, stack = call(
                    functools.partial(cell_kernel, levels=levels),
                    [((rows, cells), f32), bundle, stack_cells],
                    [stack_lat, column],
                    *operands,
                    cell_outer,
                )
            else:
                (values,) = call(functools.partial(last_kernel, levels=levels), [((levels, 1, cells), f32)], [stack_lat, column], *operands)
    return by_level(values), normal[:levels, :edges][None]


def solution(mesh):
    return jax.shard_map(
        functools.partial(on_device, mesh.shape["lat"], mesh.shape["lon"]),
        mesh=mesh,
        in_specs=(
            P("lat", None, "lon"),
            P("lat", None, "lon"),
            P("lat", None, "lon"),
            P("lat", None, "lon"),
            P("lat", None, "lon"),
            P("lat", None, "lon"),
            P("lat", "lon"),
            P("lat", None, "lon"),
            P("lat", "lon"),
            P("lat", None, "lon"),
        ),
        out_specs=(P("lat", None, "lon"), P("lat", None, "lon")),
        check_vma=False,
    )
```

```python
import functools

import jax
import jax.numpy as jnp
from jax import lax
from jax.experimental import pallas as pl
from jax.experimental.pallas import tpu as pltpu
from jax.sharding import PartitionSpec as P


NSUB = 3
STEP_SCALE = 0.5
LANES = 128
PARTS = 3

f32 = jnp.float32
bf16 = jnp.bfloat16
i16 = jnp.int16


def round_up(value, step):
    return -(-value // step) * step


def swap_routes(count):
    inner = [(i, i ^ 1) for i in range(count)]
    outer = [(i, (((i + 1) ^ 1) - 1) % count) for i in range(count)]
    return inner, outer


def lat_outer_routes(lat_count, lon_count):
    routes = []
    for a, target in swap_routes(lat_count)[1]:
        for b in range(lon_count):
            alone = a in (0, lat_count - 1)
            routes.append((a * lon_count + b, a * lon_count + (b ^ 1) if alone else target * lon_count + b))
    return routes


OUTER_SENT = ((0, 2), (1, 2), (2, 2))
REST_SENT = ((0, 1), (1, 1), (2, 1), (1, 0), (2, 0))


def link_signs():
    lat_inner = 1 - 2 * lax.rem(lax.axis_index("lat"), 2)
    lon_inner = 1 - 2 * lax.rem(lax.axis_index("lon"), 2)
    return lat_inner, lon_inner


def sent_row(member):
    lat_inner, lon_inner = link_signs()
    lat_link, lon_link = member
    p = (0, lat_inner, -lat_inner)[lat_link]
    q = (0, lon_inner, -lon_inner)[lon_link]
    flat = (p + 1) * 3 + (q + 1)
    return flat - jnp.where(flat > 4, 1, 0)


def local_positions(index, own, own_padded, halo, lat_count):
    lat_inner, lon_inner = link_signs()
    a = lax.axis_index("lat")
    beyond = index - own
    piece = lax.div(jnp.maximum(beyond, 0), halo)
    slot = beyond - piece * halo
    flat = piece + jnp.where(piece >= 4, 1, 0)
    p = jnp.where(flat >= 6, 1, jnp.where(flat >= 3, 0, -1))
    q = flat - 3 * (p + 1) - 1
    lon_member = jnp.where(q == 0, 2, jnp.where(q == lon_inner, 0, 1))
    member = jnp.where(p == 0, lon_member, jnp.where(p == lat_inner, 2, 5) + lon_member)
    outside = (a + p < 0) | (a + p >= lat_count)
    row = own_padded + member * halo + slot
    return jnp.where(beyond < 0, index, jnp.where(outside, -1, row))


def put_parts(stack_ref, value, start):
    rows, width = value.shape
    rest = value
    for part in range(PARTS):
        piece = rest.astype(bf16)
        stack_ref[part * rows : (part + 1) * rows, start : start + width] = piece
        if part < PARTS - 1:
            rest = rest - piece.astype(f32)


def sum_parts(product, rows):
    total = product[(PARTS - 1) * rows : PARTS * rows]
    for part in range(PARTS - 2, -1, -1):
        total = total + product[part * rows : (part + 1) * rows]
    return total


def gather_matmul(stack_ref, matrices, rows):
    product = None
    for matrix in matrices:
        term = jnp.dot(stack_ref[...], matrix, preferred_element_type=f32)
        product = term if product is None else product + term
    return sum_parts(product, rows)


def start_fetch(pairs, sems):
    copies = [pltpu.make_async_copy(source, target, sems.at[i]) for i, (source, target) in enumerate(pairs)]
    for copy in copies:
        copy.start()
    return copies


def fetch(pairs, sems):
    for copy in start_fetch(pairs, sems):
        copy.wait()


def by_blocks(rows, body):
    block = 64 if rows % 64 == 0 else 16

    def step(i, carry):
        first = pl.multiple_of(i * block, block)
        body(first, block)
        return carry

    lax.fori_loop(0, rows // block, step, 0)


def row_numbers(first, block, width):
    return (lax.broadcasted_iota(jnp.int32, (block, width), 0) + first).astype(i16)


def fill_sent(matrix_ref, list_ref, members):
    rows = matrix_ref.shape[0]
    halo = list_ref.shape[1]
    lanes = [list_ref[pl.ds(sent_row(member), 1), :].astype(i16) for member in members]

    def body(first, block):
        row = row_numbers(first, block, halo)
        for member, index in enumerate(lanes):
            hit = jnp.where(row == index, jnp.ones((), bf16), jnp.zeros((), bf16))
            matrix_ref[pl.ds(first, block), member * halo : (member + 1) * halo] = hit

    by_blocks(rows, body)


def store_outer(pieces, outer_ref):
    halo = outer_ref.shape[2]
    for member in range(3):
        outer_ref[member] = pieces[:, member * halo : (member + 1) * halo]


def store_rest(pieces, inner_ref, lat_inner_ref, lat_outer_ref):
    halo = inner_ref.shape[2]
    for member in range(3):
        inner_ref[member] = pieces[:, member * halo : (member + 1) * halo]
    lat_inner_ref[...] = pieces[:, 3 * halo : 4 * halo]
    lat_outer_ref[...] = pieces[:, 4 * halo : 5 * halo]


def start_kernel(pressure_hbm, list_hbm, cells_ref, stack_ref, outer_ref, lists_ref, pressure_ref, matrix_ref, sems):
    lists, pressure = start_fetch([(list_hbm, lists_ref), (pressure_hbm, pressure_ref)], sems)
    levels = pressure_ref.shape[0]
    rows = cells_ref.shape[0]
    lists.wait()
    fill_sent(matrix_ref, lists_ref, OUTER_SENT)
    pressure.wait()
    cells_ref[0:levels, :] = pressure_ref[:, 0, :]
    cells_ref[levels:rows, :] = jnp.zeros((rows - levels, cells_ref.shape[1]), f32)
    put_parts(stack_ref, cells_ref[...], 0)
    store_outer(gather_matmul(stack_ref, [matrix_ref[...]], rows), outer_ref)


def first_rest_kernel(stack_ref, list_ref, inner_ref, lat_inner_ref, lat_outer_ref, matrix_ref):
    fill_sent(matrix_ref, list_ref, REST_SENT)
    store_rest(gather_matmul(stack_ref, [matrix_ref[...]], inner_ref.shape[1]), inner_ref, lat_inner_ref, lat_outer_ref)


def rest_kernel(stack_ref, matrix_ref, inner_ref, lat_inner_ref, lat_outer_ref):
    store_rest(gather_matmul(stack_ref, [matrix_ref[...]], inner_ref.shape[1]), inner_ref, lat_inner_ref, lat_outer_ref)


def gradient_kernel(edge_cells_hbm, near_ref, far_ref, ends_ref, sems, *, cells, halo, lat_count):
    fetch([(edge_cells_hbm, ends_ref)], sems)
    edges = ends_ref.shape[1]
    edge_pad = near_ref.shape[1]
    ends = local_positions(ends_ref[...], cells, cells, halo, lat_count)
    near, far = ends[0:1, :], ends[1:2, :]
    same = near == far
    near, far = jnp.where(same, -1, near), jnp.where(same, -1, far)
    if edge_pad > edges:
        fill = jnp.full((1, edge_pad - edges), -1, jnp.int32)
        near, far = jnp.concatenate([near, fill], axis=1), jnp.concatenate([far, fill], axis=1)
    near, far = near.astype(i16), far.astype(i16)

    def fill_rows(matrix_ref, base):
        def body(first, block):
            row = row_numbers(first + base, block, edge_pad)
            one = jnp.ones((), bf16)
            matrix_ref[pl.ds(first, block), :] = jnp.where(row == far, one, jnp.where(row == near, -one, jnp.zeros((), bf16)))

        by_blocks(matrix_ref.shape[0], body)

    fill_rows(near_ref, 0)
    fill_rows(far_ref, near_ref.shape[0])


def edge_setup_kernel(velocity_hbm, list_hbm, dual_hbm, edges_ref, scale_ref, outer_matrix_ref, rest_matrix_ref, velocity_ref, list_ref, dual_ref, sems):
    lists, velocity, dual = start_fetch([(list_hbm, list_ref), (velocity_hbm, velocity_ref), (dual_hbm, dual_ref)], sems)
    levels, _, edges = velocity_ref.shape
    edges_ref[...] = jnp.zeros(edges_ref.shape, f32)
    scale_ref[...] = jnp.zeros(scale_ref.shape, f32)
    lists.wait()
    fill_sent(outer_matrix_ref, list_ref, OUTER_SENT)
    fill_sent(rest_matrix_ref, list_ref, REST_SENT)
    velocity.wait()
    dual.wait()
    edges_ref[0:levels, 0:edges] = velocity_ref[:, 0, :]
    scale_ref[:, 0:edges] = STEP_SCALE * dual_ref[...]


def weight_kernel(
    sides_hbm, weight_hbm, near_high_ref, near_low_ref, far_high_ref, far_low_ref, sides_ref, weight_ref, sems, *, edges, edge_pad, halo, lat_count
):
    fetch([(sides_hbm, sides_ref), (weight_hbm, weight_ref)], sems)
    cells = sides_ref.shape[2]
    place = [local_positions(sides_ref[i], edges, edge_pad, halo, lat_count) for i in range(3)]
    weight = [weight_ref[i] for i in range(3)]
    for later in (1, 2):
        for earlier in range(later):
            same = place[later] == place[earlier]
            weight[earlier] = weight[earlier] + jnp.where(same, weight[later], 0.0)
            weight[later] = jnp.where(same, 0.0, weight[later])
            place[later] = jnp.where(same, -1, place[later])
    high = [value.astype(bf16) for value in weight]
    low = [(value - top.astype(f32)).astype(bf16) for value, top in zip(weight, high)]
    place = [value.astype(i16) for value in place]
    zero = jnp.zeros((), bf16)

    def fill_rows(high_ref, low_ref, base):
        def body(first, block):
            row = row_numbers(first + base, block, cells)
            hits = [row == value for value in place]
            for target, values in ((high_ref, high), (low_ref, low)):
                entry = jnp.where(hits[0], values[0], jnp.where(hits[1], values[1], jnp.where(hits[2], values[2], zero)))
                target[pl.ds(first, block), :] = entry

        by_blocks(high_ref.shape[0], body)

    fill_rows(near_high_ref, near_low_ref, 0)
    fill_rows(far_high_ref, far_low_ref, near_high_ref.shape[0])


def cell_setup_kernel(
    coupling_hbm, list_ref, speed_hbm, speed_ref, inverse_ref, forward_ref, back_ref, outer_matrix_ref, rest_matrix_ref, coupling_ref, column_ref, sems
):
    coupling, speed = start_fetch([(coupling_hbm, coupling_ref), (speed_hbm, speed_ref)], sems)
    levels, _, cells = coupling_ref.shape
    fill_sent(outer_matrix_ref, list_ref, OUTER_SENT)
    fill_sent(rest_matrix_ref, list_ref, REST_SENT)
    coupling.wait()
    speed.wait()
    step = column_ref.shape[0] // round_up(levels, 16)
    column_ref[...] = jnp.zeros(column_ref.shape, f32)
    for group in range(cells // LANES):
        column_ref[pl.ds(group, levels, stride=step), :] = coupling_ref[:, 0, group * LANES : (group + 1) * LANES]
    at = lambda level: slice(level * step, (level + 1) * step)
    above = column_ref[at(0), :]
    inverse = 1.0 / (1.0 + above)
    inverse_ref[at(0), :] = inverse
    ratio = above * inverse
    back_ref[at(0), :] = ratio
    for level in range(1, levels):
        below = above
        above = column_ref[at(level), :]
        inverse = 1.0 / (1.0 + below + above - below * ratio)
        inverse_ref[at(level), :] = inverse
        forward_ref[at(level), :] = below * inverse
        ratio = above * inverse
        back_ref[at(level), :] = ratio


def part_kernel(own_ref, inner_ref, outer_ref, *rest):
    *matrix_refs, total_ref, stack_ref = rest
    rows, width = own_ref.shape
    halo = inner_ref.shape[2]
    put_parts(stack_ref, own_ref[...], 0)
    put_parts(stack_ref, inner_ref[0], width)
    put_parts(stack_ref, outer_ref[0], width + halo)
    total_ref[...] = gather_matmul(stack_ref, [ref[...] for ref in matrix_refs], rows)


def lat_share(total_ref, lat_inner_ref, lat_outer_ref, matrix_refs, stack_ref):
    rows = total_ref.shape[0]
    halo = lat_inner_ref.shape[2]
    for member in range(3):
        put_parts(stack_ref, lat_inner_ref[member], member * halo)
        put_parts(stack_ref, lat_outer_ref[member], (3 + member) * halo)
    return total_ref[...] + gather_matmul(stack_ref, [ref[...] for ref in matrix_refs], rows)


def edge_kernel(total_ref, lat_inner_ref, lat_outer_ref, far_ref, edges_ref, scale_ref, matrix_ref, new_edges_ref, outer_ref, own_stack_ref, stack_ref):
    rows = edges_ref.shape[0]
    difference = lat_share(total_ref, lat_inner_ref, lat_outer_ref, [far_ref], stack_ref)
    new_edges = edges_ref[...] - scale_ref[...] * difference
    new_edges_ref[...] = new_edges
    put_parts(own_stack_ref, new_edges, 0)
    store_outer(gather_matmul(own_stack_ref, [matrix_ref[...]], rows), outer_ref)


def solve_columns(total_ref, lat_inner_ref, lat_outer_ref, high_ref, low_ref, cells_ref, speed_ref, inverse_ref, forward_ref, back_ref, levels, stack_ref, column_ref):
    rows, cells = cells_ref.shape
    divergence = lat_share(total_ref, lat_inner_ref, lat_outer_ref, [high_ref, low_ref], stack_ref)
    right_side = cells_ref[...] - speed_ref[...] * divergence
    step = column_ref.shape[0] // rows
    for group in range(cells // LANES):
        column_ref[pl.ds(group, rows, stride=step), :] = right_side[:, group * LANES : (group + 1) * LANES]
    for group in range(cells // LANES, step):
        column_ref[pl.ds(group, rows, stride=step), :] = jnp.zeros((rows, LANES), f32)
    at = lambda level: slice(level * step, (level + 1) * step)
    current = column_ref[at(0), :] * inverse_ref[at(0), :]
    scaled = [current]
    for level in range(1, levels):
        current = column_ref[at(level), :] * inverse_ref[at(level), :] + forward_ref[at(level), :] * current
        scaled.append(current)
    column_ref[at(levels - 1), :] = current
    for level in range(levels - 2, -1, -1):
        current = scaled[level] + back_ref[at(level), :] * current
        column_ref[at(level), :] = current
    for level in range(levels, rows):
        column_ref[at(level), :] = jnp.zeros_like(current)


def solved(column_ref, group, rows):
    return column_ref[pl.ds(group, rows, stride=column_ref.shape[0] // rows), :]


def cell_kernel(
    total_ref,
    lat_inner_ref,
    lat_outer_ref,
    high_ref,
    low_ref,
    cells_ref,
    speed_ref,
    inverse_ref,
    forward_ref,
    back_ref,
    matrix_ref,
    new_cells_ref,
    outer_ref,
    own_stack_ref,
    stack_ref,
    column_ref,
    *,
    levels,
):
    rows, cells = cells_ref.shape
    solve_columns(total_ref, lat_inner_ref, lat_outer_ref, high_ref, low_ref, cells_ref, speed_ref, inverse_ref, forward_ref, back_ref, levels, stack_ref, column_ref)
    for group in range(cells // LANES):
        part = solved(column_ref, group, rows)
        new_cells_ref[:, group * LANES : (group + 1) * LANES] = part
        put_parts(own_stack_ref, part, group * LANES)
    store_outer(gather_matmul(own_stack_ref, [matrix_ref[...]], rows), outer_ref)


def last_kernel(
    total_ref, lat_inner_ref, lat_outer_ref, high_ref, low_ref, cells_ref, speed_ref, inverse_ref, forward_ref, back_ref, out_ref, stack_ref, column_ref, *, levels
):
    rows, cells = cells_ref.shape
    solve_columns(total_ref, lat_inner_ref, lat_outer_ref, high_ref, low_ref, cells_ref, speed_ref, inverse_ref, forward_ref, back_ref, levels, stack_ref, column_ref)
    for group in range(cells // LANES):
        out_ref[:, 0, group * LANES : (group + 1) * LANES] = solved(column_ref, group, rows)[0:levels]


def call(body, outs, scratch, *operands, raw=(), copies=0):
    in_vmem = pl.BlockSpec(memory_space=pltpu.VMEM)
    in_hbm = pl.BlockSpec(memory_space=pltpu.HBM)
    scratch_shapes = [pltpu.VMEM(shape, kind) for shape, kind in scratch]
    if copies:
        scratch_shapes.append(pltpu.SemaphoreType.DMA((copies,)))
    operands = [pltpu.with_memory_space_constraint(x, pltpu.HBM) if i in raw else x for i, x in enumerate(operands)]
    return pl.pallas_call(
        body,
        out_shape=tuple(jax.ShapeDtypeStruct(shape, kind) for shape, kind in outs),
        in_specs=[in_hbm if i in raw else in_vmem for i in range(len(operands))],
        out_specs=tuple(in_vmem for _ in outs),
        scratch_shapes=scratch_shapes,
        compiler_params=pltpu.CompilerParams(vmem_limit_bytes=24 * 1024 * 1024),
    )(*operands)


def on_device(lat_count, lon_count, pressure, velocity, edge_cells, cell_edges, send_cells, send_edges, inv_dual, edge_weight, sound_speed, coupling):
    _, levels, cells = pressure.shape
    edges = velocity.shape[2]
    halo = send_cells.shape[2]
    rows = round_up(levels, 16)
    edge_pad = round_up(edges, 2 * LANES)
    bundle = ((3, rows, halo), f32)
    straight = ((rows, halo), f32)
    lon_routes = swap_routes(lon_count)
    lat_inner_route = swap_routes(lat_count)[0]
    lat_outer_route = lat_outer_routes(lat_count, lon_count)
    i32 = jnp.int32

    by_level = lambda value: value.transpose(1, 0, 2)
    stack_cells = ((PARTS * rows, cells), bf16)
    stack_edges = ((PARTS * rows, edge_pad), bf16)
    stack_lat = ((PARTS * rows, 6 * halo), bf16)
    column = ((rows * round_up(cells // LANES, 8), LANES), f32)
    sent_outer = lambda width: ((width, 3 * halo), bf16)
    sent_rest = lambda width: ((width, 5 * halo), bf16)

    for phase in range(2 * NSUB):
        at_cells = phase % 2 == 0
        if phase == 0:
            values, stack, outer, cell_list = call(
                start_kernel,
                [((rows, cells), f32), stack_cells, bundle, (send_cells.shape[1:], i32)],
                [((levels, 1, cells), f32), sent_outer(cells)],
                by_level(pressure),
                send_cells[0],
                raw=(0, 1),
                copies=2,
            )
        outer_in = lax.ppermute(outer, "lon", lon_routes[1])
        if phase == 0:
            inner, lat_inner, lat_outer = call(first_rest_kernel, [bundle, straight, straight], [sent_rest(cells)], stack, cell_list)
        else:
            inner, lat_inner, lat_outer = call(rest_kernel, [bundle, straight, straight], [], stack, cell_rest if at_cells else edge_rest)
        inner_in = lax.ppermute(inner, "lon", lon_routes[0])
        if phase == 0:
            gradient_near, gradient_far = call(
                functools.partial(gradient_kernel, cells=cells, halo=halo, lat_count=lat_count),
                [((cells + 2 * halo, edge_pad), bf16), ((6 * halo, edge_pad), bf16)],
                [(edge_cells.shape[1:], i32)],
                edge_cells[0],
                raw=(0,),
                copies=1,
            )
        if phase == 1:
            near_high, near_low, far_high, far_low = call(
                functools.partial(weight_kernel, edges=edges, edge_pad=edge_pad, halo=halo, lat_count=lat_count),
                [((edge_pad + 2 * halo, cells), bf16)] * 2 + [((6 * halo, cells), bf16)] * 2,
                [((3, 1, cells), i32), ((3, 1, cells), f32)],
                by_level(cell_edges),
                by_level(edge_weight),
                raw=(0, 1),
                copies=2,
            )
        first = jnp.stack([inner_in[1], outer_in[1], lat_inner])
        second = jnp.stack([inner_in[2], outer_in[2], lat_outer])
        first_in = lax.ppermute(first, "lat", lat_inner_route)
        second_in = lax.ppermute(second, ("lat", "lon"), lat_outer_route)
        if phase == 0:
            normal, scale, edge_outer, edge_rest = call(
                edge_setup_kernel,
                [((rows, edge_pad), f32), ((1, edge_pad), f32), sent_outer(edge_pad), sent_rest(edge_pad)],
                [((levels, 1, edges), f32), (send_edges.shape[1:], i32), ((1, edges), f32)],
                by_level(velocity),
                send_edges[0],
                inv_dual,
                raw=(0, 1, 2),
                copies=3,
            )
        if phase == 1:
            speed, inverse, forward, back, cell_outer, cell_rest = call(
                cell_setup_kernel,
                [((1, cells), f32), column, column, column, sent_outer(cells), sent_rest(cells)],
                [((levels, 1, cells), f32), column],
                by_level(coupling),
                cell_list,
                sound_speed,
                raw=(0, 2),
                copies=2,
            )
        if at_cells:
            (total,) = call(
                part_kernel,
                [((rows, edge_pad), f32)],
                [((PARTS * rows, cells + 2 * halo), bf16)],
                values,
                inner_in,
                outer_in,
                gradient_near,
            )
            normal, outer, stack = call(
                edge_kernel,
                [((rows, edge_pad), f32), bundle, stack_edges],
                [stack_lat],
                total,
                first_in,
                second_in,
                gradient_far,
                normal,
                scale,
                edge_outer,
            )
        else:
            (total,) = call(
                part_kernel,
                [((rows, cells), f32)],
                [((PARTS * rows, edge_pad + 2 * halo), bf16)],
                normal,
                inner_in,
                outer_in,
                near_high,
                near_low,
            )
            operands = (total, first_in, second_in, far_high, far_low, values, speed, inverse, forward, back)
            if phase < 2 * NSUB - 1:
                values, outer, stack = call(
                    functools.partial(cell_kernel, levels=levels),
                    [((rows, cells), f32), bundle, stack_cells],
                    [stack_lat, column],
                    *operands,
                    cell_outer,
                )
            else:
                (values,) = call(functools.partial(last_kernel, levels=levels), [((levels, 1, cells), f32)], [stack_lat, column], *operands)
    return by_level(values), normal[:levels, :edges][None]


def solution(mesh):
    return jax.shard_map(
        functools.partial(on_device, mesh.shape["lat"], mesh.shape["lon"]),
        mesh=mesh,
        in_specs=(
            P("lat", None, "lon"),
            P("lat", None, "lon"),
            P("lat", None, "lon"),
            P("lat", None, "lon"),
            P("lat", None, "lon"),
            P("lat", None, "lon"),
            P("lat", "lon"),
            P("lat", None, "lon"),
            P("lat", "lon"),
            P("lat", None, "lon"),
        ),
        out_specs=(P("lat", None, "lon"), P("lat", None, "lon")),
        check_vma=False,
    )
```

```python
import functools

import jax
import jax.numpy as jnp
from jax import lax
from jax.experimental import pallas as pl
from jax.experimental.pallas import tpu as pltpu
from jax.sharding import PartitionSpec as P


NSUB = 3
STEP_SCALE = 0.5
LANES = 128
PARTS = 3

f32 = jnp.float32
bf16 = jnp.bfloat16
i16 = jnp.int16


def round_up(value, step):
    return -(-value // step) * step


def swap_routes(count):
    inner = [(i, i ^ 1) for i in range(count)]
    outer = [(i, (((i + 1) ^ 1) - 1) % count) for i in range(count)]
    return inner, outer


def lat_outer_routes(lat_count, lon_count):
    routes = []
    for a, target in swap_routes(lat_count)[1]:
        for b in range(lon_count):
            alone = a in (0, lat_count - 1)
            routes.append((a * lon_count + b, a * lon_count + (b ^ 1) if alone else target * lon_count + b))
    return routes


OUTER_SENT = ((0, 2), (1, 2), (2, 2))
REST_SENT = ((0, 1), (1, 1), (2, 1), (1, 0), (2, 0))


def link_signs():
    lat_inner = 1 - 2 * lax.rem(lax.axis_index("lat"), 2)
    lon_inner = 1 - 2 * lax.rem(lax.axis_index("lon"), 2)
    return lat_inner, lon_inner


def sent_row(member):
    lat_inner, lon_inner = link_signs()
    lat_link, lon_link = member
    p = (0, lat_inner, -lat_inner)[lat_link]
    q = (0, lon_inner, -lon_inner)[lon_link]
    flat = (p + 1) * 3 + (q + 1)
    return flat - jnp.where(flat > 4, 1, 0)


def local_positions(index, own, own_padded, halo, lat_count):
    lat_inner, lon_inner = link_signs()
    a = lax.axis_index("lat")
    beyond = index - own
    piece = lax.div(jnp.maximum(beyond, 0), halo)
    slot = beyond - piece * halo
    flat = piece + jnp.where(piece >= 4, 1, 0)
    p = jnp.where(flat >= 6, 1, jnp.where(flat >= 3, 0, -1))
    q = flat - 3 * (p + 1) - 1
    lon_member = jnp.where(q == 0, 2, jnp.where(q == lon_inner, 0, 1))
    member = jnp.where(p == 0, lon_member, jnp.where(p == lat_inner, 2, 5) + lon_member)
    outside = (a + p < 0) | (a + p >= lat_count)
    row = own_padded + member * halo + slot
    return jnp.where(beyond < 0, index, jnp.where(outside, -1, row))


def put_parts(stack_ref, value, start):
    rows, width = value.shape
    rest = value
    for part in range(PARTS):
        piece = rest.astype(bf16)
        stack_ref[part * rows : (part + 1) * rows, start : start + width] = piece
        if part < PARTS - 1:
            rest = rest - piece.astype(f32)


def sum_parts(product, rows):
    total = product[(PARTS - 1) * rows : PARTS * rows]
    for part in range(PARTS - 2, -1, -1):
        total = total + product[part * rows : (part + 1) * rows]
    return total


def gather_matmul(stack_ref, matrices, rows):
    product = None
    for matrix in matrices:
        term = jnp.dot(stack_ref[...], matrix, preferred_element_type=f32)
        product = term if product is None else product + term
    return sum_parts(product, rows)


def start_fetch(pairs, sems):
    copies = [pltpu.make_async_copy(source, target, sems.at[i]) for i, (source, target) in enumerate(pairs)]
    for copy in copies:
        copy.start()
    return copies


def fetch(pairs, sems):
    for copy in start_fetch(pairs, sems):
        copy.wait()


def by_blocks(rows, body):
    block = 64 if rows % 64 == 0 else 16

    def step(i, carry):
        first = pl.multiple_of(i * block, block)
        body(first, block)
        return carry

    lax.fori_loop(0, rows // block, step, 0)


def row_numbers(first, block, width):
    return (lax.broadcasted_iota(jnp.int32, (block, width), 0) + first).astype(i16)


def fill_sent(matrix_ref, list_ref, members):
    rows = matrix_ref.shape[0]
    halo = list_ref.shape[1]
    lanes = [list_ref[pl.ds(sent_row(member), 1), :].astype(i16) for member in members]

    def body(first, block):
        row = row_numbers(first, block, halo)
        for member, index in enumerate(lanes):
            hit = jnp.where(row == index, jnp.ones((), bf16), jnp.zeros((), bf16))
            matrix_ref[pl.ds(first, block), member * halo : (member + 1) * halo] = hit

    by_blocks(rows, body)


def store_outer(pieces, outer_ref):
    halo = outer_ref.shape[2]
    for member in range(3):
        outer_ref[member] = pieces[:, member * halo : (member + 1) * halo]


def store_rest(pieces, inner_ref, lat_inner_ref, lat_outer_ref):
    halo = inner_ref.shape[2]
    for member in range(3):
        inner_ref[member] = pieces[:, member * halo : (member + 1) * halo]
    lat_inner_ref[...] = pieces[:, 3 * halo : 4 * halo]
    lat_outer_ref[...] = pieces[:, 4 * halo : 5 * halo]


def start_kernel(pressure_hbm, list_hbm, cells_ref, stack_ref, outer_ref, lists_ref, pressure_ref, matrix_ref, sems):
    lists, pressure = start_fetch([(list_hbm, lists_ref), (pressure_hbm, pressure_ref)], sems)
    levels = pressure_ref.shape[0]
    rows = cells_ref.shape[0]
    lists.wait()
    fill_sent(matrix_ref, lists_ref, OUTER_SENT)
    pressure.wait()
    cells_ref[0:levels, :] = pressure_ref[:, 0, :]
    cells_ref[levels:rows, :] = jnp.zeros((rows - levels, cells_ref.shape[1]), f32)
    put_parts(stack_ref, cells_ref[...], 0)
    store_outer(gather_matmul(stack_ref, [matrix_ref[...]], rows), outer_ref)


def first_rest_kernel(stack_ref, list_ref, inner_ref, lat_inner_ref, lat_outer_ref, matrix_ref):
    fill_sent(matrix_ref, list_ref, REST_SENT)
    store_rest(gather_matmul(stack_ref, [matrix_ref[...]], inner_ref.shape[1]), inner_ref, lat_inner_ref, lat_outer_ref)


def rest_kernel(stack_ref, matrix_ref, inner_ref, lat_inner_ref, lat_outer_ref):
    store_rest(gather_matmul(stack_ref, [matrix_ref[...]], inner_ref.shape[1]), inner_ref, lat_inner_ref, lat_outer_ref)


def gradient_kernel(edge_cells_hbm, near_ref, far_ref, ends_ref, sems, *, cells, halo, lat_count):
    fetch([(edge_cells_hbm, ends_ref)], sems)
    edges = ends_ref.shape[1]
    edge_pad = near_ref.shape[1]
    ends = local_positions(ends_ref[...], cells, cells, halo, lat_count)
    near, far = ends[0:1, :], ends[1:2, :]
    same = near == far
    near, far = jnp.where(same, -1, near), jnp.where(same, -1, far)
    if edge_pad > edges:
        fill = jnp.full((1, edge_pad - edges), -1, jnp.int32)
        near, far = jnp.concatenate([near, fill], axis=1), jnp.concatenate([far, fill], axis=1)
    near, far = near.astype(i16), far.astype(i16)

    def fill_rows(matrix_ref, base):
        def body(first, block):
            row = row_numbers(first + base, block, edge_pad)
            one = jnp.ones((), bf16)
            matrix_ref[pl.ds(first, block), :] = jnp.where(row == far, one, jnp.where(row == near, -one, jnp.zeros((), bf16)))

        by_blocks(matrix_ref.shape[0], body)

    fill_rows(near_ref, 0)
    fill_rows(far_ref, near_ref.shape[0])


def edge_setup_kernel(velocity_hbm, list_hbm, dual_hbm, edges_ref, scale_ref, outer_matrix_ref, rest_matrix_ref, velocity_ref, list_ref, dual_ref, sems):
    lists, velocity, dual = start_fetch([(list_hbm, list_ref), (velocity_hbm, velocity_ref), (dual_hbm, dual_ref)], sems)
    levels, _, edges = velocity_ref.shape
    edges_ref[...] = jnp.zeros(edges_ref.shape, f32)
    scale_ref[...] = jnp.zeros(scale_ref.shape, f32)
    lists.wait()
    fill_sent(outer_matrix_ref, list_ref, OUTER_SENT)
    fill_sent(rest_matrix_ref, list_ref, REST_SENT)
    velocity.wait()
    dual.wait()
    edges_ref[0:levels, 0:edges] = velocity_ref[:, 0, :]
    scale_ref[:, 0:edges] = STEP_SCALE * dual_ref[...]


def weight_kernel(
    sides_hbm, weight_hbm, near_high_ref, near_low_ref, far_high_ref, far_low_ref, sides_ref, weight_ref, sems, *, edges, edge_pad, halo, lat_count
):
    fetch([(sides_hbm, sides_ref), (weight_hbm, weight_ref)], sems)
    cells = sides_ref.shape[2]
    place = [local_positions(sides_ref[i], edges, edge_pad, halo, lat_count) for i in range(3)]
    weight = [weight_ref[i] for i in range(3)]
    for later in (1, 2):
        for earlier in range(later):
            same = place[later] == place[earlier]
            weight[earlier] = weight[earlier] + jnp.where(same, weight[later], 0.0)
            weight[later] = jnp.where(same, 0.0, weight[later])
            place[later] = jnp.where(same, -1, place[later])
    high = [value.astype(bf16) for value in weight]
    low = [(value - top.astype(f32)).astype(bf16) for value, top in zip(weight, high)]
    place = [value.astype(i16) for value in place]
    zero = jnp.zeros((), bf16)

    def fill_rows(high_ref, low_ref, base):
        def body(first, block):
            row = row_numbers(first + base, block, cells)
            hits = [row == value for value in place]
            for target, values in ((high_ref, high), (low_ref, low)):
                entry = jnp.where(hits[0], values[0], jnp.where(hits[1], values[1], jnp.where(hits[2], values[2], zero)))
                target[pl.ds(first, block), :] = entry

        by_blocks(high_ref.shape[0], body)

    fill_rows(near_high_ref, near_low_ref, 0)
    fill_rows(far_high_ref, far_low_ref, near_high_ref.shape[0])


def cell_setup_kernel(
    coupling_hbm, list_ref, speed_hbm, speed_ref, inverse_ref, forward_ref, back_ref, outer_matrix_ref, rest_matrix_ref, coupling_ref, column_ref, sems
):
    coupling, speed = start_fetch([(coupling_hbm, coupling_ref), (speed_hbm, speed_ref)], sems)
    levels, _, cells = coupling_ref.shape
    fill_sent(outer_matrix_ref, list_ref, OUTER_SENT)
    fill_sent(rest_matrix_ref, list_ref, REST_SENT)
    coupling.wait()
    speed.wait()
    step = column_ref.shape[0] // round_up(levels, 16)
    column_ref[...] = jnp.zeros(column_ref.shape, f32)
    for group in range(cells // LANES):
        column_ref[pl.ds(group, levels, stride=step), :] = coupling_ref[:, 0, group * LANES : (group + 1) * LANES]
    at = lambda level: slice(level * step, (level + 1) * step)
    above = column_ref[at(0), :]
    inverse = 1.0 / (1.0 + above)
    inverse_ref[at(0), :] = inverse
    ratio = above * inverse
    back_ref[at(0), :] = ratio
    for level in range(1, levels):
        below = above
        above = column_ref[at(level), :]
        inverse = 1.0 / (1.0 + below + above - below * ratio)
        inverse_ref[at(level), :] = inverse
        forward_ref[at(level), :] = below * inverse
        ratio = above * inverse
        back_ref[at(level), :] = ratio


def part_kernel(own_ref, inner_ref, outer_ref, *rest):
    *matrix_refs, total_ref, stack_ref = rest
    rows, width = own_ref.shape
    halo = inner_ref.shape[2]
    put_parts(stack_ref, own_ref[...], 0)
    put_parts(stack_ref, inner_ref[0], width)
    put_parts(stack_ref, outer_ref[0], width + halo)
    total_ref[...] = gather_matmul(stack_ref, [ref[...] for ref in matrix_refs], rows)


def lat_share(total_ref, lat_ref, matrix_refs, stack_ref, half):
    rows = total_ref.shape[0]
    halo = lat_ref.shape[2]
    for member in range(3):
        put_parts(stack_ref, lat_ref[member], member * halo)
    matrices = [ref[half * 3 * halo : (half + 1) * 3 * halo, :] for ref in matrix_refs]
    return total_ref[...] + gather_matmul(stack_ref, matrices, rows)


def inner_share_kernel(total_ref, lat_inner_ref, *rest):
    *matrix_refs, new_total_ref, stack_ref = rest
    new_total_ref[...] = lat_share(total_ref, lat_inner_ref, matrix_refs, stack_ref, 0)


def edge_kernel(total_ref, lat_outer_ref, far_ref, edges_ref, scale_ref, matrix_ref, new_edges_ref, outer_ref, own_stack_ref, stack_ref):
    rows = edges_ref.shape[0]
    difference = lat_share(total_ref, lat_outer_ref, [far_ref], stack_ref, 1)
    new_edges = edges_ref[...] - scale_ref[...] * difference
    new_edges_ref[...] = new_edges
    put_parts(own_stack_ref, new_edges, 0)
    store_outer(gather_matmul(own_stack_ref, [matrix_ref[...]], rows), outer_ref)


def solve_columns(total_ref, lat_outer_ref, high_ref, low_ref, cells_ref, speed_ref, inverse_ref, forward_ref, back_ref, levels, stack_ref, column_ref):
    rows, cells = cells_ref.shape
    divergence = lat_share(total_ref, lat_outer_ref, [high_ref, low_ref], stack_ref, 1)
    right_side = cells_ref[...] - speed_ref[...] * divergence
    step = column_ref.shape[0] // rows
    for group in range(cells // LANES):
        column_ref[pl.ds(group, rows, stride=step), :] = right_side[:, group * LANES : (group + 1) * LANES]
    for group in range(cells // LANES, step):
        column_ref[pl.ds(group, rows, stride=step), :] = jnp.zeros((rows, LANES), f32)
    at = lambda level: slice(level * step, (level + 1) * step)
    current = column_ref[at(0), :] * inverse_ref[at(0), :]
    scaled = [current]
    for level in range(1, levels):
        current = column_ref[at(level), :] * inverse_ref[at(level), :] + forward_ref[at(level), :] * current
        scaled.append(current)
    column_ref[at(levels - 1), :] = current
    for level in range(levels - 2, -1, -1):
        current = scaled[level] + back_ref[at(level), :] * current
        column_ref[at(level), :] = current
    for level in range(levels, rows):
        column_ref[at(level), :] = jnp.zeros_like(current)


def solved(column_ref, group, rows):
    return column_ref[pl.ds(group, rows, stride=column_ref.shape[0] // rows), :]


def cell_kernel(
    total_ref,
    lat_outer_ref,
    high_ref,
    low_ref,
    cells_ref,
    speed_ref,
    inverse_ref,
    forward_ref,
    back_ref,
    matrix_ref,
    new_cells_ref,
    outer_ref,
    own_stack_ref,
    stack_ref,
    column_ref,
    *,
    levels,
):
    rows, cells = cells_ref.shape
    solve_columns(total_ref, lat_outer_ref, high_ref, low_ref, cells_ref, speed_ref, inverse_ref, forward_ref, back_ref, levels, stack_ref, column_ref)
    for group in range(cells // LANES):
        part = solved(column_ref, group, rows)
        new_cells_ref[:, group * LANES : (group + 1) * LANES] = part
        put_parts(own_stack_ref, part, group * LANES)
    store_outer(gather_matmul(own_stack_ref, [matrix_ref[...]], rows), outer_ref)


def last_kernel(
    total_ref, lat_outer_ref, high_ref, low_ref, cells_ref, speed_ref, inverse_ref, forward_ref, back_ref, out_ref, stack_ref, column_ref, *, levels
):
    rows, cells = cells_ref.shape
    solve_columns(total_ref, lat_outer_ref, high_ref, low_ref, cells_ref, speed_ref, inverse_ref, forward_ref, back_ref, levels, stack_ref, column_ref)
    for group in range(cells // LANES):
        out_ref[:, 0, group * LANES : (group + 1) * LANES] = solved(column_ref, group, rows)[0:levels]


def call(body, outs, scratch, *operands, raw=(), copies=0):
    in_vmem = pl.BlockSpec(memory_space=pltpu.VMEM)
    in_hbm = pl.BlockSpec(memory_space=pltpu.HBM)
    scratch_shapes = [pltpu.VMEM(shape, kind) for shape, kind in scratch]
    if copies:
        scratch_shapes.append(pltpu.SemaphoreType.DMA((copies,)))
    operands = [pltpu.with_memory_space_constraint(x, pltpu.HBM) if i in raw else x for i, x in enumerate(operands)]
    return pl.pallas_call(
        body,
        out_shape=tuple(jax.ShapeDtypeStruct(shape, kind) for shape, kind in outs),
        in_specs=[in_hbm if i in raw else in_vmem for i in range(len(operands))],
        out_specs=tuple(in_vmem for _ in outs),
        scratch_shapes=scratch_shapes,
        compiler_params=pltpu.CompilerParams(vmem_limit_bytes=24 * 1024 * 1024),
    )(*operands)


def on_device(lat_count, lon_count, pressure, velocity, edge_cells, cell_edges, send_cells, send_edges, inv_dual, edge_weight, sound_speed, coupling):
    _, levels, cells = pressure.shape
    edges = velocity.shape[2]
    halo = send_cells.shape[2]
    rows = round_up(levels, 16)
    edge_pad = round_up(edges, 2 * LANES)
    bundle = ((3, rows, halo), f32)
    straight = ((rows, halo), f32)
    lon_routes = swap_routes(lon_count)
    lat_inner_route = swap_routes(lat_count)[0]
    lat_outer_route = lat_outer_routes(lat_count, lon_count)
    i32 = jnp.int32

    by_level = lambda value: value.transpose(1, 0, 2)
    stack_cells = ((PARTS * rows, cells), bf16)
    stack_edges = ((PARTS * rows, edge_pad), bf16)
    stack_lat = ((PARTS * rows, 3 * halo), bf16)
    column = ((rows * round_up(cells // LANES, 8), LANES), f32)
    sent_outer = lambda width: ((width, 3 * halo), bf16)
    sent_rest = lambda width: ((width, 5 * halo), bf16)

    for phase in range(2 * NSUB):
        at_cells = phase % 2 == 0
        if phase == 0:
            values, stack, outer, cell_list = call(
                start_kernel,
                [((rows, cells), f32), stack_cells, bundle, (send_cells.shape[1:], i32)],
                [((levels, 1, cells), f32), sent_outer(cells)],
                by_level(pressure),
                send_cells[0],
                raw=(0, 1),
                copies=2,
            )
        outer_in = lax.ppermute(outer, "lon", lon_routes[1])
        if phase == 0:
            inner, lat_inner, lat_outer = call(first_rest_kernel, [bundle, straight, straight], [sent_rest(cells)], stack, cell_list)
        else:
            inner, lat_inner, lat_outer = call(rest_kernel, [bundle, straight, straight], [], stack, cell_rest if at_cells else edge_rest)
        inner_in = lax.ppermute(inner, "lon", lon_routes[0])
        if phase == 0:
            gradient_near, gradient_far = call(
                functools.partial(gradient_kernel, cells=cells, halo=halo, lat_count=lat_count),
                [((cells + 2 * halo, edge_pad), bf16), ((6 * halo, edge_pad), bf16)],
                [(edge_cells.shape[1:], i32)],
                edge_cells[0],
                raw=(0,),
                copies=1,
            )
        if phase == 1:
            near_high, near_low, far_high, far_low = call(
                functools.partial(weight_kernel, edges=edges, edge_pad=edge_pad, halo=halo, lat_count=lat_count),
                [((edge_pad + 2 * halo, cells), bf16)] * 2 + [((6 * halo, cells), bf16)] * 2,
                [((3, 1, cells), i32), ((3, 1, cells), f32)],
                by_level(cell_edges),
                by_level(edge_weight),
                raw=(0, 1),
                copies=2,
            )
        first = jnp.stack([inner_in[1], outer_in[1], lat_inner])
        second = jnp.stack([inner_in[2], outer_in[2], lat_outer])
        first_in = lax.ppermute(first, "lat", lat_inner_route)
        second_in = lax.ppermute(second, ("lat", "lon"), lat_outer_route)
        if phase == 0:
            normal, scale, edge_outer, edge_rest = call(
                edge_setup_kernel,
                [((rows, edge_pad), f32), ((1, edge_pad), f32), sent_outer(edge_pad), sent_rest(edge_pad)],
                [((levels, 1, edges), f32), (send_edges.shape[1:], i32), ((1, edges), f32)],
                by_level(velocity),
                send_edges[0],
                inv_dual,
                raw=(0, 1, 2),
                copies=3,
            )
        if phase == 1:
            speed, inverse, forward, back, cell_outer, cell_rest = call(
                cell_setup_kernel,
                [((1, cells), f32), column, column, column, sent_outer(cells), sent_rest(cells)],
                [((levels, 1, cells), f32), column],
                by_level(coupling),
                cell_list,
                sound_speed,
                raw=(0, 2),
                copies=2,
            )
        if at_cells:
            (total,) = call(
                part_kernel,
                [((rows, edge_pad), f32)],
                [((PARTS * rows, cells + 2 * halo), bf16)],
                values,
                inner_in,
                outer_in,
                gradient_near,
            )
            (total,) = call(inner_share_kernel, [((rows, edge_pad), f32)], [stack_lat], total, first_in, gradient_far)
            normal, outer, stack = call(
                edge_kernel,
                [((rows, edge_pad), f32), bundle, stack_edges],
                [stack_lat],
                total,
                second_in,
                gradient_far,
                normal,
                scale,
                edge_outer,
            )
        else:
            (total,) = call(
                part_kernel,
                [((rows, cells), f32)],
                [((PARTS * rows, edge_pad + 2 * halo), bf16)],
                normal,
                inner_in,
                outer_in,
                near_high,
                near_low,
            )
            (total,) = call(inner_share_kernel, [((rows, cells), f32)], [stack_lat], total, first_in, far_high, far_low)
            operands = (total, second_in, far_high, far_low, values, speed, inverse, forward, back)
            if phase < 2 * NSUB - 1:
                values, outer, stack = call(
                    functools.partial(cell_kernel, levels=levels),
                    [((rows, cells), f32), bundle, stack_cells],
                    [stack_lat, column],
                    *operands,
                    cell_outer,
                )
            else:
                (values,) = call(functools.partial(last_kernel, levels=levels), [((levels, 1, cells), f32)], [stack_lat, column], *operands)
    return by_level(values), normal[:levels, :edges][None]


def solution(mesh):
    return jax.shard_map(
        functools.partial(on_device, mesh.shape["lat"], mesh.shape["lon"]),
        mesh=mesh,
        in_specs=(
            P("lat", None, "lon"),
            P("lat", None, "lon"),
            P("lat", None, "lon"),
            P("lat", None, "lon"),
            P("lat", None, "lon"),
            P("lat", None, "lon"),
            P("lat", "lon"),
            P("lat", None, "lon"),
            P("lat", "lon"),
            P("lat", None, "lon"),
        ),
        out_specs=(P("lat", None, "lon"), P("lat", None, "lon")),
        check_vma=False,
    )
```

```python
import functools

import jax
import jax.numpy as jnp
from jax import lax
from jax.experimental import pallas as pl
from jax.experimental.pallas import tpu as pltpu
from jax.sharding import PartitionSpec as P


NSUB = 3
STEP_SCALE = 0.5
LANES = 128
PARTS = 3

f32 = jnp.float32
bf16 = jnp.bfloat16
i16 = jnp.int16


def round_up(value, step):
    return -(-value // step) * step


def swap_routes(count):
    inner = [(i, i ^ 1) for i in range(count)]
    outer = [(i, (((i + 1) ^ 1) - 1) % count) for i in range(count)]
    return inner, outer


def lat_outer_routes(lat_count, lon_count):
    routes = []
    for a, target in swap_routes(lat_count)[1]:
        for b in range(lon_count):
            alone = a in (0, lat_count - 1)
            routes.append((a * lon_count + b, a * lon_count + (b ^ 1) if alone else target * lon_count + b))
    return routes


OUTER_SENT = ((0, 2), (1, 2), (2, 2))
REST_SENT = ((0, 1), (1, 1), (2, 1), (1, 0), (2, 0))


def link_signs():
    lat_inner = 1 - 2 * lax.rem(lax.axis_index("lat"), 2)
    lon_inner = 1 - 2 * lax.rem(lax.axis_index("lon"), 2)
    return lat_inner, lon_inner


def sent_row(member):
    lat_inner, lon_inner = link_signs()
    lat_link, lon_link = member
    p = (0, lat_inner, -lat_inner)[lat_link]
    q = (0, lon_inner, -lon_inner)[lon_link]
    flat = (p + 1) * 3 + (q + 1)
    return flat - jnp.where(flat > 4, 1, 0)


def local_positions(index, own, own_padded, halo, lat_count):
    lat_inner, lon_inner = link_signs()
    a = lax.axis_index("lat")
    beyond = index - own
    piece = lax.div(jnp.maximum(beyond, 0), halo)
    slot = beyond - piece * halo
    flat = piece + jnp.where(piece >= 4, 1, 0)
    p = jnp.where(flat >= 6, 1, jnp.where(flat >= 3, 0, -1))
    q = flat - 3 * (p + 1) - 1
    lon_member = jnp.where(q == 0, 1, jnp.where(q == lon_inner, 0, 2))
    member = jnp.where(p == 0, jnp.minimum(lon_member, 1), jnp.where(p == lat_inner, 2, 5) + lon_member)
    outside = (a + p < 0) | (a + p >= lat_count)
    row = own_padded + member * halo + slot
    return jnp.where(beyond < 0, index, jnp.where(outside, -1, row))


def put_parts(stack_ref, value, start):
    rows, width = value.shape
    rest = value
    for part in range(PARTS):
        piece = rest.astype(bf16)
        stack_ref[part * rows : (part + 1) * rows, start : start + width] = piece
        if part < PARTS - 1:
            rest = rest - piece.astype(f32)


def sum_parts(product, rows):
    total = product[(PARTS - 1) * rows : PARTS * rows]
    for part in range(PARTS - 2, -1, -1):
        total = total + product[part * rows : (part + 1) * rows]
    return total


def gather_matmul(stack_ref, matrices, rows):
    product = None
    for matrix in matrices:
        term = jnp.dot(stack_ref[...], matrix, preferred_element_type=f32)
        product = term if product is None else product + term
    return sum_parts(product, rows)


def start_fetch(pairs, sems):
    copies = [pltpu.make_async_copy(source, target, sems.at[i]) for i, (source, target) in enumerate(pairs)]
    for copy in copies:
        copy.start()
    return copies


def fetch(pairs, sems):
    for copy in start_fetch(pairs, sems):
        copy.wait()


def by_blocks(rows, body):
    block = 64 if rows % 64 == 0 else 16

    def step(i, carry):
        first = pl.multiple_of(i * block, block)
        body(first, block)
        return carry

    lax.fori_loop(0, rows // block, step, 0)


def row_numbers(first, block, width):
    return (lax.broadcasted_iota(jnp.int32, (block, width), 0) + first).astype(i16)


def fill_sent(matrix_ref, list_ref, members):
    rows = matrix_ref.shape[0]
    halo = list_ref.shape[1]
    lanes = [list_ref[pl.ds(sent_row(member), 1), :].astype(i16) for member in members]

    def body(first, block):
        row = row_numbers(first, block, halo)
        for member, index in enumerate(lanes):
            hit = jnp.where(row == index, jnp.ones((), bf16), jnp.zeros((), bf16))
            matrix_ref[pl.ds(first, block), member * halo : (member + 1) * halo] = hit

    by_blocks(rows, body)


def store_outer(pieces, outer_ref):
    halo = outer_ref.shape[2]
    for member in range(3):
        outer_ref[member] = pieces[:, member * halo : (member + 1) * halo]


def store_rest(pieces, inner_ref, lat_inner_ref, lat_outer_ref):
    halo = inner_ref.shape[2]
    for member in range(3):
        inner_ref[member] = pieces[:, member * halo : (member + 1) * halo]
    lat_inner_ref[...] = pieces[:, 3 * halo : 4 * halo]
    lat_outer_ref[...] = pieces[:, 4 * halo : 5 * halo]


def start_kernel(pressure_hbm, list_hbm, cells_ref, stack_ref, outer_ref, lists_ref, pressure_ref, matrix_ref, sems):
    lists, pressure = start_fetch([(list_hbm, lists_ref), (pressure_hbm, pressure_ref)], sems)
    levels = pressure_ref.shape[0]
    rows = cells_ref.shape[0]
    lists.wait()
    fill_sent(matrix_ref, lists_ref, OUTER_SENT)
    pressure.wait()
    cells_ref[0:levels, :] = pressure_ref[:, 0, :]
    cells_ref[levels:rows, :] = jnp.zeros((rows - levels, cells_ref.shape[1]), f32)
    put_parts(stack_ref, cells_ref[...], 0)
    store_outer(gather_matmul(stack_ref, [matrix_ref[...]], rows), outer_ref)


def first_rest_kernel(stack_ref, list_ref, inner_ref, lat_inner_ref, lat_outer_ref, matrix_ref):
    fill_sent(matrix_ref, list_ref, REST_SENT)
    store_rest(gather_matmul(stack_ref, [matrix_ref[...]], inner_ref.shape[1]), inner_ref, lat_inner_ref, lat_outer_ref)


def rest_kernel(stack_ref, matrix_ref, inner_ref, lat_inner_ref, lat_outer_ref):
    store_rest(gather_matmul(stack_ref, [matrix_ref[...]], inner_ref.shape[1]), inner_ref, lat_inner_ref, lat_outer_ref)


def gradient_kernel(edge_cells_hbm, near_ref, far_ref, ends_ref, sems, *, cells, halo, lat_count):
    fetch([(edge_cells_hbm, ends_ref)], sems)
    edges = ends_ref.shape[1]
    edge_pad = near_ref.shape[1]
    ends = local_positions(ends_ref[...], cells, cells, halo, lat_count)
    near, far = ends[0:1, :], ends[1:2, :]
    same = near == far
    near, far = jnp.where(same, -1, near), jnp.where(same, -1, far)
    if edge_pad > edges:
        fill = jnp.full((1, edge_pad - edges), -1, jnp.int32)
        near, far = jnp.concatenate([near, fill], axis=1), jnp.concatenate([far, fill], axis=1)
    near, far = near.astype(i16), far.astype(i16)

    def fill_rows(matrix_ref, base):
        def body(first, block):
            row = row_numbers(first + base, block, edge_pad)
            one = jnp.ones((), bf16)
            matrix_ref[pl.ds(first, block), :] = jnp.where(row == far, one, jnp.where(row == near, -one, jnp.zeros((), bf16)))

        by_blocks(matrix_ref.shape[0], body)

    fill_rows(near_ref, 0)
    fill_rows(far_ref, near_ref.shape[0])


def edge_setup_kernel(velocity_hbm, list_hbm, dual_hbm, edges_ref, scale_ref, outer_matrix_ref, rest_matrix_ref, velocity_ref, list_ref, dual_ref, sems):
    lists, velocity, dual = start_fetch([(list_hbm, list_ref), (velocity_hbm, velocity_ref), (dual_hbm, dual_ref)], sems)
    levels, _, edges = velocity_ref.shape
    edges_ref[...] = jnp.zeros(edges_ref.shape, f32)
    scale_ref[...] = jnp.zeros(scale_ref.shape, f32)
    lists.wait()
    fill_sent(outer_matrix_ref, list_ref, OUTER_SENT)
    fill_sent(rest_matrix_ref, list_ref, REST_SENT)
    velocity.wait()
    dual.wait()
    edges_ref[0:levels, 0:edges] = velocity_ref[:, 0, :]
    scale_ref[:, 0:edges] = STEP_SCALE * dual_ref[...]


def weight_kernel(
    sides_hbm, weight_hbm, near_high_ref, near_low_ref, far_high_ref, far_low_ref, sides_ref, weight_ref, sems, *, edges, edge_pad, halo, lat_count
):
    fetch([(sides_hbm, sides_ref), (weight_hbm, weight_ref)], sems)
    cells = sides_ref.shape[2]
    place = [local_positions(sides_ref[i], edges, edge_pad, halo, lat_count) for i in range(3)]
    weight = [weight_ref[i] for i in range(3)]
    for later in (1, 2):
        for earlier in range(later):
            same = place[later] == place[earlier]
            weight[earlier] = weight[earlier] + jnp.where(same, weight[later], 0.0)
            weight[later] = jnp.where(same, 0.0, weight[later])
            place[later] = jnp.where(same, -1, place[later])
    high = [value.astype(bf16) for value in weight]
    low = [(value - top.astype(f32)).astype(bf16) for value, top in zip(weight, high)]
    place = [value.astype(i16) for value in place]
    zero = jnp.zeros((), bf16)

    def fill_rows(high_ref, low_ref, base):
        def body(first, block):
            row = row_numbers(first + base, block, cells)
            hits = [row == value for value in place]
            for target, values in ((high_ref, high), (low_ref, low)):
                entry = jnp.where(hits[0], values[0], jnp.where(hits[1], values[1], jnp.where(hits[2], values[2], zero)))
                target[pl.ds(first, block), :] = entry

        by_blocks(high_ref.shape[0], body)

    fill_rows(near_high_ref, near_low_ref, 0)
    fill_rows(far_high_ref, far_low_ref, near_high_ref.shape[0])


def cell_setup_kernel(
    coupling_hbm, list_ref, speed_hbm, speed_ref, inverse_ref, forward_ref, back_ref, outer_matrix_ref, rest_matrix_ref, coupling_ref, column_ref, sems
):
    coupling, speed = start_fetch([(coupling_hbm, coupling_ref), (speed_hbm, speed_ref)], sems)
    levels, _, cells = coupling_ref.shape
    fill_sent(outer_matrix_ref, list_ref, OUTER_SENT)
    fill_sent(rest_matrix_ref, list_ref, REST_SENT)
    coupling.wait()
    speed.wait()
    step = column_ref.shape[0] // round_up(levels, 16)
    column_ref[...] = jnp.zeros(column_ref.shape, f32)
    for group in range(cells // LANES):
        column_ref[pl.ds(group, levels, stride=step), :] = coupling_ref[:, 0, group * LANES : (group + 1) * LANES]
    at = lambda level: slice(level * step, (level + 1) * step)
    above = column_ref[at(0), :]
    inverse = 1.0 / (1.0 + above)
    inverse_ref[at(0), :] = inverse
    ratio = above * inverse
    back_ref[at(0), :] = ratio
    for level in range(1, levels):
        below = above
        above = column_ref[at(level), :]
        inverse = 1.0 / (1.0 + below + above - below * ratio)
        inverse_ref[at(level), :] = inverse
        forward_ref[at(level), :] = below * inverse
        ratio = above * inverse
        back_ref[at(level), :] = ratio


def part_kernel(own_ref, inner_ref, outer_ref, *rest):
    *matrix_refs, total_ref, stack_ref = rest
    rows, width = own_ref.shape
    halo = inner_ref.shape[2]
    put_parts(stack_ref, own_ref[...], 0)
    put_parts(stack_ref, inner_ref[0], width)
    put_parts(stack_ref, outer_ref[0], width + halo)
    total_ref[...] = gather_matmul(stack_ref, [ref[...] for ref in matrix_refs], rows)


def early_part_kernel(own_ref, inner_ref, outer_ref, early_ref, *rest):
    *matrix_refs, total_ref, stack_ref, early_stack_ref = rest
    near_refs, far_refs = matrix_refs[: len(matrix_refs) // 2], matrix_refs[len(matrix_refs) // 2 :]
    part_kernel(own_ref, inner_ref, outer_ref, *near_refs, total_ref, stack_ref)
    total_ref[...] = lat_share(total_ref, early_ref, far_refs, early_stack_ref, 3)


def lat_share(total_ref, lat_ref, matrix_refs, stack_ref, first):
    rows = total_ref.shape[0]
    count, _, halo = lat_ref.shape
    for member in range(count):
        put_parts(stack_ref, lat_ref[member], member * halo)
    matrices = [ref[first * halo : (first + count) * halo, :] for ref in matrix_refs]
    return total_ref[...] + gather_matmul(stack_ref, matrices, rows)


def inner_share_kernel(total_ref, lat_inner_ref, *rest):
    *matrix_refs, new_total_ref, stack_ref = rest
    new_total_ref[...] = lat_share(total_ref, lat_inner_ref, matrix_refs, stack_ref, 0)


def edge_kernel(total_ref, lat_outer_ref, far_ref, edges_ref, scale_ref, matrix_ref, new_edges_ref, outer_ref, own_stack_ref, stack_ref):
    rows = edges_ref.shape[0]
    difference = lat_share(total_ref, lat_outer_ref, [far_ref], stack_ref, 6 - lat_outer_ref.shape[0])
    new_edges = edges_ref[...] - scale_ref[...] * difference
    new_edges_ref[...] = new_edges
    put_parts(own_stack_ref, new_edges, 0)
    store_outer(gather_matmul(own_stack_ref, [matrix_ref[...]], rows), outer_ref)


def solve_columns(total_ref, lat_outer_ref, high_ref, low_ref, cells_ref, speed_ref, inverse_ref, forward_ref, back_ref, levels, stack_ref, column_ref):
    rows, cells = cells_ref.shape
    divergence = lat_share(total_ref, lat_outer_ref, [high_ref, low_ref], stack_ref, 6 - lat_outer_ref.shape[0])
    right_side = cells_ref[...] - speed_ref[...] * divergence
    step = column_ref.shape[0] // rows
    for group in range(cells // LANES):
        column_ref[pl.ds(group, rows, stride=step), :] = right_side[:, group * LANES : (group + 1) * LANES]
    for group in range(cells // LANES, step):
        column_ref[pl.ds(group, rows, stride=step), :] = jnp.zeros((rows, LANES), f32)
    at = lambda level: slice(level * step, (level + 1) * step)
    current = column_ref[at(0), :] * inverse_ref[at(0), :]
    scaled = [current]
    for level in range(1, levels):
        current = column_ref[at(level), :] * inverse_ref[at(level), :] + forward_ref[at(level), :] * current
        scaled.append(current)
    column_ref[at(levels - 1), :] = current
    for level in range(levels - 2, -1, -1):
        current = scaled[level] + back_ref[at(level), :] * current
        column_ref[at(level), :] = current
    for level in range(levels, rows):
        column_ref[at(level), :] = jnp.zeros_like(current)


def solved(column_ref, group, rows):
    return column_ref[pl.ds(group, rows, stride=column_ref.shape[0] // rows), :]


def cell_kernel(
    total_ref,
    lat_outer_ref,
    high_ref,
    low_ref,
    cells_ref,
    speed_ref,
    inverse_ref,
    forward_ref,
    back_ref,
    matrix_ref,
    new_cells_ref,
    outer_ref,
    own_stack_ref,
    stack_ref,
    column_ref,
    *,
    levels,
):
    rows, cells = cells_ref.shape
    solve_columns(total_ref, lat_outer_ref, high_ref, low_ref, cells_ref, speed_ref, inverse_ref, forward_ref, back_ref, levels, stack_ref, column_ref)
    for group in range(cells // LANES):
        part = solved(column_ref, group, rows)
        new_cells_ref[:, group * LANES : (group + 1) * LANES] = part
        put_parts(own_stack_ref, part, group * LANES)
    store_outer(gather_matmul(own_stack_ref, [matrix_ref[...]], rows), outer_ref)


def last_kernel(
    total_ref, lat_outer_ref, high_ref, low_ref, cells_ref, speed_ref, inverse_ref, forward_ref, back_ref, out_ref, stack_ref, column_ref, *, levels
):
    rows, cells = cells_ref.shape
    solve_columns(total_ref, lat_outer_ref, high_ref, low_ref, cells_ref, speed_ref, inverse_ref, forward_ref, back_ref, levels, stack_ref, column_ref)
    for group in range(cells // LANES):
        out_ref[:, 0, group * LANES : (group + 1) * LANES] = solved(column_ref, group, rows)[0:levels]


def call(body, outs, scratch, *operands, raw=(), copies=0):
    in_vmem = pl.BlockSpec(memory_space=pltpu.VMEM)
    in_hbm = pl.BlockSpec(memory_space=pltpu.HBM)
    scratch_shapes = [pltpu.VMEM(shape, kind) for shape, kind in scratch]
    if copies:
        scratch_shapes.append(pltpu.SemaphoreType.DMA((copies,)))
    operands = [pltpu.with_memory_space_constraint(x, pltpu.HBM) if i in raw else x for i, x in enumerate(operands)]
    return pl.pallas_call(
        body,
        out_shape=tuple(jax.ShapeDtypeStruct(shape, kind) for shape, kind in outs),
        in_specs=[in_hbm if i in raw else in_vmem for i in range(len(operands))],
        out_specs=tuple(in_vmem for _ in outs),
        scratch_shapes=scratch_shapes,
        compiler_params=pltpu.CompilerParams(vmem_limit_bytes=24 * 1024 * 1024),
    )(*operands)


def on_device(lat_count, lon_count, pressure, velocity, edge_cells, cell_edges, send_cells, send_edges, inv_dual, edge_weight, sound_speed, coupling):
    _, levels, cells = pressure.shape
    edges = velocity.shape[2]
    halo = send_cells.shape[2]
    rows = round_up(levels, 16)
    edge_pad = round_up(edges, 2 * LANES)
    bundle = ((3, rows, halo), f32)
    straight = ((rows, halo), f32)
    lon_routes = swap_routes(lon_count)
    lat_inner_route = swap_routes(lat_count)[0]
    lat_outer_route = lat_outer_routes(lat_count, lon_count)
    i32 = jnp.int32

    by_level = lambda value: value.transpose(1, 0, 2)
    stack_cells = ((PARTS * rows, cells), bf16)
    stack_edges = ((PARTS * rows, edge_pad), bf16)
    stack_lat = lambda count: ((PARTS * rows, count * halo), bf16)
    column = ((rows * round_up(cells // LANES, 8), LANES), f32)
    sent_outer = lambda width: ((width, 3 * halo), bf16)
    sent_rest = lambda width: ((width, 5 * halo), bf16)

    for phase in range(2 * NSUB):
        at_cells = phase % 2 == 0
        if phase == 0:
            values, stack, outer, cell_list = call(
                start_kernel,
                [((rows, cells), f32), stack_cells, bundle, (send_cells.shape[1:], i32)],
                [((levels, 1, cells), f32), sent_outer(cells)],
                by_level(pressure),
                send_cells[0],
                raw=(0, 1),
                copies=2,
            )
        outer_in = lax.ppermute(outer, "lon", lon_routes[1])
        if phase == 0:
            inner, lat_inner, lat_outer = call(first_rest_kernel, [bundle, straight, straight], [sent_rest(cells)], stack, cell_list)
        else:
            inner, lat_inner, lat_outer = call(rest_kernel, [bundle, straight, straight], [], stack, cell_rest if at_cells else edge_rest)
        inner_in = lax.ppermute(inner, "lon", lon_routes[0])
        if phase == 0:
            gradient_near, gradient_far = call(
                functools.partial(gradient_kernel, cells=cells, halo=halo, lat_count=lat_count),
                [((cells + 2 * halo, edge_pad), bf16), ((6 * halo, edge_pad), bf16)],
                [(edge_cells.shape[1:], i32)],
                edge_cells[0],
                raw=(0,),
                copies=1,
            )
        if phase == 1:
            near_high, near_low, far_high, far_low = call(
                functools.partial(weight_kernel, edges=edges, edge_pad=edge_pad, halo=halo, lat_count=lat_count),
                [((edge_pad + 2 * halo, cells), bf16)] * 2 + [((6 * halo, cells), bf16)] * 2,
                [((3, 1, cells), i32), ((3, 1, cells), f32)],
                by_level(cell_edges),
                by_level(edge_weight),
                raw=(0, 1),
                copies=2,
            )
        early = phase >= 2
        first = jnp.stack([inner_in[1], lat_inner, outer_in[1]])
        if early:
            early_in = lax.ppermute(jnp.stack([inner_in[2], lat_outer]), ("lat", "lon"), lat_outer_route)
            second = outer_in[2:3]
        else:
            second = jnp.stack([inner_in[2], lat_outer, outer_in[2]])
        first_in = lax.ppermute(first, "lat", lat_inner_route)
        second_in = lax.ppermute(second, ("lat", "lon"), lat_outer_route)
        count = second.shape[0]
        if phase == 0:
            normal, scale, edge_outer, edge_rest = call(
                edge_setup_kernel,
                [((rows, edge_pad), f32), ((1, edge_pad), f32), sent_outer(edge_pad), sent_rest(edge_pad)],
                [((levels, 1, edges), f32), (send_edges.shape[1:], i32), ((1, edges), f32)],
                by_level(velocity),
                send_edges[0],
                inv_dual,
                raw=(0, 1, 2),
                copies=3,
            )
        if phase == 1:
            speed, inverse, forward, back, cell_outer, cell_rest = call(
                cell_setup_kernel,
                [((1, cells), f32), column, column, column, sent_outer(cells), sent_rest(cells)],
                [((levels, 1, cells), f32), column],
                by_level(coupling),
                cell_list,
                sound_speed,
                raw=(0, 2),
                copies=2,
            )
        if at_cells:
            (total,) = call(
                early_part_kernel if early else part_kernel,
                [((rows, edge_pad), f32)],
                [((PARTS * rows, cells + 2 * halo), bf16)] + ([stack_lat(2)] if early else []),
                values,
                inner_in,
                outer_in,
                *([early_in, gradient_near, gradient_far] if early else [gradient_near]),
            )
            (total,) = call(inner_share_kernel, [((rows, edge_pad), f32)], [stack_lat(3)], total, first_in, gradient_far)
            normal, outer, stack = call(
                edge_kernel,
                [((rows, edge_pad), f32), bundle, stack_edges],
                [stack_lat(count)],
                total,
                second_in,
                gradient_far,
                normal,
                scale,
                edge_outer,
            )
        else:
            (total,) = call(
                early_part_kernel if early else part_kernel,
                [((rows, cells), f32)],
                [((PARTS * rows, edge_pad + 2 * halo), bf16)] + ([stack_lat(2)] if early else []),
                normal,
                inner_in,
                outer_in,
                *([early_in, near_high, near_low, far_high, far_low] if early else [near_high, near_low]),
            )
            (total,) = call(inner_share_kernel, [((rows, cells), f32)], [stack_lat(3)], total, first_in, far_high, far_low)
            operands = (total, second_in, far_high, far_low, values, speed, inverse, forward, back)
            if phase < 2 * NSUB - 1:
                values, outer, stack = call(
                    functools.partial(cell_kernel, levels=levels),
                    [((rows, cells), f32), bundle, stack_cells],
                    [stack_lat(count), column],
                    *operands,
                    cell_outer,
                )
            else:
                (values,) = call(functools.partial(last_kernel, levels=levels), [((levels, 1, cells), f32)], [stack_lat(count), column], *operands)
    return by_level(values), normal[:levels, :edges][None]


def solution(mesh):
    return jax.shard_map(
        functools.partial(on_device, mesh.shape["lat"], mesh.shape["lon"]),
        mesh=mesh,
        in_specs=(
            P("lat", None, "lon"),
            P("lat", None, "lon"),
            P("lat", None, "lon"),
            P("lat", None, "lon"),
            P("lat", None, "lon"),
            P("lat", None, "lon"),
            P("lat", "lon"),
            P("lat", None, "lon"),
            P("lat", "lon"),
            P("lat", None, "lon"),
        ),
        out_specs=(P("lat", None, "lon"), P("lat", None, "lon")),
        check_vma=False,
    )
```

```python
import functools

import jax
import jax.numpy as jnp
from jax import lax
from jax.experimental import pallas as pl
from jax.experimental.pallas import tpu as pltpu
from jax.sharding import PartitionSpec as P


NSUB = 3
STEP_SCALE = 0.5
LANES = 128
PARTS = 3

f32 = jnp.float32
bf16 = jnp.bfloat16
i16 = jnp.int16


def round_up(value, step):
    return -(-value // step) * step


def swap_routes(count):
    inner = [(i, i ^ 1) for i in range(count)]
    outer = [(i, (((i + 1) ^ 1) - 1) % count) for i in range(count)]
    return inner, outer


def lat_outer_routes(lat_count, lon_count):
    routes = []
    for a, target in swap_routes(lat_count)[1]:
        for b in range(lon_count):
            alone = a in (0, lat_count - 1)
            routes.append((a * lon_count + b, a * lon_count + (b ^ 1) if alone else target * lon_count + b))
    return routes


OUTER_SENT = ((0, 2), (1, 2), (2, 2))
REST_SENT = ((0, 1), (1, 1), (2, 1), (1, 0), (2, 0))


def link_signs():
    lat_inner = 1 - 2 * lax.rem(lax.axis_index("lat"), 2)
    lon_inner = 1 - 2 * lax.rem(lax.axis_index("lon"), 2)
    return lat_inner, lon_inner


def sent_row(member):
    lat_inner, lon_inner = link_signs()
    lat_link, lon_link = member
    p = (0, lat_inner, -lat_inner)[lat_link]
    q = (0, lon_inner, -lon_inner)[lon_link]
    flat = (p + 1) * 3 + (q + 1)
    return flat - jnp.where(flat > 4, 1, 0)


def local_positions(index, own, own_padded, halo, lat_count):
    lat_inner, lon_inner = link_signs()
    a = lax.axis_index("lat")
    beyond = index - own
    piece = lax.div(jnp.maximum(beyond, 0), halo)
    slot = beyond - piece * halo
    flat = piece + jnp.where(piece >= 4, 1, 0)
    p = jnp.where(flat >= 6, 1, jnp.where(flat >= 3, 0, -1))
    q = flat - 3 * (p + 1) - 1
    lon_member = jnp.where(q == 0, 1, jnp.where(q == lon_inner, 0, 2))
    member = jnp.where(p == 0, jnp.minimum(lon_member, 1), jnp.where(p == lat_inner, 2, 5) + lon_member)
    outside = (a + p < 0) | (a + p >= lat_count)
    row = own_padded + member * halo + slot
    return jnp.where(beyond < 0, index, jnp.where(outside, -1, row))


def put_parts(stack_ref, value, start):
    rows, width = value.shape
    rest = value
    for part in range(PARTS):
        piece = rest.astype(bf16)
        stack_ref[part * rows : (part + 1) * rows, start : start + width] = piece
        if part < PARTS - 1:
            rest = rest - piece.astype(f32)


def sum_parts(product, rows):
    total = product[(PARTS - 1) * rows : PARTS * rows]
    for part in range(PARTS - 2, -1, -1):
        total = total + product[part * rows : (part + 1) * rows]
    return total


def gather_matmul(stack_ref, matrices, rows):
    product = None
    for matrix in matrices:
        term = jnp.dot(stack_ref[...], matrix, preferred_element_type=f32)
        product = term if product is None else product + term
    return sum_parts(product, rows)


def start_fetch(pairs, sems):
    copies = [pltpu.make_async_copy(source, target, sems.at[i]) for i, (source, target) in enumerate(pairs)]
    for copy in copies:
        copy.start()
    return copies


def fetch(pairs, sems):
    for copy in start_fetch(pairs, sems):
        copy.wait()


def by_blocks(rows, body):
    block = 64 if rows % 64 == 0 else 16

    def step(i, carry):
        first = pl.multiple_of(i * block, block)
        body(first, block)
        return carry

    lax.fori_loop(0, rows // block, step, 0)


def row_numbers(first, block, width):
    return (lax.broadcasted_iota(jnp.int32, (block, width), 0) + first).astype(i16)


def fill_sent(matrix_ref, list_ref, members):
    rows = matrix_ref.shape[0]
    halo = list_ref.shape[1]
    lanes = [list_ref[pl.ds(sent_row(member), 1), :].astype(i16) for member in members]

    def body(first, block):
        row = row_numbers(first, block, halo)
        for member, index in enumerate(lanes):
            hit = jnp.where(row == index, jnp.ones((), bf16), jnp.zeros((), bf16))
            matrix_ref[pl.ds(first, block), member * halo : (member + 1) * halo] = hit

    by_blocks(rows, body)


def store_outer(pieces, outer_ref):
    halo = outer_ref.shape[2]
    for member in range(3):
        outer_ref[member] = pieces[:, member * halo : (member + 1) * halo]


def store_rest(pieces, inner_ref, lat_inner_ref, lat_outer_ref):
    halo = inner_ref.shape[2]
    for member in range(3):
        inner_ref[member] = pieces[:, member * halo : (member + 1) * halo]
    lat_inner_ref[...] = pieces[:, 3 * halo : 4 * halo]
    lat_outer_ref[...] = pieces[:, 4 * halo : 5 * halo]


def start_kernel(pressure_hbm, list_hbm, cells_ref, stack_ref, outer_ref, lists_ref, pressure_ref, matrix_ref, sems):
    lists, pressure = start_fetch([(list_hbm, lists_ref), (pressure_hbm, pressure_ref)], sems)
    levels = pressure_ref.shape[0]
    rows = cells_ref.shape[0]
    lists.wait()
    fill_sent(matrix_ref, lists_ref, OUTER_SENT)
    pressure.wait()
    cells_ref[0:levels, :] = pressure_ref[:, 0, :]
    cells_ref[levels:rows, :] = jnp.zeros((rows - levels, cells_ref.shape[1]), f32)
    put_parts(stack_ref, cells_ref[...], 0)
    store_outer(gather_matmul(stack_ref, [matrix_ref[...]], rows), outer_ref)


def first_rest_kernel(stack_ref, list_ref, inner_ref, lat_inner_ref, lat_outer_ref, matrix_ref):
    fill_sent(matrix_ref, list_ref, REST_SENT)
    store_rest(gather_matmul(stack_ref, [matrix_ref[...]], inner_ref.shape[1]), inner_ref, lat_inner_ref, lat_outer_ref)


def rest_kernel(stack_ref, matrix_ref, inner_ref, lat_inner_ref, lat_outer_ref):
    store_rest(gather_matmul(stack_ref, [matrix_ref[...]], inner_ref.shape[1]), inner_ref, lat_inner_ref, lat_outer_ref)


def gradient_kernel(edge_cells_hbm, near_ref, far_ref, ends_ref, sems, *, cells, halo, lat_count):
    fetch([(edge_cells_hbm, ends_ref)], sems)
    edges = ends_ref.shape[1]
    edge_pad = near_ref.shape[1]
    ends = local_positions(ends_ref[...], cells, cells, halo, lat_count)
    near, far = ends[0:1, :], ends[1:2, :]
    same = near == far
    near, far = jnp.where(same, -1, near), jnp.where(same, -1, far)
    if edge_pad > edges:
        fill = jnp.full((1, edge_pad - edges), -1, jnp.int32)
        near, far = jnp.concatenate([near, fill], axis=1), jnp.concatenate([far, fill], axis=1)
    near, far = near.astype(i16), far.astype(i16)

    def fill_rows(matrix_ref, base):
        def body(first, block):
            row = row_numbers(first + base, block, edge_pad)
            one = jnp.ones((), bf16)
            matrix_ref[pl.ds(first, block), :] = jnp.where(row == far, one, jnp.where(row == near, -one, jnp.zeros((), bf16)))

        by_blocks(matrix_ref.shape[0], body)

    fill_rows(near_ref, 0)
    fill_rows(far_ref, near_ref.shape[0])


def edge_setup_kernel(velocity_hbm, list_hbm, dual_hbm, edges_ref, scale_ref, outer_matrix_ref, rest_matrix_ref, velocity_ref, list_ref, dual_ref, sems):
    lists, velocity, dual = start_fetch([(list_hbm, list_ref), (velocity_hbm, velocity_ref), (dual_hbm, dual_ref)], sems)
    levels, _, edges = velocity_ref.shape
    edges_ref[...] = jnp.zeros(edges_ref.shape, f32)
    scale_ref[...] = jnp.zeros(scale_ref.shape, f32)
    lists.wait()
    fill_sent(outer_matrix_ref, list_ref, OUTER_SENT)
    fill_sent(rest_matrix_ref, list_ref, REST_SENT)
    velocity.wait()
    dual.wait()
    edges_ref[0:levels, 0:edges] = velocity_ref[:, 0, :]
    scale_ref[:, 0:edges] = STEP_SCALE * dual_ref[...]


def weight_kernel(
    sides_hbm, weight_hbm, near_high_ref, near_low_ref, far_high_ref, far_low_ref, sides_ref, weight_ref, sems, *, edges, edge_pad, halo, lat_count
):
    fetch([(sides_hbm, sides_ref), (weight_hbm, weight_ref)], sems)
    cells = sides_ref.shape[2]
    place = [local_positions(sides_ref[i], edges, edge_pad, halo, lat_count) for i in range(3)]
    weight = [weight_ref[i] for i in range(3)]
    for later in (1, 2):
        for earlier in range(later):
            same = place[later] == place[earlier]
            weight[earlier] = weight[earlier] + jnp.where(same, weight[later], 0.0)
            weight[later] = jnp.where(same, 0.0, weight[later])
            place[later] = jnp.where(same, -1, place[later])
    high = [value.astype(bf16) for value in weight]
    low = [(value - top.astype(f32)).astype(bf16) for value, top in zip(weight, high)]
    place = [value.astype(i16) for value in place]
    zero = jnp.zeros((), bf16)

    def fill_rows(high_ref, low_ref, base):
        def body(first, block):
            row = row_numbers(first + base, block, cells)
            hits = [row == value for value in place]
            for target, values in ((high_ref, high), (low_ref, low)):
                entry = jnp.where(hits[0], values[0], jnp.where(hits[1], values[1], jnp.where(hits[2], values[2], zero)))
                target[pl.ds(first, block), :] = entry

        by_blocks(high_ref.shape[0], body)

    fill_rows(near_high_ref, near_low_ref, 0)
    fill_rows(far_high_ref, far_low_ref, near_high_ref.shape[0])


def cell_setup_kernel(
    coupling_hbm, list_ref, speed_hbm, speed_ref, inverse_ref, forward_ref, back_ref, outer_matrix_ref, rest_matrix_ref, coupling_ref, column_ref, sems
):
    coupling, speed = start_fetch([(coupling_hbm, coupling_ref), (speed_hbm, speed_ref)], sems)
    levels, _, cells = coupling_ref.shape
    fill_sent(outer_matrix_ref, list_ref, OUTER_SENT)
    fill_sent(rest_matrix_ref, list_ref, REST_SENT)
    coupling.wait()
    speed.wait()
    step = column_ref.shape[0] // round_up(levels, 16)
    column_ref[...] = jnp.zeros(column_ref.shape, f32)
    for group in range(cells // LANES):
        column_ref[pl.ds(group, levels, stride=step), :] = coupling_ref[:, 0, group * LANES : (group + 1) * LANES]
    at = lambda level: slice(level * step, (level + 1) * step)
    above = column_ref[at(0), :]
    inverse = 1.0 / (1.0 + above)
    inverse_ref[at(0), :] = inverse
    ratio = above * inverse
    back_ref[at(0), :] = ratio
    for level in range(1, levels):
        below = above
        above = column_ref[at(level), :]
        inverse = 1.0 / (1.0 + below + above - below * ratio)
        inverse_ref[at(level), :] = inverse
        forward_ref[at(level), :] = below * inverse
        ratio = above * inverse
        back_ref[at(level), :] = ratio


def part_kernel(own_ref, inner_ref, outer_ref, *rest):
    *matrix_refs, total_ref, stack_ref = rest
    rows, width = own_ref.shape
    halo = inner_ref.shape[2]
    put_parts(stack_ref, own_ref[...], 0)
    put_parts(stack_ref, inner_ref[0], width)
    put_parts(stack_ref, outer_ref[0], width + halo)
    total_ref[...] = gather_matmul(stack_ref, [ref[...] for ref in matrix_refs], rows)


def early_part_kernel(own_ref, inner_ref, outer_ref, early_ref, *rest):
    *matrix_refs, total_ref, stack_ref, early_stack_ref = rest
    near_refs, far_refs = matrix_refs[: len(matrix_refs) // 2], matrix_refs[len(matrix_refs) // 2 :]
    part_kernel(own_ref, inner_ref, outer_ref, *near_refs, total_ref, stack_ref)
    total_ref[...] = lat_share(total_ref, early_ref, far_refs, early_stack_ref, 3)


def lat_share(total_ref, lat_ref, matrix_refs, stack_ref, first):
    rows = total_ref.shape[0]
    count, _, halo = lat_ref.shape
    for member in range(count):
        put_parts(stack_ref, lat_ref[member], member * halo)
    matrices = [ref[first * halo : (first + count) * halo, :] for ref in matrix_refs]
    return total_ref[...] + gather_matmul(stack_ref, matrices, rows)


def inner_share_kernel(total_ref, lat_inner_ref, *rest):
    *matrix_refs, new_total_ref, stack_ref = rest
    new_total_ref[...] = lat_share(total_ref, lat_inner_ref, matrix_refs, stack_ref, 0)


def edge_kernel(total_ref, lat_outer_ref, far_ref, edges_ref, scale_ref, matrix_ref, new_edges_ref, outer_ref, own_stack_ref, stack_ref):
    rows = edges_ref.shape[0]
    difference = lat_share(total_ref, lat_outer_ref, [far_ref], stack_ref, 6 - lat_outer_ref.shape[0])
    new_edges = edges_ref[...] - scale_ref[...] * difference
    new_edges_ref[...] = new_edges
    put_parts(own_stack_ref, new_edges, 0)
    store_outer(gather_matmul(own_stack_ref, [matrix_ref[...]], rows), outer_ref)


def solve_columns(total_ref, lat_outer_ref, high_ref, low_ref, cells_ref, speed_ref, inverse_ref, forward_ref, back_ref, levels, stack_ref, column_ref):
    rows, cells = cells_ref.shape
    divergence = lat_share(total_ref, lat_outer_ref, [high_ref, low_ref], stack_ref, 6 - lat_outer_ref.shape[0])
    right_side = cells_ref[...] - speed_ref[...] * divergence
    step = column_ref.shape[0] // rows
    for group in range(cells // LANES):
        column_ref[pl.ds(group, rows, stride=step), :] = right_side[:, group * LANES : (group + 1) * LANES]
    for group in range(cells // LANES, step):
        column_ref[pl.ds(group, rows, stride=step), :] = jnp.zeros((rows, LANES), f32)
    at = lambda level: slice(level * step, (level + 1) * step)
    current = column_ref[at(0), :] * inverse_ref[at(0), :]
    scaled = [current]
    for level in range(1, levels):
        current = column_ref[at(level), :] * inverse_ref[at(level), :] + forward_ref[at(level), :] * current
        scaled.append(current)
    column_ref[at(levels - 1), :] = current
    for level in range(levels - 2, -1, -1):
        current = scaled[level] + back_ref[at(level), :] * current
        column_ref[at(level), :] = current
    for level in range(levels, rows):
        column_ref[at(level), :] = jnp.zeros_like(current)


def solved(column_ref, group, rows):
    return column_ref[pl.ds(group, rows, stride=column_ref.shape[0] // rows), :]


def cell_kernel(
    total_ref,
    lat_outer_ref,
    high_ref,
    low_ref,
    cells_ref,
    speed_ref,
    inverse_ref,
    forward_ref,
    back_ref,
    matrix_ref,
    new_cells_ref,
    outer_ref,
    own_stack_ref,
    stack_ref,
    column_ref,
    *,
    levels,
):
    rows, cells = cells_ref.shape
    solve_columns(total_ref, lat_outer_ref, high_ref, low_ref, cells_ref, speed_ref, inverse_ref, forward_ref, back_ref, levels, stack_ref, column_ref)
    for group in range(cells // LANES):
        part = solved(column_ref, group, rows)
        new_cells_ref[:, group * LANES : (group + 1) * LANES] = part
        put_parts(own_stack_ref, part, group * LANES)
    store_outer(gather_matmul(own_stack_ref, [matrix_ref[...]], rows), outer_ref)


def last_kernel(
    total_ref, lat_outer_ref, high_ref, low_ref, cells_ref, speed_ref, inverse_ref, forward_ref, back_ref, out_ref, stack_ref, column_ref, *, levels
):
    rows, cells = cells_ref.shape
    solve_columns(total_ref, lat_outer_ref, high_ref, low_ref, cells_ref, speed_ref, inverse_ref, forward_ref, back_ref, levels, stack_ref, column_ref)
    for group in range(cells // LANES):
        out_ref[:, 0, group * LANES : (group + 1) * LANES] = solved(column_ref, group, rows)[0:levels]


def call(body, outs, scratch, *operands, raw=(), copies=0):
    in_vmem = pl.BlockSpec(memory_space=pltpu.VMEM)
    in_hbm = pl.BlockSpec(memory_space=pltpu.HBM)
    scratch_shapes = [pltpu.VMEM(shape, kind) for shape, kind in scratch]
    if copies:
        scratch_shapes.append(pltpu.SemaphoreType.DMA((copies,)))
    operands = [pltpu.with_memory_space_constraint(x, pltpu.HBM) if i in raw else x for i, x in enumerate(operands)]
    return pl.pallas_call(
        body,
        out_shape=tuple(jax.ShapeDtypeStruct(shape, kind) for shape, kind in outs),
        in_specs=[in_hbm if i in raw else in_vmem for i in range(len(operands))],
        out_specs=tuple(in_vmem for _ in outs),
        scratch_shapes=scratch_shapes,
        compiler_params=pltpu.CompilerParams(vmem_limit_bytes=24 * 1024 * 1024),
    )(*operands)


def on_device(lat_count, lon_count, pressure, velocity, edge_cells, cell_edges, send_cells, send_edges, inv_dual, edge_weight, sound_speed, coupling):
    _, levels, cells = pressure.shape
    edges = velocity.shape[2]
    halo = send_cells.shape[2]
    rows = round_up(levels, 16)
    edge_pad = round_up(edges, 2 * LANES)
    bundle = ((3, rows, halo), f32)
    straight = ((rows, halo), f32)
    lon_routes = swap_routes(lon_count)
    lat_inner_route = swap_routes(lat_count)[0]
    lat_outer_route = lat_outer_routes(lat_count, lon_count)
    i32 = jnp.int32

    by_level = lambda value: value.transpose(1, 0, 2)
    stack_cells = ((PARTS * rows, cells), bf16)
    stack_edges = ((PARTS * rows, edge_pad), bf16)
    stack_lat = lambda count: ((PARTS * rows, count * halo), bf16)
    column = ((rows * round_up(cells // LANES, 8), LANES), f32)
    sent_outer = lambda width: ((width, 3 * halo), bf16)
    sent_rest = lambda width: ((width, 5 * halo), bf16)

    for phase in range(2 * NSUB):
        at_cells = phase % 2 == 0
        if phase == 0:
            values, stack, outer, cell_list = call(
                start_kernel,
                [((rows, cells), f32), stack_cells, bundle, (send_cells.shape[1:], i32)],
                [((levels, 1, cells), f32), sent_outer(cells)],
                by_level(pressure),
                send_cells[0],
                raw=(0, 1),
                copies=2,
            )
        outer_in = lax.ppermute(outer, "lon", lon_routes[1])
        if phase == 0:
            inner, lat_inner, lat_outer = call(first_rest_kernel, [bundle, straight, straight], [sent_rest(cells)], stack, cell_list)
        else:
            inner, lat_inner, lat_outer = call(rest_kernel, [bundle, straight, straight], [], stack, cell_rest if at_cells else edge_rest)
        inner_in = lax.ppermute(inner, "lon", lon_routes[0])
        if phase == 0:
            gradient_near, gradient_far = call(
                functools.partial(gradient_kernel, cells=cells, halo=halo, lat_count=lat_count),
                [((cells + 2 * halo, edge_pad), bf16), ((6 * halo, edge_pad), bf16)],
                [(edge_cells.shape[1:], i32)],
                edge_cells[0],
                raw=(0,),
                copies=1,
            )
        if phase == 1:
            near_high, near_low, far_high, far_low = call(
                functools.partial(weight_kernel, edges=edges, edge_pad=edge_pad, halo=halo, lat_count=lat_count),
                [((edge_pad + 2 * halo, cells), bf16)] * 2 + [((6 * halo, cells), bf16)] * 2,
                [((3, 1, cells), i32), ((3, 1, cells), f32)],
                by_level(cell_edges),
                by_level(edge_weight),
                raw=(0, 1),
                copies=2,
            )
        early_in = lax.ppermute(jnp.stack([inner_in[2], lat_outer]), ("lat", "lon"), lat_outer_route)
        first_in = lax.ppermute(jnp.stack([inner_in[1], lat_inner, outer_in[1]]), "lat", lat_inner_route)
        second_in = lax.ppermute(outer_in[2:3], ("lat", "lon"), lat_outer_route)
        if phase == 0:
            normal, scale, edge_outer, edge_rest = call(
                edge_setup_kernel,
                [((rows, edge_pad), f32), ((1, edge_pad), f32), sent_outer(edge_pad), sent_rest(edge_pad)],
                [((levels, 1, edges), f32), (send_edges.shape[1:], i32), ((1, edges), f32)],
                by_level(velocity),
                send_edges[0],
                inv_dual,
                raw=(0, 1, 2),
                copies=3,
            )
        if phase == 1:
            speed, inverse, forward, back, cell_outer, cell_rest = call(
                cell_setup_kernel,
                [((1, cells), f32), column, column, column, sent_outer(cells), sent_rest(cells)],
                [((levels, 1, cells), f32), column],
                by_level(coupling),
                cell_list,
                sound_speed,
                raw=(0, 2),
                copies=2,
            )
        if at_cells:
            (total,) = call(
                early_part_kernel,
                [((rows, edge_pad), f32)],
                [((PARTS * rows, cells + 2 * halo), bf16)] + [stack_lat(2)],
                values,
                inner_in,
                outer_in,
                early_in,
                gradient_near,
                gradient_far,
            )
            (total,) = call(inner_share_kernel, [((rows, edge_pad), f32)], [stack_lat(3)], total, first_in, gradient_far)
            normal, outer, stack = call(
                edge_kernel,
                [((rows, edge_pad), f32), bundle, stack_edges],
                [stack_lat(1)],
                total,
                second_in,
                gradient_far,
                normal,
                scale,
                edge_outer,
            )
        else:
            (total,) = call(
                early_part_kernel,
                [((rows, cells), f32)],
                [((PARTS * rows, edge_pad + 2 * halo), bf16)] + [stack_lat(2)],
                normal,
                inner_in,
                outer_in,
                early_in,
                near_high,
                near_low,
                far_high,
                far_low,
            )
            (total,) = call(inner_share_kernel, [((rows, cells), f32)], [stack_lat(3)], total, first_in, far_high, far_low)
            operands = (total, second_in, far_high, far_low, values, speed, inverse, forward, back)
            if phase < 2 * NSUB - 1:
                values, outer, stack = call(
                    functools.partial(cell_kernel, levels=levels),
                    [((rows, cells), f32), bundle, stack_cells],
                    [stack_lat(1), column],
                    *operands,
                    cell_outer,
                )
            else:
                (values,) = call(functools.partial(last_kernel, levels=levels), [((levels, 1, cells), f32)], [stack_lat(1), column], *operands)
    return by_level(values), normal[:levels, :edges][None]


def solution(mesh):
    return jax.shard_map(
        functools.partial(on_device, mesh.shape["lat"], mesh.shape["lon"]),
        mesh=mesh,
        in_specs=(
            P("lat", None, "lon"),
            P("lat", None, "lon"),
            P("lat", None, "lon"),
            P("lat", None, "lon"),
            P("lat", None, "lon"),
            P("lat", None, "lon"),
            P("lat", "lon"),
            P("lat", None, "lon"),
            P("lat", "lon"),
            P("lat", None, "lon"),
        ),
        out_specs=(P("lat", None, "lon"), P("lat", None, "lon")),
        check_vma=False,
    )
```

```python
import functools

import jax
import jax.numpy as jnp
from jax import lax
from jax.experimental import pallas as pl
from jax.experimental.pallas import tpu as pltpu
from jax.sharding import PartitionSpec as P


NSUB = 3
STEP_SCALE = 0.5
LANES = 128
PARTS = 3

f32 = jnp.float32
bf16 = jnp.bfloat16
i16 = jnp.int16


def round_up(value, step):
    return -(-value // step) * step


def swap_routes(count):
    inner = [(i, i ^ 1) for i in range(count)]
    outer = [(i, (((i + 1) ^ 1) - 1) % count) for i in range(count)]
    return inner, outer


def lat_outer_routes(lat_count, lon_count):
    routes = []
    for a, target in swap_routes(lat_count)[1]:
        for b in range(lon_count):
            alone = a in (0, lat_count - 1)
            routes.append((a * lon_count + b, a * lon_count + (b ^ 1) if alone else target * lon_count + b))
    return routes


OUTER_SENT = ((0, 2), (1, 2), (2, 2))
REST_SENT = ((0, 1), (1, 1), (2, 1), (1, 0), (2, 0))


def link_signs():
    lat_inner = 1 - 2 * lax.rem(lax.axis_index("lat"), 2)
    lon_inner = 1 - 2 * lax.rem(lax.axis_index("lon"), 2)
    return lat_inner, lon_inner


def sent_row(member):
    lat_inner, lon_inner = link_signs()
    lat_link, lon_link = member
    p = (0, lat_inner, -lat_inner)[lat_link]
    q = (0, lon_inner, -lon_inner)[lon_link]
    flat = (p + 1) * 3 + (q + 1)
    return flat - jnp.where(flat > 4, 1, 0)


def local_positions(index, own, own_padded, halo, lat_count):
    lat_inner, lon_inner = link_signs()
    a = lax.axis_index("lat")
    beyond = index - own
    piece = lax.div(jnp.maximum(beyond, 0), halo)
    slot = beyond - piece * halo
    flat = piece + jnp.where(piece >= 4, 1, 0)
    p = jnp.where(flat >= 6, 1, jnp.where(flat >= 3, 0, -1))
    q = flat - 3 * (p + 1) - 1
    lon_member = jnp.where(q == 0, 1, jnp.where(q == lon_inner, 0, 2))
    member = jnp.where(p == 0, jnp.minimum(lon_member, 1), jnp.where(p == lat_inner, 2, 5) + lon_member)
    outside = (a + p < 0) | (a + p >= lat_count)
    row = own_padded + member * halo + slot
    return jnp.where(beyond < 0, index, jnp.where(outside, -1, row))


def put_parts(stack_ref, value, start):
    rows, width = value.shape
    rest = value
    for part in range(PARTS):
        piece = rest.astype(bf16)
        stack_ref[part * rows : (part + 1) * rows, start : start + width] = piece
        if part < PARTS - 1:
            rest = rest - piece.astype(f32)


def sum_parts(product, rows):
    total = product[(PARTS - 1) * rows : PARTS * rows]
    for part in range(PARTS - 2, -1, -1):
        total = total + product[part * rows : (part + 1) * rows]
    return total


def gather_matmul(stack_ref, matrices, rows):
    product = None
    for matrix in matrices:
        term = jnp.dot(stack_ref[...], matrix, preferred_element_type=f32)
        product = term if product is None else product + term
    return sum_parts(product, rows)


def start_fetch(pairs, sems):
    copies = [pltpu.make_async_copy(source, target, sems.at[i]) for i, (source, target) in enumerate(pairs)]
    for copy in copies:
        copy.start()
    return copies


def fetch(pairs, sems):
    for copy in start_fetch(pairs, sems):
        copy.wait()


def by_blocks(rows, body):
    block = 64 if rows % 64 == 0 else 16

    def step(i, carry):
        first = pl.multiple_of(i * block, block)
        body(first, block)
        return carry

    lax.fori_loop(0, rows // block, step, 0)


def row_numbers(first, block, width):
    return (lax.broadcasted_iota(jnp.int32, (block, width), 0) + first).astype(i16)


def fill_sent(matrix_ref, list_ref, members):
    rows = matrix_ref.shape[0]
    halo = list_ref.shape[1]
    lanes = [list_ref[pl.ds(sent_row(member), 1), :].astype(i16) for member in members]

    def body(first, block):
        row = row_numbers(first, block, halo)
        for member, index in enumerate(lanes):
            hit = jnp.where(row == index, jnp.ones((), bf16), jnp.zeros((), bf16))
            matrix_ref[pl.ds(first, block), member * halo : (member + 1) * halo] = hit

    by_blocks(rows, body)


def store_outer(pieces, outer_ref):
    halo = outer_ref.shape[2]
    for member in range(3):
        outer_ref[member] = pieces[:, member * halo : (member + 1) * halo]


def store_rest(pieces, inner_ref, lat_inner_ref, lat_outer_ref):
    halo = inner_ref.shape[2]
    for member in range(3):
        inner_ref[member] = pieces[:, member * halo : (member + 1) * halo]
    lat_inner_ref[...] = pieces[:, 3 * halo : 4 * halo]
    lat_outer_ref[...] = pieces[:, 4 * halo : 5 * halo]


def start_kernel(pressure_hbm, list_hbm, cells_ref, stack_ref, outer_ref, lists_ref, pressure_ref, matrix_ref, sems):
    lists, pressure = start_fetch([(list_hbm, lists_ref), (pressure_hbm, pressure_ref)], sems)
    levels = pressure_ref.shape[0]
    rows = cells_ref.shape[0]
    lists.wait()
    fill_sent(matrix_ref, lists_ref, OUTER_SENT)
    pressure.wait()
    cells_ref[0:levels, :] = pressure_ref[:, 0, :]
    cells_ref[levels:rows, :] = jnp.zeros((rows - levels, cells_ref.shape[1]), f32)
    put_parts(stack_ref, cells_ref[...], 0)
    store_outer(gather_matmul(stack_ref, [matrix_ref[...]], rows), outer_ref)


def first_rest_kernel(stack_ref, list_ref, inner_ref, lat_inner_ref, lat_outer_ref, matrix_ref):
    fill_sent(matrix_ref, list_ref, REST_SENT)
    store_rest(gather_matmul(stack_ref, [matrix_ref[...]], inner_ref.shape[1]), inner_ref, lat_inner_ref, lat_outer_ref)


def rest_kernel(stack_ref, matrix_ref, inner_ref, lat_inner_ref, lat_outer_ref):
    store_rest(gather_matmul(stack_ref, [matrix_ref[...]], inner_ref.shape[1]), inner_ref, lat_inner_ref, lat_outer_ref)


def gradient_kernel(edge_cells_hbm, near_ref, far_ref, ends_ref, sems, *, cells, halo, lat_count):
    fetch([(edge_cells_hbm, ends_ref)], sems)
    edges = ends_ref.shape[1]
    edge_pad = near_ref.shape[1]
    ends = local_positions(ends_ref[...], cells, cells, halo, lat_count)
    near, far = ends[0:1, :], ends[1:2, :]
    same = near == far
    near, far = jnp.where(same, -1, near), jnp.where(same, -1, far)
    if edge_pad > edges:
        fill = jnp.full((1, edge_pad - edges), -1, jnp.int32)
        near, far = jnp.concatenate([near, fill], axis=1), jnp.concatenate([far, fill], axis=1)
    near, far = near.astype(i16), far.astype(i16)

    def fill_rows(matrix_ref, base):
        def body(first, block):
            row = row_numbers(first + base, block, edge_pad)
            one = jnp.ones((), bf16)
            matrix_ref[pl.ds(first, block), :] = jnp.where(row == far, one, jnp.where(row == near, -one, jnp.zeros((), bf16)))

        by_blocks(matrix_ref.shape[0], body)

    fill_rows(near_ref, 0)
    fill_rows(far_ref, near_ref.shape[0])


def edge_setup_kernel(
    velocity_hbm, list_hbm, dual_hbm, far_ref, edges_ref, scale_ref, outer_matrix_ref, rest_matrix_ref, late_ref, sent_scale_ref, velocity_ref, list_ref, dual_ref, stack_ref, sems
):
    lists, velocity, dual = start_fetch([(list_hbm, list_ref), (velocity_hbm, velocity_ref), (dual_hbm, dual_ref)], sems)
    levels, _, edges = velocity_ref.shape
    edges_ref[...] = jnp.zeros(edges_ref.shape, f32)
    scale_ref[...] = jnp.zeros(scale_ref.shape, f32)
    lists.wait()
    fill_sent(outer_matrix_ref, list_ref, OUTER_SENT)
    fill_sent(rest_matrix_ref, list_ref, REST_SENT)
    velocity.wait()
    dual.wait()
    edges_ref[0:levels, 0:edges] = velocity_ref[:, 0, :]
    scale_ref[:, 0:edges] = STEP_SCALE * dual_ref[...]
    late = far_ref[far_ref.shape[0] - late_ref.shape[0] :, :]
    late_ref[...] = jnp.dot(late, outer_matrix_ref[...], preferred_element_type=f32).astype(bf16)
    rows = stack_ref.shape[0] // PARTS
    put_parts(stack_ref, jnp.broadcast_to(scale_ref[...], (rows, scale_ref.shape[1])), 0)
    sent_scale_ref[...] = gather_matmul(stack_ref, [outer_matrix_ref[...]], rows)[0:1]


def weight_kernel(
    sides_hbm, weight_hbm, near_high_ref, near_low_ref, far_high_ref, far_low_ref, sides_ref, weight_ref, sems, *, edges, edge_pad, halo, lat_count
):
    fetch([(sides_hbm, sides_ref), (weight_hbm, weight_ref)], sems)
    cells = sides_ref.shape[2]
    place = [local_positions(sides_ref[i], edges, edge_pad, halo, lat_count) for i in range(3)]
    weight = [weight_ref[i] for i in range(3)]
    for later in (1, 2):
        for earlier in range(later):
            same = place[later] == place[earlier]
            weight[earlier] = weight[earlier] + jnp.where(same, weight[later], 0.0)
            weight[later] = jnp.where(same, 0.0, weight[later])
            place[later] = jnp.where(same, -1, place[later])
    high = [value.astype(bf16) for value in weight]
    low = [(value - top.astype(f32)).astype(bf16) for value, top in zip(weight, high)]
    place = [value.astype(i16) for value in place]
    zero = jnp.zeros((), bf16)

    def fill_rows(high_ref, low_ref, base):
        def body(first, block):
            row = row_numbers(first + base, block, cells)
            hits = [row == value for value in place]
            for target, values in ((high_ref, high), (low_ref, low)):
                entry = jnp.where(hits[0], values[0], jnp.where(hits[1], values[1], jnp.where(hits[2], values[2], zero)))
                target[pl.ds(first, block), :] = entry

        by_blocks(high_ref.shape[0], body)

    fill_rows(near_high_ref, near_low_ref, 0)
    fill_rows(far_high_ref, far_low_ref, near_high_ref.shape[0])


def cell_setup_kernel(
    coupling_hbm, list_ref, speed_hbm, speed_ref, inverse_ref, forward_ref, back_ref, outer_matrix_ref, rest_matrix_ref, coupling_ref, column_ref, sems
):
    coupling, speed = start_fetch([(coupling_hbm, coupling_ref), (speed_hbm, speed_ref)], sems)
    levels, _, cells = coupling_ref.shape
    fill_sent(outer_matrix_ref, list_ref, OUTER_SENT)
    fill_sent(rest_matrix_ref, list_ref, REST_SENT)
    coupling.wait()
    speed.wait()
    step = column_ref.shape[0] // round_up(levels, 16)
    column_ref[...] = jnp.zeros(column_ref.shape, f32)
    for group in range(cells // LANES):
        column_ref[pl.ds(group, levels, stride=step), :] = coupling_ref[:, 0, group * LANES : (group + 1) * LANES]
    at = lambda level: slice(level * step, (level + 1) * step)
    above = column_ref[at(0), :]
    inverse = 1.0 / (1.0 + above)
    inverse_ref[at(0), :] = inverse
    ratio = above * inverse
    back_ref[at(0), :] = ratio
    for level in range(1, levels):
        below = above
        above = column_ref[at(level), :]
        inverse = 1.0 / (1.0 + below + above - below * ratio)
        inverse_ref[at(level), :] = inverse
        forward_ref[at(level), :] = below * inverse
        ratio = above * inverse
        back_ref[at(level), :] = ratio


def part_kernel(own_ref, inner_ref, outer_ref, *rest):
    *matrix_refs, total_ref, stack_ref = rest
    rows, width = own_ref.shape
    halo = inner_ref.shape[2]
    put_parts(stack_ref, own_ref[...], 0)
    put_parts(stack_ref, inner_ref[0], width)
    put_parts(stack_ref, outer_ref[0], width + halo)
    total_ref[...] = gather_matmul(stack_ref, [ref[...] for ref in matrix_refs], rows)


def early_part_kernel(own_ref, inner_ref, outer_ref, early_ref, *rest):
    *matrix_refs, total_ref, stack_ref, early_stack_ref = rest
    near_refs, far_refs = matrix_refs[: len(matrix_refs) // 2], matrix_refs[len(matrix_refs) // 2 :]
    part_kernel(own_ref, inner_ref, outer_ref, *near_refs, total_ref, stack_ref)
    total_ref[...] = lat_share(total_ref, early_ref, far_refs, early_stack_ref, 3)


def lat_share(total_ref, lat_ref, matrix_refs, stack_ref, first):
    rows = total_ref.shape[0]
    count, _, halo = lat_ref.shape
    for member in range(count):
        put_parts(stack_ref, lat_ref[member], member * halo)
    matrices = [ref[first * halo : (first + count) * halo, :] for ref in matrix_refs]
    return total_ref[...] + gather_matmul(stack_ref, matrices, rows)


def inner_share_kernel(total_ref, lat_inner_ref, *rest):
    *matrix_refs, new_total_ref, stack_ref = rest
    new_total_ref[...] = lat_share(total_ref, lat_inner_ref, matrix_refs, stack_ref, 0)


def sent_base_kernel(total_ref, lat_inner_ref, far_ref, edges_ref, scale_ref, matrix_ref, new_total_ref, base_ref, stack_ref, own_stack_ref):
    total = lat_share(total_ref, lat_inner_ref, [far_ref], stack_ref, 0)
    new_total_ref[...] = total
    put_parts(own_stack_ref, edges_ref[...] - scale_ref[...] * total, 0)
    base_ref[...] = gather_matmul(own_stack_ref, [matrix_ref[...]], total_ref.shape[0])


def edge_sent_kernel(base_ref, lat_outer_ref, late_ref, sent_scale_ref, outer_ref, stack_ref):
    rows = base_ref.shape[0]
    count, _, halo = lat_outer_ref.shape
    for member in range(count):
        put_parts(stack_ref, lat_outer_ref[member], member * halo)
    late = late_ref[late_ref.shape[0] - count * halo :, :]
    store_outer(base_ref[...] - sent_scale_ref[...] * gather_matmul(stack_ref, [late], rows), outer_ref)


def edge_rest_kernel(total_ref, lat_outer_ref, far_ref, edges_ref, scale_ref, matrix_ref, new_edges_ref, inner_ref, lat_inner_ref, lat_outer_out_ref, stack_ref, own_stack_ref):
    difference = lat_share(total_ref, lat_outer_ref, [far_ref], stack_ref, 6 - lat_outer_ref.shape[0])
    new_edges = edges_ref[...] - scale_ref[...] * difference
    new_edges_ref[...] = new_edges
    put_parts(own_stack_ref, new_edges, 0)
    store_rest(gather_matmul(own_stack_ref, [matrix_ref[...]], edges_ref.shape[0]), inner_ref, lat_inner_ref, lat_outer_out_ref)


def solve_columns(total_ref, lat_outer_ref, high_ref, low_ref, cells_ref, speed_ref, inverse_ref, forward_ref, back_ref, levels, stack_ref, column_ref):
    rows, cells = cells_ref.shape
    divergence = lat_share(total_ref, lat_outer_ref, [high_ref, low_ref], stack_ref, 6 - lat_outer_ref.shape[0])
    right_side = cells_ref[...] - speed_ref[...] * divergence
    step = column_ref.shape[0] // rows
    for group in range(cells // LANES):
        column_ref[pl.ds(group, rows, stride=step), :] = right_side[:, group * LANES : (group + 1) * LANES]
    for group in range(cells // LANES, step):
        column_ref[pl.ds(group, rows, stride=step), :] = jnp.zeros((rows, LANES), f32)
    at = lambda level: slice(level * step, (level + 1) * step)
    current = column_ref[at(0), :] * inverse_ref[at(0), :]
    scaled = [current]
    for level in range(1, levels):
        current = column_ref[at(level), :] * inverse_ref[at(level), :] + forward_ref[at(level), :] * current
        scaled.append(current)
    column_ref[at(levels - 1), :] = current
    for level in range(levels - 2, -1, -1):
        current = scaled[level] + back_ref[at(level), :] * current
        column_ref[at(level), :] = current
    for level in range(levels, rows):
        column_ref[at(level), :] = jnp.zeros_like(current)


def solved(column_ref, group, rows):
    return column_ref[pl.ds(group, rows, stride=column_ref.shape[0] // rows), :]


def cell_kernel(
    total_ref,
    lat_outer_ref,
    high_ref,
    low_ref,
    cells_ref,
    speed_ref,
    inverse_ref,
    forward_ref,
    back_ref,
    matrix_ref,
    new_cells_ref,
    outer_ref,
    own_stack_ref,
    stack_ref,
    column_ref,
    *,
    levels,
):
    rows, cells = cells_ref.shape
    solve_columns(total_ref, lat_outer_ref, high_ref, low_ref, cells_ref, speed_ref, inverse_ref, forward_ref, back_ref, levels, stack_ref, column_ref)
    for group in range(cells // LANES):
        part = solved(column_ref, group, rows)
        new_cells_ref[:, group * LANES : (group + 1) * LANES] = part
        put_parts(own_stack_ref, part, group * LANES)
    store_outer(gather_matmul(own_stack_ref, [matrix_ref[...]], rows), outer_ref)


def last_kernel(
    total_ref, lat_outer_ref, high_ref, low_ref, cells_ref, speed_ref, inverse_ref, forward_ref, back_ref, out_ref, stack_ref, column_ref, *, levels
):
    rows, cells = cells_ref.shape
    solve_columns(total_ref, lat_outer_ref, high_ref, low_ref, cells_ref, speed_ref, inverse_ref, forward_ref, back_ref, levels, stack_ref, column_ref)
    for group in range(cells // LANES):
        out_ref[:, 0, group * LANES : (group + 1) * LANES] = solved(column_ref, group, rows)[0:levels]


def call(body, outs, scratch, *operands, raw=(), copies=0):
    in_vmem = pl.BlockSpec(memory_space=pltpu.VMEM)
    in_hbm = pl.BlockSpec(memory_space=pltpu.HBM)
    scratch_shapes = [pltpu.VMEM(shape, kind) for shape, kind in scratch]
    if copies:
        scratch_shapes.append(pltpu.SemaphoreType.DMA((copies,)))
    operands = [pltpu.with_memory_space_constraint(x, pltpu.HBM) if i in raw else x for i, x in enumerate(operands)]
    return pl.pallas_call(
        body,
        out_shape=tuple(jax.ShapeDtypeStruct(shape, kind) for shape, kind in outs),
        in_specs=[in_hbm if i in raw else in_vmem for i in range(len(operands))],
        out_specs=tuple(in_vmem for _ in outs),
        scratch_shapes=scratch_shapes,
        compiler_params=pltpu.CompilerParams(vmem_limit_bytes=24 * 1024 * 1024),
    )(*operands)


def on_device(lat_count, lon_count, pressure, velocity, edge_cells, cell_edges, send_cells, send_edges, inv_dual, edge_weight, sound_speed, coupling):
    _, levels, cells = pressure.shape
    edges = velocity.shape[2]
    halo = send_cells.shape[2]
    rows = round_up(levels, 16)
    edge_pad = round_up(edges, 2 * LANES)
    bundle = ((3, rows, halo), f32)
    straight = ((rows, halo), f32)
    lon_routes = swap_routes(lon_count)
    lat_inner_route = swap_routes(lat_count)[0]
    lat_outer_route = lat_outer_routes(lat_count, lon_count)
    i32 = jnp.int32

    by_level = lambda value: value.transpose(1, 0, 2)
    stack_cells = ((PARTS * rows, cells), bf16)
    stack_edges = ((PARTS * rows, edge_pad), bf16)
    stack_lat = lambda count: ((PARTS * rows, count * halo), bf16)
    column = ((rows * round_up(cells // LANES, 8), LANES), f32)
    sent_outer = lambda width: ((width, 3 * halo), bf16)
    sent_rest = lambda width: ((width, 5 * halo), bf16)

    for phase in range(2 * NSUB):
        at_cells = phase % 2 == 0
        if phase == 0:
            values, stack, outer, cell_list = call(
                start_kernel,
                [((rows, cells), f32), stack_cells, bundle, (send_cells.shape[1:], i32)],
                [((levels, 1, cells), f32), sent_outer(cells)],
                by_level(pressure),
                send_cells[0],
                raw=(0, 1),
                copies=2,
            )
        outer_in = lax.ppermute(outer, "lon", lon_routes[1])
        if phase == 0:
            inner, lat_inner, lat_outer = call(first_rest_kernel, [bundle, straight, straight], [sent_rest(cells)], stack, cell_list)
        elif at_cells:
            inner, lat_inner, lat_outer = call(rest_kernel, [bundle, straight, straight], [], stack, cell_rest)
        else:
            normal, inner, lat_inner, lat_outer = call(
                edge_rest_kernel,
                [((rows, edge_pad), f32), bundle, straight, straight],
                [stack_lat(second_in.shape[0]), stack_edges],
                total,
                second_in,
                gradient_far,
                normal,
                scale,
                edge_rest,
            )
        inner_in = lax.ppermute(inner, "lon", lon_routes[0])
        if phase == 0:
            gradient_near, gradient_far = call(
                functools.partial(gradient_kernel, cells=cells, halo=halo, lat_count=lat_count),
                [((cells + 2 * halo, edge_pad), bf16), ((6 * halo, edge_pad), bf16)],
                [(edge_cells.shape[1:], i32)],
                edge_cells[0],
                raw=(0,),
                copies=1,
            )
        if phase == 1:
            near_high, near_low, far_high, far_low = call(
                functools.partial(weight_kernel, edges=edges, edge_pad=edge_pad, halo=halo, lat_count=lat_count),
                [((edge_pad + 2 * halo, cells), bf16)] * 2 + [((6 * halo, cells), bf16)] * 2,
                [((3, 1, cells), i32), ((3, 1, cells), f32)],
                by_level(cell_edges),
                by_level(edge_weight),
                raw=(0, 1),
                copies=2,
            )
        early = phase >= 2
        first = jnp.stack([inner_in[1], lat_inner, outer_in[1]])
        if early:
            early_in = lax.ppermute(jnp.stack([inner_in[2], lat_outer]), ("lat", "lon"), lat_outer_route)
            second = outer_in[2:3]
        else:
            second = jnp.stack([inner_in[2], lat_outer, outer_in[2]])
        first_in = lax.ppermute(first, "lat", lat_inner_route)
        second_in = lax.ppermute(second, ("lat", "lon"), lat_outer_route)
        count = second.shape[0]
        if phase == 0:
            normal, scale, edge_outer, edge_rest, late_sent, sent_scale = call(
                edge_setup_kernel,
                [((rows, edge_pad), f32), ((1, edge_pad), f32), sent_outer(edge_pad), sent_rest(edge_pad), sent_outer(3 * halo), ((1, 3 * halo), f32)],
                [((levels, 1, edges), f32), (send_edges.shape[1:], i32), ((1, edges), f32), ((PARTS * 16, edge_pad), bf16)],
                by_level(velocity),
                send_edges[0],
                inv_dual,
                gradient_far,
                raw=(0, 1, 2),
                copies=3,
            )
        if phase == 1:
            speed, inverse, forward, back, cell_outer, cell_rest = call(
                cell_setup_kernel,
                [((1, cells), f32), column, column, column, sent_outer(cells), sent_rest(cells)],
                [((levels, 1, cells), f32), column],
                by_level(coupling),
                cell_list,
                sound_speed,
                raw=(0, 2),
                copies=2,
            )
        if at_cells:
            (total,) = call(
                early_part_kernel if early else part_kernel,
                [((rows, edge_pad), f32)],
                [((PARTS * rows, cells + 2 * halo), bf16)] + ([stack_lat(2)] if early else []),
                values,
                inner_in,
                outer_in,
                *([early_in, gradient_near, gradient_far] if early else [gradient_near]),
            )
            total, base = call(
                sent_base_kernel,
                [((rows, edge_pad), f32), ((rows, 3 * halo), f32)],
                [stack_lat(3), stack_edges],
                total,
                first_in,
                gradient_far,
                normal,
                scale,
                edge_outer,
            )
            (outer,) = call(edge_sent_kernel, [bundle], [stack_lat(count)], base, second_in, late_sent, sent_scale)
        else:
            (total,) = call(
                early_part_kernel if early else part_kernel,
                [((rows, cells), f32)],
                [((PARTS * rows, edge_pad + 2 * halo), bf16)] + ([stack_lat(2)] if early else []),
                normal,
                inner_in,
                outer_in,
                *([early_in, near_high, near_low, far_high, far_low] if early else [near_high, near_low]),
            )
            (total,) = call(inner_share_kernel, [((rows, cells), f32)], [stack_lat(3)], total, first_in, far_high, far_low)
            operands = (total, second_in, far_high, far_low, values, speed, inverse, forward, back)
            if phase < 2 * NSUB - 1:
                values, outer, stack = call(
                    functools.partial(cell_kernel, levels=levels),
                    [((rows, cells), f32), bundle, stack_cells],
                    [stack_lat(count), column],
                    *operands,
                    cell_outer,
                )
            else:
                (values,) = call(functools.partial(last_kernel, levels=levels), [((levels, 1, cells), f32)], [stack_lat(count), column], *operands)
    return by_level(values), normal[:levels, :edges][None]


def solution(mesh):
    return jax.shard_map(
        functools.partial(on_device, mesh.shape["lat"], mesh.shape["lon"]),
        mesh=mesh,
        in_specs=(
            P("lat", None, "lon"),
            P("lat", None, "lon"),
            P("lat", None, "lon"),
            P("lat", None, "lon"),
            P("lat", None, "lon"),
            P("lat", None, "lon"),
            P("lat", "lon"),
            P("lat", None, "lon"),
            P("lat", "lon"),
            P("lat", None, "lon"),
        ),
        out_specs=(P("lat", None, "lon"), P("lat", None, "lon")),
        check_vma=False,
    )
```

```python
import functools

import jax
import jax.numpy as jnp
from jax import lax
from jax.experimental import pallas as pl
from jax.experimental.pallas import tpu as pltpu
from jax.sharding import PartitionSpec as P


NSUB = 3
STEP_SCALE = 0.5
LANES = 128
PARTS = 3

f32 = jnp.float32
bf16 = jnp.bfloat16
i16 = jnp.int16


def round_up(value, step):
    return -(-value // step) * step


def swap_routes(count):
    inner = [(i, i ^ 1) for i in range(count)]
    outer = [(i, (((i + 1) ^ 1) - 1) % count) for i in range(count)]
    return inner, outer


def lat_outer_routes(lat_count, lon_count):
    routes = []
    for a, target in swap_routes(lat_count)[1]:
        for b in range(lon_count):
            alone = a in (0, lat_count - 1)
            routes.append((a * lon_count + b, a * lon_count + (b ^ 1) if alone else target * lon_count + b))
    return routes


OUTER_SENT = ((0, 2), (1, 2), (2, 2))
REST_SENT = ((0, 1), (1, 1), (2, 1), (1, 0), (2, 0))


def link_signs():
    lat_inner = 1 - 2 * lax.rem(lax.axis_index("lat"), 2)
    lon_inner = 1 - 2 * lax.rem(lax.axis_index("lon"), 2)
    return lat_inner, lon_inner


def sent_row(member):
    lat_inner, lon_inner = link_signs()
    lat_link, lon_link = member
    p = (0, lat_inner, -lat_inner)[lat_link]
    q = (0, lon_inner, -lon_inner)[lon_link]
    flat = (p + 1) * 3 + (q + 1)
    return flat - jnp.where(flat > 4, 1, 0)


def local_positions(index, own, own_padded, halo, lat_count):
    lat_inner, lon_inner = link_signs()
    a = lax.axis_index("lat")
    beyond = index - own
    piece = lax.div(jnp.maximum(beyond, 0), halo)
    slot = beyond - piece * halo
    flat = piece + jnp.where(piece >= 4, 1, 0)
    p = jnp.where(flat >= 6, 1, jnp.where(flat >= 3, 0, -1))
    q = flat - 3 * (p + 1) - 1
    lon_member = jnp.where(q == 0, 1, jnp.where(q == lon_inner, 0, 2))
    member = jnp.where(p == 0, jnp.minimum(lon_member, 1), jnp.where(p == lat_inner, 2, 5) + lon_member)
    outside = (a + p < 0) | (a + p >= lat_count)
    row = own_padded + member * halo + slot
    return jnp.where(beyond < 0, index, jnp.where(outside, -1, row))


def put_parts(stack_ref, value, start):
    rows, width = value.shape
    rest = value
    for part in range(PARTS):
        piece = rest.astype(bf16)
        stack_ref[part * rows : (part + 1) * rows, start : start + width] = piece
        if part < PARTS - 1:
            rest = rest - piece.astype(f32)


def sum_parts(product, rows):
    total = product[(PARTS - 1) * rows : PARTS * rows]
    for part in range(PARTS - 2, -1, -1):
        total = total + product[part * rows : (part + 1) * rows]
    return total


def gather_matmul(stack_ref, matrices, rows):
    product = None
    for matrix in matrices:
        term = jnp.dot(stack_ref[...], matrix, preferred_element_type=f32)
        product = term if product is None else product + term
    return sum_parts(product, rows)


def start_fetch(pairs, sems):
    copies = [pltpu.make_async_copy(source, target, sems.at[i]) for i, (source, target) in enumerate(pairs)]
    for copy in copies:
        copy.start()
    return copies


def fetch(pairs, sems):
    for copy in start_fetch(pairs, sems):
        copy.wait()


def by_blocks(rows, body):
    block = 64 if rows % 64 == 0 else 16

    def step(i, carry):
        first = pl.multiple_of(i * block, block)
        body(first, block)
        return carry

    lax.fori_loop(0, rows // block, step, 0)


def row_numbers(first, block, width):
    return (lax.broadcasted_iota(jnp.int32, (block, width), 0) + first).astype(i16)


def fill_sent(matrix_ref, list_ref, members):
    rows = matrix_ref.shape[0]
    halo = list_ref.shape[1]
    lanes = [list_ref[pl.ds(sent_row(member), 1), :].astype(i16) for member in members]

    def body(first, block):
        row = row_numbers(first, block, halo)
        for member, index in enumerate(lanes):
            hit = jnp.where(row == index, jnp.ones((), bf16), jnp.zeros((), bf16))
            matrix_ref[pl.ds(first, block), member * halo : (member + 1) * halo] = hit

    by_blocks(rows, body)


def store_outer(pieces, outer_ref):
    halo = outer_ref.shape[2]
    for member in range(3):
        outer_ref[member] = pieces[:, member * halo : (member + 1) * halo]


def store_rest(pieces, inner_ref, lat_inner_ref, lat_outer_ref):
    halo = inner_ref.shape[2]
    for member in range(3):
        inner_ref[member] = pieces[:, member * halo : (member + 1) * halo]
    lat_inner_ref[...] = pieces[:, 3 * halo : 4 * halo]
    lat_outer_ref[...] = pieces[:, 4 * halo : 5 * halo]


def start_kernel(pressure_hbm, list_hbm, cells_ref, stack_ref, outer_ref, lists_ref, pressure_ref, matrix_ref, sems):
    lists, pressure = start_fetch([(list_hbm, lists_ref), (pressure_hbm, pressure_ref)], sems)
    levels = pressure_ref.shape[0]
    rows = cells_ref.shape[0]
    lists.wait()
    fill_sent(matrix_ref, lists_ref, OUTER_SENT)
    pressure.wait()
    cells_ref[0:levels, :] = pressure_ref[:, 0, :]
    cells_ref[levels:rows, :] = jnp.zeros((rows - levels, cells_ref.shape[1]), f32)
    put_parts(stack_ref, cells_ref[...], 0)
    store_outer(gather_matmul(stack_ref, [matrix_ref[...]], rows), outer_ref)


def first_rest_kernel(stack_ref, list_ref, inner_ref, lat_inner_ref, lat_outer_ref, matrix_ref):
    fill_sent(matrix_ref, list_ref, REST_SENT)
    store_rest(gather_matmul(stack_ref, [matrix_ref[...]], inner_ref.shape[1]), inner_ref, lat_inner_ref, lat_outer_ref)


def rest_kernel(stack_ref, matrix_ref, inner_ref, lat_inner_ref, lat_outer_ref):
    store_rest(gather_matmul(stack_ref, [matrix_ref[...]], inner_ref.shape[1]), inner_ref, lat_inner_ref, lat_outer_ref)


def gradient_kernel(edge_cells_hbm, near_ref, far_ref, ends_ref, sems, *, cells, halo, lat_count):
    fetch([(edge_cells_hbm, ends_ref)], sems)
    edges = ends_ref.shape[1]
    edge_pad = near_ref.shape[1]
    ends = local_positions(ends_ref[...], cells, cells, halo, lat_count)
    near, far = ends[0:1, :], ends[1:2, :]
    same = near == far
    near, far = jnp.where(same, -1, near), jnp.where(same, -1, far)
    if edge_pad > edges:
        fill = jnp.full((1, edge_pad - edges), -1, jnp.int32)
        near, far = jnp.concatenate([near, fill], axis=1), jnp.concatenate([far, fill], axis=1)
    near, far = near.astype(i16), far.astype(i16)

    def fill_rows(matrix_ref, base):
        def body(first, block):
            row = row_numbers(first + base, block, edge_pad)
            one = jnp.ones((), bf16)
            matrix_ref[pl.ds(first, block), :] = jnp.where(row == far, one, jnp.where(row == near, -one, jnp.zeros((), bf16)))

        by_blocks(matrix_ref.shape[0], body)

    fill_rows(near_ref, 0)
    fill_rows(far_ref, near_ref.shape[0])


def edge_setup_kernel(
    velocity_hbm, list_hbm, dual_hbm, far_ref, edges_ref, scale_ref, outer_matrix_ref, rest_matrix_ref, late_ref, sent_scale_ref, velocity_ref, list_ref, dual_ref, stack_ref, sems
):
    lists, velocity, dual = start_fetch([(list_hbm, list_ref), (velocity_hbm, velocity_ref), (dual_hbm, dual_ref)], sems)
    levels, _, edges = velocity_ref.shape
    edges_ref[...] = jnp.zeros(edges_ref.shape, f32)
    scale_ref[...] = jnp.zeros(scale_ref.shape, f32)
    lists.wait()
    fill_sent(outer_matrix_ref, list_ref, OUTER_SENT)
    fill_sent(rest_matrix_ref, list_ref, REST_SENT)
    velocity.wait()
    dual.wait()
    edges_ref[0:levels, 0:edges] = velocity_ref[:, 0, :]
    scale_ref[:, 0:edges] = STEP_SCALE * dual_ref[...]
    late = far_ref[far_ref.shape[0] - late_ref.shape[0] :, :]
    late_ref[...] = jnp.dot(late, outer_matrix_ref[...], preferred_element_type=f32).astype(bf16)
    rows = stack_ref.shape[0] // PARTS
    put_parts(stack_ref, jnp.broadcast_to(scale_ref[...], (rows, scale_ref.shape[1])), 0)
    sent_scale_ref[...] = gather_matmul(stack_ref, [outer_matrix_ref[...]], rows)[0:1]


def fill_weights(high_ref, low_ref, place, weight, base):
    high = [value.astype(bf16) for value in weight]
    low = [(value - top.astype(f32)).astype(bf16) for value, top in zip(weight, high)]
    place = [value.astype(i16) for value in place]
    zero = jnp.zeros((), bf16)

    def body(first, block):
        row = row_numbers(first + base, block, high_ref.shape[1])
        hits = [row == value for value in place]
        for target, values in ((high_ref, high), (low_ref, low)):
            entry = jnp.where(hits[0], values[0], jnp.where(hits[1], values[1], jnp.where(hits[2], values[2], zero)))
            target[pl.ds(first, block), :] = entry

    by_blocks(high_ref.shape[0], body)


def weight_kernel(sides_hbm, weight_hbm, high_ref, low_ref, place_ref, merged_ref, sides_ref, weight_ref, sems, *, edges, edge_pad, halo, lat_count):
    fetch([(sides_hbm, sides_ref), (weight_hbm, weight_ref)], sems)
    place = [local_positions(sides_ref[i], edges, edge_pad, halo, lat_count) for i in range(3)]
    weight = [weight_ref[i] for i in range(3)]
    for later in (1, 2):
        for earlier in range(later):
            same = place[later] == place[earlier]
            weight[earlier] = weight[earlier] + jnp.where(same, weight[later], 0.0)
            weight[later] = jnp.where(same, 0.0, weight[later])
            place[later] = jnp.where(same, -1, place[later])
    for i in range(3):
        place_ref[i] = place[i]
        merged_ref[i] = weight[i]
    fill_weights(high_ref, low_ref, place, weight, 0)


def far_weight_kernel(place_ref, merged_ref, high_ref, low_ref, *, base):
    fill_weights(high_ref, low_ref, [place_ref[i] for i in range(3)], [merged_ref[i] for i in range(3)], base)


def cell_setup_kernel(
    coupling_hbm, list_ref, speed_hbm, speed_ref, inverse_ref, forward_ref, back_ref, outer_matrix_ref, rest_matrix_ref, coupling_ref, column_ref, sems
):
    coupling, speed = start_fetch([(coupling_hbm, coupling_ref), (speed_hbm, speed_ref)], sems)
    levels, _, cells = coupling_ref.shape
    fill_sent(outer_matrix_ref, list_ref, OUTER_SENT)
    fill_sent(rest_matrix_ref, list_ref, REST_SENT)
    coupling.wait()
    speed.wait()
    step = column_ref.shape[0] // round_up(levels, 16)
    column_ref[...] = jnp.zeros(column_ref.shape, f32)
    for group in range(cells // LANES):
        column_ref[pl.ds(group, levels, stride=step), :] = coupling_ref[:, 0, group * LANES : (group + 1) * LANES]
    at = lambda level: slice(level * step, (level + 1) * step)
    above = column_ref[at(0), :]
    inverse = 1.0 / (1.0 + above)
    inverse_ref[at(0), :] = inverse
    ratio = above * inverse
    back_ref[at(0), :] = ratio
    for level in range(1, levels):
        below = above
        above = column_ref[at(level), :]
        inverse = 1.0 / (1.0 + below + above - below * ratio)
        inverse_ref[at(level), :] = inverse
        forward_ref[at(level), :] = below * inverse
        ratio = above * inverse
        back_ref[at(level), :] = ratio


def part_kernel(own_ref, inner_ref, outer_ref, *rest):
    *matrix_refs, total_ref, stack_ref = rest
    rows, width = own_ref.shape
    halo = inner_ref.shape[2]
    put_parts(stack_ref, own_ref[...], 0)
    put_parts(stack_ref, inner_ref[0], width)
    put_parts(stack_ref, outer_ref[0], width + halo)
    total_ref[...] = gather_matmul(stack_ref, [ref[...] for ref in matrix_refs], rows)


def early_part_kernel(own_ref, inner_ref, outer_ref, early_ref, *rest):
    *matrix_refs, total_ref, stack_ref, early_stack_ref = rest
    near_refs, far_refs = matrix_refs[: len(matrix_refs) // 2], matrix_refs[len(matrix_refs) // 2 :]
    part_kernel(own_ref, inner_ref, outer_ref, *near_refs, total_ref, stack_ref)
    total_ref[...] = lat_share(total_ref, early_ref, far_refs, early_stack_ref, 3)


def lat_share(total_ref, lat_ref, matrix_refs, stack_ref, first):
    rows = total_ref.shape[0]
    count, _, halo = lat_ref.shape
    for member in range(count):
        put_parts(stack_ref, lat_ref[member], member * halo)
    matrices = [ref[first * halo : (first + count) * halo, :] for ref in matrix_refs]
    return total_ref[...] + gather_matmul(stack_ref, matrices, rows)


def inner_share_kernel(total_ref, lat_inner_ref, *rest):
    *matrix_refs, new_total_ref, stack_ref = rest
    new_total_ref[...] = lat_share(total_ref, lat_inner_ref, matrix_refs, stack_ref, 0)


def sent_base_kernel(total_ref, lat_inner_ref, far_ref, edges_ref, scale_ref, matrix_ref, new_total_ref, base_ref, stack_ref, own_stack_ref):
    total = lat_share(total_ref, lat_inner_ref, [far_ref], stack_ref, 0)
    new_total_ref[...] = total
    put_parts(own_stack_ref, edges_ref[...] - scale_ref[...] * total, 0)
    base_ref[...] = gather_matmul(own_stack_ref, [matrix_ref[...]], total_ref.shape[0])


def edge_sent_kernel(base_ref, lat_outer_ref, late_ref, sent_scale_ref, outer_ref, stack_ref):
    rows = base_ref.shape[0]
    count, _, halo = lat_outer_ref.shape
    for member in range(count):
        put_parts(stack_ref, lat_outer_ref[member], member * halo)
    late = late_ref[late_ref.shape[0] - count * halo :, :]
    store_outer(base_ref[...] - sent_scale_ref[...] * gather_matmul(stack_ref, [late], rows), outer_ref)


def edge_rest_kernel(total_ref, lat_outer_ref, far_ref, edges_ref, scale_ref, matrix_ref, new_edges_ref, inner_ref, lat_inner_ref, lat_outer_out_ref, stack_ref, own_stack_ref):
    difference = lat_share(total_ref, lat_outer_ref, [far_ref], stack_ref, 6 - lat_outer_ref.shape[0])
    new_edges = edges_ref[...] - scale_ref[...] * difference
    new_edges_ref[...] = new_edges
    put_parts(own_stack_ref, new_edges, 0)
    store_rest(gather_matmul(own_stack_ref, [matrix_ref[...]], edges_ref.shape[0]), inner_ref, lat_inner_ref, lat_outer_out_ref)


def solve_columns(total_ref, lat_outer_ref, high_ref, low_ref, cells_ref, speed_ref, inverse_ref, forward_ref, back_ref, levels, stack_ref, column_ref):
    rows, cells = cells_ref.shape
    divergence = lat_share(total_ref, lat_outer_ref, [high_ref, low_ref], stack_ref, 6 - lat_outer_ref.shape[0])
    right_side = cells_ref[...] - speed_ref[...] * divergence
    step = column_ref.shape[0] // rows
    for group in range(cells // LANES):
        column_ref[pl.ds(group, rows, stride=step), :] = right_side[:, group * LANES : (group + 1) * LANES]
    for group in range(cells // LANES, step):
        column_ref[pl.ds(group, rows, stride=step), :] = jnp.zeros((rows, LANES), f32)
    at = lambda level: slice(level * step, (level + 1) * step)
    current = column_ref[at(0), :] * inverse_ref[at(0), :]
    scaled = [current]
    for level in range(1, levels):
        current = column_ref[at(level), :] * inverse_ref[at(level), :] + forward_ref[at(level), :] * current
        scaled.append(current)
    column_ref[at(levels - 1), :] = current
    for level in range(levels - 2, -1, -1):
        current = scaled[level] + back_ref[at(level), :] * current
        column_ref[at(level), :] = current
    for level in range(levels, rows):
        column_ref[at(level), :] = jnp.zeros_like(current)


def solved(column_ref, group, rows):
    return column_ref[pl.ds(group, rows, stride=column_ref.shape[0] // rows), :]


def cell_kernel(
    total_ref,
    lat_outer_ref,
    high_ref,
    low_ref,
    cells_ref,
    speed_ref,
    inverse_ref,
    forward_ref,
    back_ref,
    matrix_ref,
    new_cells_ref,
    outer_ref,
    own_stack_ref,
    stack_ref,
    column_ref,
    *,
    levels,
):
    rows, cells = cells_ref.shape
    solve_columns(total_ref, lat_outer_ref, high_ref, low_ref, cells_ref, speed_ref, inverse_ref, forward_ref, back_ref, levels, stack_ref, column_ref)
    for group in range(cells // LANES):
        part = solved(column_ref, group, rows)
        new_cells_ref[:, group * LANES : (group + 1) * LANES] = part
        put_parts(own_stack_ref, part, group * LANES)
    store_outer(gather_matmul(own_stack_ref, [matrix_ref[...]], rows), outer_ref)


def last_kernel(
    total_ref, lat_outer_ref, high_ref, low_ref, cells_ref, speed_ref, inverse_ref, forward_ref, back_ref, out_ref, stack_ref, column_ref, *, levels
):
    rows, cells = cells_ref.shape
    solve_columns(total_ref, lat_outer_ref, high_ref, low_ref, cells_ref, speed_ref, inverse_ref, forward_ref, back_ref, levels, stack_ref, column_ref)
    for group in range(cells // LANES):
        out_ref[:, 0, group * LANES : (group + 1) * LANES] = solved(column_ref, group, rows)[0:levels]


def call(body, outs, scratch, *operands, raw=(), copies=0):
    in_vmem = pl.BlockSpec(memory_space=pltpu.VMEM)
    in_hbm = pl.BlockSpec(memory_space=pltpu.HBM)
    scratch_shapes = [pltpu.VMEM(shape, kind) for shape, kind in scratch]
    if copies:
        scratch_shapes.append(pltpu.SemaphoreType.DMA((copies,)))
    operands = [pltpu.with_memory_space_constraint(x, pltpu.HBM) if i in raw else x for i, x in enumerate(operands)]
    return pl.pallas_call(
        body,
        out_shape=tuple(jax.ShapeDtypeStruct(shape, kind) for shape, kind in outs),
        in_specs=[in_hbm if i in raw else in_vmem for i in range(len(operands))],
        out_specs=tuple(in_vmem for _ in outs),
        scratch_shapes=scratch_shapes,
        compiler_params=pltpu.CompilerParams(vmem_limit_bytes=24 * 1024 * 1024),
    )(*operands)


def on_device(lat_count, lon_count, pressure, velocity, edge_cells, cell_edges, send_cells, send_edges, inv_dual, edge_weight, sound_speed, coupling):
    _, levels, cells = pressure.shape
    edges = velocity.shape[2]
    halo = send_cells.shape[2]
    rows = round_up(levels, 16)
    edge_pad = round_up(edges, 2 * LANES)
    bundle = ((3, rows, halo), f32)
    straight = ((rows, halo), f32)
    lon_routes = swap_routes(lon_count)
    lat_inner_route = swap_routes(lat_count)[0]
    lat_outer_route = lat_outer_routes(lat_count, lon_count)
    i32 = jnp.int32

    by_level = lambda value: value.transpose(1, 0, 2)
    stack_cells = ((PARTS * rows, cells), bf16)
    stack_edges = ((PARTS * rows, edge_pad), bf16)
    stack_lat = lambda count: ((PARTS * rows, count * halo), bf16)
    column = ((rows * round_up(cells // LANES, 8), LANES), f32)
    sent_outer = lambda width: ((width, 3 * halo), bf16)
    sent_rest = lambda width: ((width, 5 * halo), bf16)

    for phase in range(2 * NSUB):
        at_cells = phase % 2 == 0
        if phase == 0:
            values, stack, outer, cell_list = call(
                start_kernel,
                [((rows, cells), f32), stack_cells, bundle, (send_cells.shape[1:], i32)],
                [((levels, 1, cells), f32), sent_outer(cells)],
                by_level(pressure),
                send_cells[0],
                raw=(0, 1),
                copies=2,
            )
        outer_in = lax.ppermute(outer, "lon", lon_routes[1])
        if phase == 0:
            inner, lat_inner, lat_outer = call(first_rest_kernel, [bundle, straight, straight], [sent_rest(cells)], stack, cell_list)
        elif at_cells:
            inner, lat_inner, lat_outer = call(rest_kernel, [bundle, straight, straight], [], stack, cell_rest)
        else:
            normal, inner, lat_inner, lat_outer = call(
                edge_rest_kernel,
                [((rows, edge_pad), f32), bundle, straight, straight],
                [stack_lat(second_in.shape[0]), stack_edges],
                total,
                second_in,
                gradient_far,
                normal,
                scale,
                edge_rest,
            )
        inner_in = lax.ppermute(inner, "lon", lon_routes[0])
        if phase == 0:
            gradient_near, gradient_far = call(
                functools.partial(gradient_kernel, cells=cells, halo=halo, lat_count=lat_count),
                [((cells + 2 * halo, edge_pad), bf16), ((6 * halo, edge_pad), bf16)],
                [(edge_cells.shape[1:], i32)],
                edge_cells[0],
                raw=(0,),
                copies=1,
            )
        if phase == 1:
            near_high, near_low, place, merged = call(
                functools.partial(weight_kernel, edges=edges, edge_pad=edge_pad, halo=halo, lat_count=lat_count),
                [((edge_pad + 2 * halo, cells), bf16)] * 2 + [((3, 1, cells), i32), ((3, 1, cells), f32)],
                [((3, 1, cells), i32), ((3, 1, cells), f32)],
                by_level(cell_edges),
                by_level(edge_weight),
                raw=(0, 1),
                copies=2,
            )
            far_high, far_low = call(
                functools.partial(far_weight_kernel, base=edge_pad + 2 * halo),
                [((6 * halo, cells), bf16)] * 2,
                [],
                place,
                merged,
            )
        early = phase >= 2
        first = jnp.stack([inner_in[1], lat_inner, outer_in[1]])
        if early:
            early_in = lax.ppermute(jnp.stack([inner_in[2], lat_outer]), ("lat", "lon"), lat_outer_route)
            second = outer_in[2:3]
        else:
            second = jnp.stack([inner_in[2], lat_outer, outer_in[2]])
        first_in = lax.ppermute(first, "lat", lat_inner_route)
        second_in = lax.ppermute(second, ("lat", "lon"), lat_outer_route)
        count = second.shape[0]
        if phase == 0:
            normal, scale, edge_outer, edge_rest, late_sent, sent_scale = call(
                edge_setup_kernel,
                [((rows, edge_pad), f32), ((1, edge_pad), f32), sent_outer(edge_pad), sent_rest(edge_pad), sent_outer(3 * halo), ((1, 3 * halo), f32)],
                [((levels, 1, edges), f32), (send_edges.shape[1:], i32), ((1, edges), f32), ((PARTS * 16, edge_pad), bf16)],
                by_level(velocity),
                send_edges[0],
                inv_dual,
                gradient_far,
                raw=(0, 1, 2),
                copies=3,
            )
        if phase == 1:
            speed, inverse, forward, back, cell_outer, cell_rest = call(
                cell_setup_kernel,
                [((1, cells), f32), column, column, column, sent_outer(cells), sent_rest(cells)],
                [((levels, 1, cells), f32), column],
                by_level(coupling),
                cell_list,
                sound_speed,
                raw=(0, 2),
                copies=2,
            )
        if at_cells:
            (total,) = call(
                early_part_kernel if early else part_kernel,
                [((rows, edge_pad), f32)],
                [((PARTS * rows, cells + 2 * halo), bf16)] + ([stack_lat(2)] if early else []),
                values,
                inner_in,
                outer_in,
                *([early_in, gradient_near, gradient_far] if early else [gradient_near]),
            )
            total, base = call(
                sent_base_kernel,
                [((rows, edge_pad), f32), ((rows, 3 * halo), f32)],
                [stack_lat(3), stack_edges],
                total,
                first_in,
                gradient_far,
                normal,
                scale,
                edge_outer,
            )
            (outer,) = call(edge_sent_kernel, [bundle], [stack_lat(count)], base, second_in, late_sent, sent_scale)
        else:
            (total,) = call(
                early_part_kernel if early else part_kernel,
                [((rows, cells), f32)],
                [((PARTS * rows, edge_pad + 2 * halo), bf16)] + ([stack_lat(2)] if early else []),
                normal,
                inner_in,
                outer_in,
                *([early_in, near_high, near_low, far_high, far_low] if early else [near_high, near_low]),
            )
            (total,) = call(inner_share_kernel, [((rows, cells), f32)], [stack_lat(3)], total, first_in, far_high, far_low)
            operands = (total, second_in, far_high, far_low, values, speed, inverse, forward, back)
            if phase < 2 * NSUB - 1:
                values, outer, stack = call(
                    functools.partial(cell_kernel, levels=levels),
                    [((rows, cells), f32), bundle, stack_cells],
                    [stack_lat(count), column],
                    *operands,
                    cell_outer,
                )
            else:
                (values,) = call(functools.partial(last_kernel, levels=levels), [((levels, 1, cells), f32)], [stack_lat(count), column], *operands)
    return by_level(values), normal[:levels, :edges][None]


def solution(mesh):
    return jax.shard_map(
        functools.partial(on_device, mesh.shape["lat"], mesh.shape["lon"]),
        mesh=mesh,
        in_specs=(
            P("lat", None, "lon"),
            P("lat", None, "lon"),
            P("lat", None, "lon"),
            P("lat", None, "lon"),
            P("lat", None, "lon"),
            P("lat", None, "lon"),
            P("lat", "lon"),
            P("lat", None, "lon"),
            P("lat", "lon"),
            P("lat", None, "lon"),
        ),
        out_specs=(P("lat", None, "lon"), P("lat", None, "lon")),
        check_vma=False,
    )
```

```python
import functools

import jax
import jax.numpy as jnp
from jax import lax
from jax.experimental import pallas as pl
from jax.experimental.pallas import tpu as pltpu
from jax.sharding import PartitionSpec as P


NSUB = 3
STEP_SCALE = 0.5
LANES = 128
PARTS = 3

f32 = jnp.float32
bf16 = jnp.bfloat16
i16 = jnp.int16


def round_up(value, step):
    return -(-value // step) * step


def swap_routes(count):
    inner = [(i, i ^ 1) for i in range(count)]
    outer = [(i, (((i + 1) ^ 1) - 1) % count) for i in range(count)]
    return inner, outer


def lat_outer_routes(lat_count, lon_count):
    routes = []
    for a, target in swap_routes(lat_count)[1]:
        for b in range(lon_count):
            alone = a in (0, lat_count - 1)
            routes.append((a * lon_count + b, a * lon_count + (b ^ 1) if alone else target * lon_count + b))
    return routes


OUTER_SENT = ((0, 2), (1, 2), (2, 2))
REST_SENT = ((0, 1), (1, 1), (2, 1), (1, 0), (2, 0))


def link_signs():
    lat_inner = 1 - 2 * lax.rem(lax.axis_index("lat"), 2)
    lon_inner = 1 - 2 * lax.rem(lax.axis_index("lon"), 2)
    return lat_inner, lon_inner


def sent_row(member):
    lat_inner, lon_inner = link_signs()
    lat_link, lon_link = member
    p = (0, lat_inner, -lat_inner)[lat_link]
    q = (0, lon_inner, -lon_inner)[lon_link]
    flat = (p + 1) * 3 + (q + 1)
    return flat - jnp.where(flat > 4, 1, 0)


def local_positions(index, own, own_padded, halo, lat_count):
    lat_inner, lon_inner = link_signs()
    a = lax.axis_index("lat")
    beyond = index - own
    piece = lax.div(jnp.maximum(beyond, 0), halo)
    slot = beyond - piece * halo
    flat = piece + jnp.where(piece >= 4, 1, 0)
    p = jnp.where(flat >= 6, 1, jnp.where(flat >= 3, 0, -1))
    q = flat - 3 * (p + 1) - 1
    lon_member = jnp.where(q == 0, 1, jnp.where(q == lon_inner, 0, 2))
    member = jnp.where(p == 0, jnp.minimum(lon_member, 1), jnp.where(p == lat_inner, 2, 5) + lon_member)
    outside = (a + p < 0) | (a + p >= lat_count)
    row = own_padded + member * halo + slot
    return jnp.where(beyond < 0, index, jnp.where(outside, -1, row))


def put_parts(stack_ref, value, start):
    rows, width = value.shape
    rest = value
    for part in range(PARTS):
        piece = rest.astype(bf16)
        stack_ref[part * rows : (part + 1) * rows, start : start + width] = piece
        if part < PARTS - 1:
            rest = rest - piece.astype(f32)


def sum_parts(product, rows):
    total = product[(PARTS - 1) * rows : PARTS * rows]
    for part in range(PARTS - 2, -1, -1):
        total = total + product[part * rows : (part + 1) * rows]
    return total


def gather_matmul(stack_ref, matrices, rows):
    product = None
    for matrix in matrices:
        term = jnp.dot(stack_ref[...], matrix, preferred_element_type=f32)
        product = term if product is None else product + term
    return sum_parts(product, rows)


def start_fetch(pairs, sems):
    copies = [pltpu.make_async_copy(source, target, sems.at[i]) for i, (source, target) in enumerate(pairs)]
    for copy in copies:
        copy.start()
    return copies


def fetch(pairs, sems):
    for copy in start_fetch(pairs, sems):
        copy.wait()


def by_blocks(rows, body):
    block = 64 if rows % 64 == 0 else 16

    def step(i, carry):
        first = pl.multiple_of(i * block, block)
        body(first, block)
        return carry

    lax.fori_loop(0, rows // block, step, 0)


def row_numbers(first, block, width):
    return (lax.broadcasted_iota(jnp.int32, (block, width), 0) + first).astype(i16)


def fill_sent(matrix_ref, list_ref, members):
    rows = matrix_ref.shape[0]
    halo = list_ref.shape[1]
    lanes = [list_ref[pl.ds(sent_row(member), 1), :].astype(i16) for member in members]

    def body(first, block):
        row = row_numbers(first, block, halo)
        for member, index in enumerate(lanes):
            hit = jnp.where(row == index, jnp.ones((), bf16), jnp.zeros((), bf16))
            matrix_ref[pl.ds(first, block), member * halo : (member + 1) * halo] = hit

    by_blocks(rows, body)


def store_outer(pieces, outer_ref):
    halo = outer_ref.shape[2]
    for member in range(3):
        outer_ref[member] = pieces[:, member * halo : (member + 1) * halo]


def store_rest(pieces, inner_ref, lat_inner_ref, lat_outer_ref):
    halo = inner_ref.shape[2]
    for member in range(3):
        inner_ref[member] = pieces[:, member * halo : (member + 1) * halo]
    lat_inner_ref[...] = pieces[:, 3 * halo : 4 * halo]
    lat_outer_ref[...] = pieces[:, 4 * halo : 5 * halo]


def start_kernel(pressure_hbm, list_hbm, cells_ref, stack_ref, outer_ref, lists_ref, pressure_ref, matrix_ref, sems):
    lists, pressure = start_fetch([(list_hbm, lists_ref), (pressure_hbm, pressure_ref)], sems)
    levels = pressure_ref.shape[0]
    rows = cells_ref.shape[0]
    lists.wait()
    fill_sent(matrix_ref, lists_ref, OUTER_SENT)
    pressure.wait()
    cells_ref[0:levels, :] = pressure_ref[:, 0, :]
    cells_ref[levels:rows, :] = jnp.zeros((rows - levels, cells_ref.shape[1]), f32)
    put_parts(stack_ref, cells_ref[...], 0)
    store_outer(gather_matmul(stack_ref, [matrix_ref[...]], rows), outer_ref)


def first_rest_kernel(stack_ref, list_ref, inner_ref, lat_inner_ref, lat_outer_ref, matrix_ref):
    fill_sent(matrix_ref, list_ref, REST_SENT)
    store_rest(gather_matmul(stack_ref, [matrix_ref[...]], inner_ref.shape[1]), inner_ref, lat_inner_ref, lat_outer_ref)


def rest_kernel(stack_ref, matrix_ref, inner_ref, lat_inner_ref, lat_outer_ref):
    store_rest(gather_matmul(stack_ref, [matrix_ref[...]], inner_ref.shape[1]), inner_ref, lat_inner_ref, lat_outer_ref)


def gradient_kernel(edge_cells_hbm, near_ref, far_ref, ends_ref, sems, *, cells, halo, lat_count):
    fetch([(edge_cells_hbm, ends_ref)], sems)
    edges = ends_ref.shape[1]
    edge_pad = near_ref.shape[1]
    ends = local_positions(ends_ref[...], cells, cells, halo, lat_count)
    near, far = ends[0:1, :], ends[1:2, :]
    same = near == far
    near, far = jnp.where(same, -1, near), jnp.where(same, -1, far)
    if edge_pad > edges:
        fill = jnp.full((1, edge_pad - edges), -1, jnp.int32)
        near, far = jnp.concatenate([near, fill], axis=1), jnp.concatenate([far, fill], axis=1)
    near, far = near.astype(i16), far.astype(i16)

    def fill_rows(matrix_ref, base):
        def body(first, block):
            row = row_numbers(first + base, block, edge_pad)
            one = jnp.ones((), bf16)
            matrix_ref[pl.ds(first, block), :] = jnp.where(row == far, one, jnp.where(row == near, -one, jnp.zeros((), bf16)))

        by_blocks(matrix_ref.shape[0], body)

    fill_rows(near_ref, 0)
    fill_rows(far_ref, near_ref.shape[0])


def edge_setup_kernel(
    velocity_hbm, list_hbm, dual_hbm, far_ref, edges_ref, scale_ref, outer_matrix_ref, rest_matrix_ref, late_ref, sent_scale_ref, velocity_ref, list_ref, dual_ref, stack_ref, sems
):
    lists, velocity, dual = start_fetch([(list_hbm, list_ref), (velocity_hbm, velocity_ref), (dual_hbm, dual_ref)], sems)
    levels, _, edges = velocity_ref.shape
    edges_ref[...] = jnp.zeros(edges_ref.shape, f32)
    scale_ref[...] = jnp.zeros(scale_ref.shape, f32)
    lists.wait()
    fill_sent(outer_matrix_ref, list_ref, OUTER_SENT)
    fill_sent(rest_matrix_ref, list_ref, REST_SENT)
    velocity.wait()
    dual.wait()
    edges_ref[0:levels, 0:edges] = velocity_ref[:, 0, :]
    scale_ref[:, 0:edges] = STEP_SCALE * dual_ref[...]
    late = far_ref[far_ref.shape[0] - late_ref.shape[0] :, :]
    late_ref[...] = jnp.dot(late, outer_matrix_ref[...], preferred_element_type=f32).astype(bf16)
    rows = stack_ref.shape[0] // PARTS
    put_parts(stack_ref, jnp.broadcast_to(scale_ref[...], (rows, scale_ref.shape[1])), 0)
    sent_scale_ref[...] = gather_matmul(stack_ref, [outer_matrix_ref[...]], rows)[0:1]


def weight_kernel(
    sides_hbm, weight_hbm, near_high_ref, near_low_ref, far_high_ref, far_low_ref, sides_ref, weight_ref, sems, *, edges, edge_pad, halo, lat_count
):
    fetch([(sides_hbm, sides_ref), (weight_hbm, weight_ref)], sems)
    cells = sides_ref.shape[2]
    place = [local_positions(sides_ref[i], edges, edge_pad, halo, lat_count) for i in range(3)]
    weight = [weight_ref[i] for i in range(3)]
    for later in (1, 2):
        for earlier in range(later):
            same = place[later] == place[earlier]
            weight[earlier] = weight[earlier] + jnp.where(same, weight[later], 0.0)
            weight[later] = jnp.where(same, 0.0, weight[later])
            place[later] = jnp.where(same, -1, place[later])
    high = [value.astype(bf16) for value in weight]
    low = [(value - top.astype(f32)).astype(bf16) for value, top in zip(weight, high)]
    place = [value.astype(i16) for value in place]
    zero = jnp.zeros((), bf16)

    def fill_rows(high_ref, low_ref, base):
        def body(first, block):
            row = row_numbers(first + base, block, cells)
            hits = [row == value for value in place]
            for target, values in ((high_ref, high), (low_ref, low)):
                entry = jnp.where(hits[0], values[0], jnp.where(hits[1], values[1], jnp.where(hits[2], values[2], zero)))
                target[pl.ds(first, block), :] = entry

        by_blocks(high_ref.shape[0], body)

    fill_rows(near_high_ref, near_low_ref, 0)
    fill_rows(far_high_ref, far_low_ref, near_high_ref.shape[0])


def cell_setup_kernel(
    coupling_hbm, list_ref, speed_hbm, speed_ref, inverse_ref, forward_ref, back_ref, outer_matrix_ref, rest_matrix_ref, coupling_ref, column_ref, sems
):
    coupling, speed = start_fetch([(coupling_hbm, coupling_ref), (speed_hbm, speed_ref)], sems)
    levels, _, cells = coupling_ref.shape
    fill_sent(outer_matrix_ref, list_ref, OUTER_SENT)
    fill_sent(rest_matrix_ref, list_ref, REST_SENT)
    coupling.wait()
    speed.wait()
    step = column_ref.shape[0] // round_up(levels, 16)
    column_ref[...] = jnp.zeros(column_ref.shape, f32)
    for group in range(cells // LANES):
        column_ref[pl.ds(group, levels, stride=step), :] = coupling_ref[:, 0, group * LANES : (group + 1) * LANES]
    at = lambda level: slice(level * step, (level + 1) * step)
    above = column_ref[at(0), :]
    inverse = 1.0 / (1.0 + above)
    inverse_ref[at(0), :] = inverse
    ratio = above * inverse
    back_ref[at(0), :] = ratio
    for level in range(1, levels):
        below = above
        above = column_ref[at(level), :]
        inverse = 1.0 / (1.0 + below + above - below * ratio)
        inverse_ref[at(level), :] = inverse
        forward_ref[at(level), :] = below * inverse
        ratio = above * inverse
        back_ref[at(level), :] = ratio


def part_kernel(own_ref, inner_ref, outer_ref, *rest):
    *matrix_refs, total_ref, stack_ref = rest
    rows, width = own_ref.shape
    halo = inner_ref.shape[2]
    put_parts(stack_ref, own_ref[...], 0)
    put_parts(stack_ref, inner_ref[0], width)
    put_parts(stack_ref, outer_ref[0], width + halo)
    total_ref[...] = gather_matmul(stack_ref, [ref[...] for ref in matrix_refs], rows)


def early_part_kernel(own_ref, inner_ref, outer_ref, early_first_ref, early_second_ref, *rest):
    *matrix_refs, total_ref, stack_ref, early_stack_ref = rest
    near_refs, far_refs = matrix_refs[: len(matrix_refs) // 2], matrix_refs[len(matrix_refs) // 2 :]
    part_kernel(own_ref, inner_ref, outer_ref, *near_refs, total_ref, stack_ref)
    total_ref[...] = lat_share(total_ref, early_first_ref, far_refs, early_stack_ref, 0)
    total_ref[...] = lat_share(total_ref, early_second_ref, far_refs, early_stack_ref, 3)


def lat_share(total_ref, lat_ref, matrix_refs, stack_ref, first):
    rows = total_ref.shape[0]
    count, _, halo = lat_ref.shape
    for member in range(count):
        put_parts(stack_ref, lat_ref[member], member * halo)
    matrices = [ref[first * halo : (first + count) * halo, :] for ref in matrix_refs]
    return total_ref[...] + gather_matmul(stack_ref, matrices, rows)


def inner_share_kernel(total_ref, lat_inner_ref, *rest):
    *matrix_refs, new_total_ref, stack_ref = rest
    new_total_ref[...] = lat_share(total_ref, lat_inner_ref, matrix_refs, stack_ref, 3 - lat_inner_ref.shape[0])


def sent_base_kernel(total_ref, lat_inner_ref, far_ref, edges_ref, scale_ref, matrix_ref, new_total_ref, base_ref, stack_ref, own_stack_ref):
    total = lat_share(total_ref, lat_inner_ref, [far_ref], stack_ref, 3 - lat_inner_ref.shape[0])
    new_total_ref[...] = total
    put_parts(own_stack_ref, edges_ref[...] - scale_ref[...] * total, 0)
    base_ref[...] = gather_matmul(own_stack_ref, [matrix_ref[...]], total_ref.shape[0])


def edge_sent_kernel(base_ref, lat_outer_ref, late_ref, sent_scale_ref, outer_ref, stack_ref):
    rows = base_ref.shape[0]
    count, _, halo = lat_outer_ref.shape
    for member in range(count):
        put_parts(stack_ref, lat_outer_ref[member], member * halo)
    late = late_ref[late_ref.shape[0] - count * halo :, :]
    store_outer(base_ref[...] - sent_scale_ref[...] * gather_matmul(stack_ref, [late], rows), outer_ref)


def edge_rest_kernel(total_ref, lat_outer_ref, far_ref, edges_ref, scale_ref, matrix_ref, new_edges_ref, inner_ref, lat_inner_ref, lat_outer_out_ref, stack_ref, own_stack_ref):
    difference = lat_share(total_ref, lat_outer_ref, [far_ref], stack_ref, 6 - lat_outer_ref.shape[0])
    new_edges = edges_ref[...] - scale_ref[...] * difference
    new_edges_ref[...] = new_edges
    put_parts(own_stack_ref, new_edges, 0)
    store_rest(gather_matmul(own_stack_ref, [matrix_ref[...]], edges_ref.shape[0]), inner_ref, lat_inner_ref, lat_outer_out_ref)


def solve_columns(total_ref, lat_outer_ref, high_ref, low_ref, cells_ref, speed_ref, inverse_ref, forward_ref, back_ref, levels, stack_ref, column_ref):
    rows, cells = cells_ref.shape
    divergence = lat_share(total_ref, lat_outer_ref, [high_ref, low_ref], stack_ref, 6 - lat_outer_ref.shape[0])
    right_side = cells_ref[...] - speed_ref[...] * divergence
    step = column_ref.shape[0] // rows
    for group in range(cells // LANES):
        column_ref[pl.ds(group, rows, stride=step), :] = right_side[:, group * LANES : (group + 1) * LANES]
    for group in range(cells // LANES, step):
        column_ref[pl.ds(group, rows, stride=step), :] = jnp.zeros((rows, LANES), f32)
    at = lambda level: slice(level * step, (level + 1) * step)
    current = column_ref[at(0), :] * inverse_ref[at(0), :]
    scaled = [current]
    for level in range(1, levels):
        current = column_ref[at(level), :] * inverse_ref[at(level), :] + forward_ref[at(level), :] * current
        scaled.append(current)
    column_ref[at(levels - 1), :] = current
    for level in range(levels - 2, -1, -1):
        current = scaled[level] + back_ref[at(level), :] * current
        column_ref[at(level), :] = current
    for level in range(levels, rows):
        column_ref[at(level), :] = jnp.zeros_like(current)


def solved(column_ref, group, rows):
    return column_ref[pl.ds(group, rows, stride=column_ref.shape[0] // rows), :]


def cell_kernel(
    total_ref,
    lat_outer_ref,
    high_ref,
    low_ref,
    cells_ref,
    speed_ref,
    inverse_ref,
    forward_ref,
    back_ref,
    matrix_ref,
    new_cells_ref,
    outer_ref,
    own_stack_ref,
    stack_ref,
    column_ref,
    *,
    levels,
):
    rows, cells = cells_ref.shape
    solve_columns(total_ref, lat_outer_ref, high_ref, low_ref, cells_ref, speed_ref, inverse_ref, forward_ref, back_ref, levels, stack_ref, column_ref)
    for group in range(cells // LANES):
        part = solved(column_ref, group, rows)
        new_cells_ref[:, group * LANES : (group + 1) * LANES] = part
        put_parts(own_stack_ref, part, group * LANES)
    store_outer(gather_matmul(own_stack_ref, [matrix_ref[...]], rows), outer_ref)


def last_kernel(
    total_ref, lat_outer_ref, high_ref, low_ref, cells_ref, speed_ref, inverse_ref, forward_ref, back_ref, out_ref, stack_ref, column_ref, *, levels
):
    rows, cells = cells_ref.shape
    solve_columns(total_ref, lat_outer_ref, high_ref, low_ref, cells_ref, speed_ref, inverse_ref, forward_ref, back_ref, levels, stack_ref, column_ref)
    for group in range(cells // LANES):
        out_ref[:, 0, group * LANES : (group + 1) * LANES] = solved(column_ref, group, rows)[0:levels]


def call(body, outs, scratch, *operands, raw=(), copies=0):
    in_vmem = pl.BlockSpec(memory_space=pltpu.VMEM)
    in_hbm = pl.BlockSpec(memory_space=pltpu.HBM)
    scratch_shapes = [pltpu.VMEM(shape, kind) for shape, kind in scratch]
    if copies:
        scratch_shapes.append(pltpu.SemaphoreType.DMA((copies,)))
    operands = [pltpu.with_memory_space_constraint(x, pltpu.HBM) if i in raw else x for i, x in enumerate(operands)]
    return pl.pallas_call(
        body,
        out_shape=tuple(jax.ShapeDtypeStruct(shape, kind) for shape, kind in outs),
        in_specs=[in_hbm if i in raw else in_vmem for i in range(len(operands))],
        out_specs=tuple(in_vmem for _ in outs),
        scratch_shapes=scratch_shapes,
        compiler_params=pltpu.CompilerParams(vmem_limit_bytes=24 * 1024 * 1024),
    )(*operands)


def on_device(lat_count, lon_count, pressure, velocity, edge_cells, cell_edges, send_cells, send_edges, inv_dual, edge_weight, sound_speed, coupling):
    _, levels, cells = pressure.shape
    edges = velocity.shape[2]
    halo = send_cells.shape[2]
    rows = round_up(levels, 16)
    edge_pad = round_up(edges, 2 * LANES)
    bundle = ((3, rows, halo), f32)
    straight = ((rows, halo), f32)
    lon_routes = swap_routes(lon_count)
    lat_inner_route = swap_routes(lat_count)[0]
    lat_outer_route = lat_outer_routes(lat_count, lon_count)
    i32 = jnp.int32

    by_level = lambda value: value.transpose(1, 0, 2)
    stack_cells = ((PARTS * rows, cells), bf16)
    stack_edges = ((PARTS * rows, edge_pad), bf16)
    stack_lat = lambda count: ((PARTS * rows, count * halo), bf16)
    column = ((rows * round_up(cells // LANES, 8), LANES), f32)
    sent_outer = lambda width: ((width, 3 * halo), bf16)
    sent_rest = lambda width: ((width, 5 * halo), bf16)

    for phase in range(2 * NSUB):
        at_cells = phase % 2 == 0
        if phase == 0:
            values, stack, outer, cell_list = call(
                start_kernel,
                [((rows, cells), f32), stack_cells, bundle, (send_cells.shape[1:], i32)],
                [((levels, 1, cells), f32), sent_outer(cells)],
                by_level(pressure),
                send_cells[0],
                raw=(0, 1),
                copies=2,
            )
        outer_in = lax.ppermute(outer, "lon", lon_routes[1])
        if phase == 0:
            inner, lat_inner, lat_outer = call(first_rest_kernel, [bundle, straight, straight], [sent_rest(cells)], stack, cell_list)
        elif at_cells:
            inner, lat_inner, lat_outer = call(rest_kernel, [bundle, straight, straight], [], stack, cell_rest)
        else:
            normal, inner, lat_inner, lat_outer = call(
                edge_rest_kernel,
                [((rows, edge_pad), f32), bundle, straight, straight],
                [stack_lat(second_in.shape[0]), stack_edges],
                total,
                second_in,
                gradient_far,
                normal,
                scale,
                edge_rest,
            )
        inner_in = lax.ppermute(inner, "lon", lon_routes[0])
        if phase == 0:
            gradient_near, gradient_far = call(
                functools.partial(gradient_kernel, cells=cells, halo=halo, lat_count=lat_count),
                [((cells + 2 * halo, edge_pad), bf16), ((6 * halo, edge_pad), bf16)],
                [(edge_cells.shape[1:], i32)],
                edge_cells[0],
                raw=(0,),
                copies=1,
            )
        if phase == 1:
            near_high, near_low, far_high, far_low = call(
                functools.partial(weight_kernel, edges=edges, edge_pad=edge_pad, halo=halo, lat_count=lat_count),
                [((edge_pad + 2 * halo, cells), bf16)] * 2 + [((6 * halo, cells), bf16)] * 2,
                [((3, 1, cells), i32), ((3, 1, cells), f32)],
                by_level(cell_edges),
                by_level(edge_weight),
                raw=(0, 1),
                copies=2,
            )
        early = phase >= 2
        first = outer_in[1:2] if early else jnp.stack([inner_in[1], lat_inner, outer_in[1]])
        if early:
            early_first = lax.ppermute(jnp.stack([inner_in[1], lat_inner]), "lat", lat_inner_route)
            early_in = lax.ppermute(jnp.stack([inner_in[2], lat_outer]), ("lat", "lon"), lat_outer_route)
            second = outer_in[2:3]
        else:
            second = jnp.stack([inner_in[2], lat_outer, outer_in[2]])
        first_in = lax.ppermute(first, "lat", lat_inner_route)
        second_in = lax.ppermute(second, ("lat", "lon"), lat_outer_route)
        count = second.shape[0]
        if phase == 0:
            normal, scale, edge_outer, edge_rest, late_sent, sent_scale = call(
                edge_setup_kernel,
                [((rows, edge_pad), f32), ((1, edge_pad), f32), sent_outer(edge_pad), sent_rest(edge_pad), sent_outer(3 * halo), ((1, 3 * halo), f32)],
                [((levels, 1, edges), f32), (send_edges.shape[1:], i32), ((1, edges), f32), ((PARTS * 16, edge_pad), bf16)],
                by_level(velocity),
                send_edges[0],
                inv_dual,
                gradient_far,
                raw=(0, 1, 2),
                copies=3,
            )
        if phase == 1:
            speed, inverse, forward, back, cell_outer, cell_rest = call(
                cell_setup_kernel,
                [((1, cells), f32), column, column, column, sent_outer(cells), sent_rest(cells)],
                [((levels, 1, cells), f32), column],
                by_level(coupling),
                cell_list,
                sound_speed,
                raw=(0, 2),
                copies=2,
            )
        if at_cells:
            (total,) = call(
                early_part_kernel if early else part_kernel,
                [((rows, edge_pad), f32)],
                [((PARTS * rows, cells + 2 * halo), bf16)] + ([stack_lat(2)] if early else []),
                values,
                inner_in,
                outer_in,
                *([early_first, early_in, gradient_near, gradient_far] if early else [gradient_near]),
            )
            total, base = call(
                sent_base_kernel,
                [((rows, edge_pad), f32), ((rows, 3 * halo), f32)],
                [stack_lat(count), stack_edges],
                total,
                first_in,
                gradient_far,
                normal,
                scale,
                edge_outer,
            )
            (outer,) = call(edge_sent_kernel, [bundle], [stack_lat(count)], base, second_in, late_sent, sent_scale)
        else:
            (total,) = call(
                early_part_kernel if early else part_kernel,
                [((rows, cells), f32)],
                [((PARTS * rows, edge_pad + 2 * halo), bf16)] + ([stack_lat(2)] if early else []),
                normal,
                inner_in,
                outer_in,
                *([early_first, early_in, near_high, near_low, far_high, far_low] if early else [near_high, near_low]),
            )
            (total,) = call(inner_share_kernel, [((rows, cells), f32)], [stack_lat(count)], total, first_in, far_high, far_low)
            operands = (total, second_in, far_high, far_low, values, speed, inverse, forward, back)
            if phase < 2 * NSUB - 1:
                values, outer, stack = call(
                    functools.partial(cell_kernel, levels=levels),
                    [((rows, cells), f32), bundle, stack_cells],
                    [stack_lat(count), column],
                    *operands,
                    cell_outer,
                )
            else:
                (values,) = call(functools.partial(last_kernel, levels=levels), [((levels, 1, cells), f32)], [stack_lat(count), column], *operands)
    return by_level(values), normal[:levels, :edges][None]


def solution(mesh):
    return jax.shard_map(
        functools.partial(on_device, mesh.shape["lat"], mesh.shape["lon"]),
        mesh=mesh,
        in_specs=(
            P("lat", None, "lon"),
            P("lat", None, "lon"),
            P("lat", None, "lon"),
            P("lat", None, "lon"),
            P("lat", None, "lon"),
            P("lat", None, "lon"),
            P("lat", "lon"),
            P("lat", None, "lon"),
            P("lat", "lon"),
            P("lat", None, "lon"),
        ),
        out_specs=(P("lat", None, "lon"), P("lat", None, "lon")),
        check_vma=False,
    )
```
